128 devices in a mesh: row: 8 (over x, core), col: 16 (over z, y).
Axes of the slice: x: 4, y: 4, z: 4, core: 2. Of those that a mesh axis runs over, the one named last changes fastest.
Arguments:
- jump: float32 [3, 512, 2048], P(None, 'row', 'col'), may hold values from -6 to 6
- external: float32 [3, 512, 2048], P(None, 'row', 'col'), may hold values from -12 to 12
- cohesive: float32 [512, 2048], P('row', 'col'), may hold values from 0.5 to 4
- bond_mask: int32 [2, 512, 2048], P(None, 'row', 'col'), may hold values 0 or 1
- load_factor: float32 [1], replicated, may hold values from 0.5 to 1.5
- arc_radius: float32 [1], replicated, may hold values from 0.5 to 1.5
- stiffness: bfloat16 [1536, 1536], replicated, may hold values from -1 to 2
- coupling: float32 [3, 1536], replicated, may hold values from -6 to 6
- old_state: float32 [20480, 1536], P(('row', 'col')), may hold values from -3 to 3
- old_history: float32 [20480, 1536], P(('row', 'col')), may hold values from 0 to 1.5
- newton_steps: int32 [20480], P(('row', 'col')), may hold values from 0 to 9, as said below
- point_ids: int32 [20480], P(('row', 'col')), may hold values from 0 to 8191, as said below
Outputs:
- new_jump: float32 [3, 512, 2048], P(None, 'row', 'col')
- new_load: float32 [1], replicated
- new_state: float32 [10240, 1536], P(('row', 'col'))
- new_history: float32 [10240, 1536], P(('row', 'col'))
The draws below stay inside these ranges and needn't reach their ends.
Inputs may be any that keep to these rules, and one draw needn't show every extreme that they name: `newton_steps`: within one block the live slots number between 20 and 160, and some block has all 160 live; in all at most 8960 slots are live; a live slot's count is at least 2. `point_ids`: the slots of one block name distinct points of that block.
All inputs are finite; a program needn't handle non-finite values. No bound on the sum of `bond_mask` on one device may be relied on, other than what follows from the above.
Results may differ from the reference program's by a relative error of at most 0.0028.
Values sent between devices are 32-bit elements; how exact they have to be, the bound alone decides.
No kernel may reach another device: no remote copies, remote signals or barrier semaphores. Data moves between devices by JAX's collectives and lax.ppermute only.
A program may use at most 64 MiB of HBM per device.

```python
import math
import jax
import jax.numpy as jnp
from jax import lax

CELLS = 1536
S_CAP = 160
PX = 64
PY = 128
MAX_STEPS = 9
SWEEPS = 3
NEW_CAP = 80
GX = 512
GY = 2048
SLOTS = 20480
NEW_SLOTS = 10240
N_ROW = 8
N_COL = 16


def draw_stiffness(key, part):
    first, second = jax.random.split(jax.random.fold_in(key, 11))
    noise = jax.random.normal(first, (CELLS, CELLS), jnp.float32) * (0.3 / math.sqrt(CELLS))
    symmetric = (noise + noise.T) / math.sqrt(2.0)
    leading = jax.random.uniform(second, (CELLS,), jnp.float32, 1.0, 2.0)
    identity = jnp.eye(CELLS, dtype=jnp.float32)
    return (symmetric * (1.0 - identity) + identity * leading[None, :]).astype(jnp.bfloat16)


def draw_external(key, part):
    shape = (3, GX, GY)
    position = jnp.arange(GX, dtype=jnp.float32)[None, :, None] / GX
    inner = jax.random.fold_in(key, 17)
    rough = jnp.clip(jax.random.normal(inner, shape, jnp.float32), -4.0, 4.0)
    return rough * (1.0 + 2.0 * position)


def draw_newton_steps(key, part):
    blocks = SLOTS // S_CAP
    order_key, size_key, place_key, step_key = jax.random.split(jax.random.fold_in(key, 29), 4)
    order = jax.random.permutation(order_key, blocks)
    crowded = order < blocks // 4
    sparse = jax.random.randint(size_key, (blocks,), S_CAP // 8, S_CAP // 4 + 1)
    held = jnp.where(crowded, S_CAP, sparse)

    def arrange(inner):
        return jax.random.permutation(inner, S_CAP)
    places = jax.vmap(arrange)(jax.random.split(place_key, blocks))
    occupied = places < held[:, None]
    counts = jax.random.randint(step_key, (blocks, S_CAP), 2, MAX_STEPS + 1)
    return jnp.where(occupied, counts, 0).reshape(SLOTS).astype(jnp.int32)


def draw_point_ids(key, part):
    blocks = SLOTS // S_CAP

    def choose(inner):
        return jax.random.permutation(inner, PX * PY)[:S_CAP]
    keys = jax.random.split(jax.random.fold_in(key, 31), blocks)
    return jax.vmap(choose)(keys).reshape(SLOTS).astype(jnp.int32)


def set_ends(values, stream_key, least, largest):
    extent = values.shape
    place = [jax.random.randint(jax.random.fold_in(stream_key, axis), (), 0, extent[axis]) for axis in range(len(extent))]
    values = values.at[tuple(place)].set(least)
    longest = extent.index(max(extent))
    place[longest] = (place[longest] + 1) % extent[longest]
    return values.at[tuple(place)].set(largest)


def block_levels(own_key, dims, cuts, least, top_value):
    def one(dim, shards_of):
        steps = jax.random.uniform(jax.random.fold_in(jax.random.fold_in(own_key, 6), dim), (shards_of,), jnp.float32, least / len(cuts), top_value / len(cuts))
        return jnp.repeat(jnp.exp(steps), dims[dim] // shards_of).reshape((-1,) + (1,) * (len(dims) - dim - 1))

    loudness = one(*cuts[0])
    for cut in cuts[1:]:
        loudness = loudness * one(*cut)
    return loudness


def scatter_about(stream_key, shape, spread, limit, pieces=(), kind=jnp.bfloat16):
    values = jax.random.normal(stream_key, shape, jnp.float32) * spread
    if len(pieces) > 0:
        values = block_levels(stream_key, shape, pieces, -0.22, 0.18) * values
    return jnp.clip(values, min=-limit, max=limit).astype(kind)


def setup_inputs(seed: int = 0) -> dict:
    streams_of = jax.random.split(jax.random.key(seed), 13)
    return {
        "jump": scatter_about(streams_of[0], (3, GX, GY), 1.0, 6.0, ((1, 8), (2, 16)), jnp.float32),
        "external": draw_external(jax.random.fold_in(streams_of[12], 71), 0),
        "cohesive": jnp.clip(jnp.exp(math.log(4.0) - 2.0794415 * jax.random.uniform(streams_of[2], (GX, GY), jnp.float32) ** block_levels(streams_of[2], (GX, GY), ((0, 8), (1, 16)), -0.2, 0.2)), 0.5, 4.0),
        "bond_mask": set_ends((jax.random.randint(streams_of[3], (2, GX, GY), 0, 4) < 3).astype(jnp.int32), jax.random.fold_in(streams_of[3], 1), 0, 1),
        "load_factor": jnp.clip(jax.random.uniform(streams_of[4], (1,), jnp.float32, 0.5, 1.5), 0.5, 1.5),
        "arc_radius": jnp.clip(jax.random.uniform(streams_of[5], (1,), jnp.float32, 0.5, 1.5), 0.5, 1.5),
        "stiffness": draw_stiffness(jax.random.fold_in(streams_of[12], 71), 0),
        "coupling": scatter_about(streams_of[7], (3, CELLS), 1.0, 6.0, (), jnp.float32),
        "old_state": scatter_about(streams_of[8], (SLOTS, CELLS), 0.5, 3.0, ((0, 128),), jnp.float32),
        "old_history": jnp.clip(1.5 * jax.random.uniform(streams_of[9], (SLOTS, CELLS), jnp.float32) ** block_levels(streams_of[9], (SLOTS, CELLS), ((0, 128),), -0.2, 0.2), 0.0, 1.5),
        "newton_steps": draw_newton_steps(jax.random.fold_in(streams_of[12], 71), 0),
        "point_ids": draw_point_ids(jax.random.fold_in(streams_of[12], 71), 0),
    }


softening = 1.0

def micro_solve(state, history, drive, steps, stiffness, coupling):
    diagonal = jnp.diagonal(stiffness).astype(jnp.float32)
    load = jnp.dot(drive, coupling, precision=lax.Precision.HIGHEST)
    damage = jnp.exp(-history)

    def advance(count, current):
        bent = jnp.tanh(current)
        force = jnp.dot(current.astype(jnp.bfloat16), stiffness, preferred_element_type=jnp.float32)
        misfit = force + softening * damage * bent - load
        slope = diagonal + softening * damage * (1.0 - bent * bent)
        return jnp.where((count < steps)[:, None], current - misfit / slope, current)
    state = lax.fori_loop(0, MAX_STEPS, advance, state)
    bent = jnp.tanh(state)
    cells = state.shape[1]
    traction = jnp.dot(softening * damage * bent, coupling.T, precision=lax.Precision.HIGHEST) / cells
    weight = softening * damage * (1.0 - bent * bent)
    products = jnp.stack([coupling[0] * coupling[0], coupling[1] * coupling[1], coupling[2] * coupling[2], coupling[0] * coupling[1], coupling[0] * coupling[2], coupling[1] * coupling[2]])
    tangent = jnp.dot(weight, products.T, precision=lax.Precision.HIGHEST) / cells
    history = jnp.maximum(history, jnp.abs(state))
    return (state, history, traction, tangent)

def block_solve(scale, tangent, source):
    d00 = scale + tangent[0]
    d11 = scale + tangent[1]
    d22 = scale + tangent[2]
    d01, d02, d12 = (tangent[3], tangent[4], tangent[5])
    c00 = d11 * d22 - d12 * d12
    c11 = d00 * d22 - d02 * d02
    c22 = d00 * d11 - d01 * d01
    c01 = d02 * d12 - d01 * d22
    c02 = d01 * d12 - d02 * d11
    c12 = d01 * d02 - d00 * d12
    determinant = d00 * c00 + d01 * c01 + d02 * c02
    first = (c00 * source[0] + c01 * source[1] + c02 * source[2]) / determinant
    second = (c01 * source[0] + c11 * source[1] + c12 * source[2]) / determinant
    third = (c02 * source[0] + c12 * source[1] + c22 * source[2]) / determinant
    return jnp.stack([first, second, third])

def neighbours(field, bond_x, low_x, bond_y, low_y):
    padded = jnp.pad(field, ((0, 0), (1, 1), (1, 1)))
    return bond_x * padded[:, 2:, 1:-1] + low_x * padded[:, :-2, 1:-1] + bond_y * padded[:, 1:-1, 2:] + low_y * padded[:, 1:-1, :-2]

def reference(jump, external, cohesive, bond_mask, load_factor, arc_radius, stiffness, coupling, old_state, old_history, newton_steps, point_ids):
    devices = N_ROW * N_COL
    slot_block = jnp.arange(SLOTS, dtype=jnp.int32) // S_CAP
    grid_x = slot_block // N_COL * PX + point_ids // PY
    grid_y = slot_block % N_COL * PY + point_ids % PY
    drive = jump[:, grid_x, grid_y].T
    live = newton_steps > 0
    live_float = live.astype(jnp.float32)

    def per_block(block):
        return micro_solve(block[0], block[1], block[2], block[3], stiffness, coupling)
    blocks = (old_state.reshape(devices, S_CAP, CELLS), old_history.reshape(devices, S_CAP, CELLS), drive.reshape(devices, S_CAP, 3), newton_steps.reshape(devices, S_CAP))
    state, history, traction, tangent = lax.map(per_block, blocks)
    state = state.reshape(SLOTS, CELLS)
    history = history.reshape(SLOTS, CELLS)
    traction = traction.reshape(SLOTS, 3)
    tangent = tangent.reshape(SLOTS, 6)
    soft = jnp.zeros((GX, GY), jnp.float32).at[grid_x, grid_y].add(live_float)
    rve_traction = jnp.zeros((3, GX, GY), jnp.float32).at[:, grid_x, grid_y].add((traction * live_float[:, None]).T)
    rve_tangent = jnp.zeros((6, GX, GY), jnp.float32).at[:, grid_x, grid_y].add((tangent * live_float[:, None]).T)
    bond_x = 0.25 + 0.75 * bond_mask[0].astype(jnp.float32)
    bond_y = 0.25 + 0.75 * bond_mask[1].astype(jnp.float32)
    low_x = jnp.pad(bond_x, ((1, 0), (0, 0)))[:-1]
    low_y = jnp.pad(bond_y, ((0, 0), (1, 0)))[:, :-1]
    scale = bond_x + low_x + bond_y + low_y + (1.0 - soft) * cohesive
    residual = scale * jump - neighbours(jump, bond_x, low_x, bond_y, low_y) + rve_traction - load_factor[0] * external
    source = jnp.concatenate([-residual, external])

    def solve_both(values):
        return jnp.concatenate([block_solve(scale, rve_tangent, values[:3]), block_solve(scale, rve_tangent, values[3:])])
    iterate = solve_both(source)
    for sweep in range(SWEEPS):
        iterate = solve_both(source + neighbours(iterate, bond_x, low_x, bond_y, low_y))
    correction, direction = (iterate[:3], iterate[3:])
    cross = jnp.sum(correction * direction)
    square = jnp.sum(direction * direction)
    entries = 3.0 * GX * GY
    shifted = square + 0.25 * entries
    increment = (arc_radius[0] * jnp.sqrt(entries) * jnp.sqrt(shifted) - cross) / shifted
    new_jump = jump + correction + increment * direction
    new_load = load_factor + increment
    live_int = live.astype(jnp.int32)
    rank = jnp.cumsum(live_int, dtype=jnp.int32) - live_int
    home_block = rank // 2 % devices
    home_slot = 2 * (rank // (2 * devices)) + rank % 2
    target = jnp.where(live, home_block * NEW_CAP + home_slot, NEW_SLOTS).astype(jnp.int32)
    new_state = jnp.zeros((NEW_SLOTS, CELLS), jnp.float32).at[target].set(state, mode='drop')
    new_history = jnp.zeros((NEW_SLOTS, CELLS), jnp.float32).at[target].set(history, mode='drop')
    return (new_jump, new_load, new_state, new_history)
```

```python
import functools

import jax
import jax.numpy as jnp
from jax import lax
from jax.experimental import pallas as pl
from jax.experimental.pallas import tpu as pltpu
from jax.sharding import PartitionSpec as P


MAX_STEPS = 9
SWEEPS = 3
HALO = 4
FIELDS = 9
LANES = 128
ROWS_COLS = ("row", "col")
VMEM = pl.BlockSpec(memory_space=pltpu.VMEM)
SMEM = pl.BlockSpec(memory_space=pltpu.SMEM)
ANY = pl.BlockSpec(memory_space=pl.ANY)
F32 = jnp.float32
BF16 = jnp.bfloat16


def iota(shape, dim):
    return lax.broadcasted_iota(jnp.int32, shape, dim)


def three_parts(x):
    high = x.astype(BF16)
    rest = x - high.astype(F32)
    middle = rest.astype(BF16)
    low = (rest - middle.astype(F32)).astype(BF16)
    return high, middle, low


def times_transposed(a, b):
    return lax.dot_general(a, b, (((1,), (1,)), ((), ())), preferred_element_type=F32)


def put_row_edges(get, first_ref, last_ref, rows):
    for c in range(FIELDS):
        field = get(c)
        first_ref[HALO * c : HALO * (c + 1), :] = field[:HALO]
        last_ref[HALO * c : HALO * (c + 1), :] = field[rows - HALO :]


def with_row_halo(field, below, above, c):
    part = slice(HALO * c, HALO * (c + 1))
    return jnp.concatenate([field, below[part], above[part]], axis=0)


def fields_kernel(jump_ref, external_ref, cohesive_ref, mask_ref, slots_ref, out_ref, first_ref, last_ref):
    rows, lanes = cohesive_ref.shape
    slots = slots_ref.shape[1]
    ids = slots_ref[0:1, :]
    live = slots_ref[1:2, :] > 0
    at_row = ((iota((rows, slots), 0) == ids // lanes) & live).astype(F32).astype(BF16)
    at_lane = (iota((lanes, slots), 0) == ids % lanes).astype(F32).astype(BF16)
    soft = times_transposed(at_row, at_lane)
    for c in range(3):
        out_ref[c] = jump_ref[c]
        out_ref[3 + c] = external_ref[c]
    out_ref[6] = (1.0 - soft) * cohesive_ref[...]
    out_ref[7] = 0.25 + 0.75 * mask_ref[0].astype(F32)
    out_ref[8] = 0.25 + 0.75 * mask_ref[1].astype(F32)
    put_row_edges(lambda c: out_ref[c], first_ref, last_ref, rows)


def lane_edges_kernel(field_ref, below_ref, above_ref, out_ref):
    below, above = below_ref[...], above_ref[...]
    rows = field_ref.shape[1] + 2 * HALO
    lane = iota((rows, LANES), 1)
    wide = jnp.zeros((rows, LANES), F32)
    for c in range(FIELDS):
        whole = with_row_halo(field_ref[c], below, above, c)
        turned = pltpu.roll(whole, (2 * c + 1) * HALO, 1)
        wide = jnp.where(lane // (2 * HALO) == c, turned, wide)
    square = jnp.concatenate([wide, jnp.zeros((LANES - rows, LANES), F32)], axis=0)
    out_ref[...] = square.T[: 2 * HALO * FIELDS]


def newton_kernel(
    slots_ref, jump_ref, stiffness_ref, coupling_ref, state_in_ref, history_ref,
    state_ref, grid_ref, first_ref, last_ref,
    damage_ref, load_ref, diagonal_ref, rounded_ref,
):
    slots, cells = state_in_ref.shape
    rows, lanes = jump_ref.shape[1:]
    wide = slots_ref.shape[1]
    own = iota((slots, wide), 0) == iota((slots, wide), 1)

    def column(values):
        return jnp.sum(jnp.where(own, values, 0.0), axis=1, keepdims=True)

    ids_row = slots_ref[0:1, :]
    steps_row = slots_ref[1:2, :]
    steps = column(steps_row.astype(F32))
    at_x = column((ids_row // lanes).astype(F32))
    at_y = column((ids_row % lanes).astype(F32))
    pick_x = (iota((slots, rows), 1).astype(F32) == at_x).astype(F32).astype(BF16)
    pick_y = iota((slots, lanes), 1).astype(F32) == at_y
    drive = []
    for c in range(3):
        parts = three_parts(jump_ref[c])
        picked = [jnp.dot(pick_x, part, preferred_element_type=F32) for part in parts]
        whole = (picked[0] + picked[1]) + picked[2]
        drive.append(jnp.sum(jnp.where(pick_y, whole, 0.0), axis=1, keepdims=True))
    eye = iota((LANES, LANES), 0) == iota((LANES, LANES), 1)
    for t in range(cells // LANES):
        part = slice(t * LANES, (t + 1) * LANES)
        block = stiffness_ref[part, part].astype(F32)
        diagonal_ref[:, part] = jnp.sum(jnp.where(eye, block, 0.0), axis=0, keepdims=True)
    load_ref[...] = (
        drive[0] * coupling_ref[0:1, :] + drive[1] * coupling_ref[1:2, :] + drive[2] * coupling_ref[2:3, :]
    )
    damage_ref[...] = jnp.exp(-history_ref[...])
    first = state_in_ref[...]
    state_ref[...] = first
    rounded_ref[0] = first.astype(BF16)
    width = 256

    def advance(count, carry):
        now = lax.rem(count, 2)
        rounded = rounded_ref[now]
        moves = count.astype(F32) < steps
        for t in range(cells // width):
            part = slice(t * width, (t + 1) * width)
            force = jnp.dot(rounded, stiffness_ref[:, part], preferred_element_type=F32)
            current = state_ref[:, part]
            bent = jnp.tanh(current)
            damage = damage_ref[:, part]
            misfit = force + damage * bent - load_ref[:, part]
            slope = diagonal_ref[:, part] + damage * (1.0 - bent * bent)
            current = jnp.where(moves, current - misfit / slope, current)
            state_ref[:, part] = current
            rounded_ref[1 - now, :, part] = current.astype(BF16)
        return carry

    lax.fori_loop(0, MAX_STEPS, advance, 0)
    bent = jnp.tanh(state_ref[...])
    damage = damage_ref[...]
    pull = damage * bent
    weight = damage * (1.0 - bent * bent)
    c0, c1, c2 = (coupling_ref[k : k + 1, :] for k in range(3))
    sums = [jnp.sum(pull * c, axis=1, keepdims=True) for c in (c0, c1, c2)]
    sums += [
        jnp.sum(weight * c, axis=1, keepdims=True)
        for c in (c0 * c0, c1 * c1, c2 * c2, c0 * c1, c0 * c2, c1 * c2)
    ]
    lane = iota((slots, LANES), 1)
    table = jnp.zeros((slots, LANES), F32)
    for k, value in enumerate(sums):
        table = jnp.where(lane == k, value * (1.0 / cells), table)
    table = jnp.where(steps > 0.0, table, 0.0)
    table = jnp.concatenate([table, jnp.zeros((wide - slots, LANES), F32)], axis=0).T
    at_row = iota((rows, wide), 0) == ids_row // lanes
    at_lane = (iota((lanes, wide), 0) == ids_row % lanes).astype(F32).astype(BF16)
    pieces = []
    for c in range(FIELDS):
        placed = jnp.where(at_row, table[c : c + 1, :], 0.0)
        pieces.extend(three_parts(placed))
    spread = times_transposed(jnp.concatenate(pieces, axis=0), at_lane)
    for c in range(FIELDS):
        at = 3 * c * rows
        grid_ref[c] = spread[at : at + rows] + spread[at + rows : at + 2 * rows] + spread[at + 2 * rows : at + 3 * rows]
    put_row_edges(lambda c: grid_ref[c], first_ref, last_ref, rows)


def copy_rows(source_ref, target_ref, steps_ref, start):
    slots, cells = source_ref.shape
    sides = target_ref.shape[1] // 2
    width = cells // sides
    block_rows = 2 * target_ref.shape[0]

    def one(i, rank):
        alive = steps_ref[i] > 0

        @pl.when(alive)
        def _():
            at = lax.rem(rank, block_rows)
            block, side = at // 2, lax.rem(at, 2)
            for k in range(sides):
                target_ref[block, pl.ds(side * sides + k, 1), :] = source_ref[pl.ds(i, 1), k * width : (k + 1) * width]

        return rank + alive.astype(jnp.int32)

    lax.fori_loop(0, slots, one, start)


def pack_history_kernel(here_ref, steps_ref, counts_ref, history_ref, out_ref, plan_ref):
    devices = counts_ref.shape[0]
    here = here_ref[0]
    counts = counts_ref[...]
    before = (iota((devices, devices), 1) < iota((devices, devices), 0)).astype(F32).astype(BF16)
    starts = jnp.dot(before, counts.astype(BF16), preferred_element_type=F32)
    row = iota((devices, LANES), 0)
    start = jnp.sum(jnp.where(row < here, counts, 0.0)[:, 0:1]).astype(jnp.int32)
    total = jnp.sum(counts, axis=0, keepdims=True)
    slot = iota((1, LANES), 1)
    wanted = (2 * (here + devices * (slot // 2)) + slot % 2).astype(F32)
    source = jnp.sum(jnp.where(starts <= wanted, 1.0, 0.0), axis=0, keepdims=True) - 1.0
    index = jnp.where(wanted < total, 2.0 * source + (slot % 2).astype(F32), -1.0).astype(jnp.int32)
    line = iota((8, LANES), 0)
    plan_ref[...] = jnp.where(line == 0, index, jnp.where(line == 1, start, 0))
    copy_rows(history_ref, out_ref, steps_ref, start)


def pack_state_kernel(plan_ref, steps_ref, state_ref, out_ref):
    copy_rows(state_ref, out_ref, steps_ref, plan_ref[1, 0])


def after_kernel(data_ref, first_ref, second_ref, out_ref):
    del data_ref, first_ref, second_ref, out_ref


def unpack_kernel(plan_ref, state_ref, history_ref, new_state_ref, new_history_ref):
    new_cap, cells = new_state_ref.shape
    sides = state_ref.shape[1] // 2
    width = cells // sides

    def one(s, carry):
        index = plan_ref[0, s]
        valid = index >= 0
        at = jnp.maximum(index, 0)
        block, side = at // 2, lax.rem(at, 2)
        for k in range(sides):
            part = slice(k * width, (k + 1) * width)
            state = state_ref[block, pl.ds(side * sides + k, 1), :]
            history = history_ref[block, pl.ds(side * sides + k, 1), :]
            new_state_ref[pl.ds(s, 1), part] = jnp.where(valid, state, 0.0)
            new_history_ref[pl.ds(s, 1), part] = jnp.where(valid, jnp.maximum(history, jnp.abs(state)), 0.0)
        return carry

    lax.fori_loop(0, new_cap, one, 0)


def macro_kernel(
    place_ref, load_ref,
    field_ref, f_below_ref, f_above_ref, f_left_ref, f_right_ref,
    grid_ref, g_below_ref, g_above_ref, g_left_ref, g_right_ref,
    moved_ref, sums_ref,
):
    rows = field_ref.shape[1]
    tall = rows + 2 * HALO
    lane = iota((tall, LANES), 1)
    line = iota((tall, LANES), 0)
    row_at, col_at = place_ref[0], place_ref[1]
    has_above = (row_at > 0).astype(jnp.int32)
    has_below = (row_at < place_ref[2] - 1).astype(jnp.int32)
    has_left = (col_at > 0).astype(jnp.int32)
    has_right = (col_at < place_ref[3] - 1).astype(jnp.int32)
    row_ok = jnp.where(line < rows, 1, jnp.where(line < rows + HALO, has_below, has_above)) > 0
    side_ok = jnp.where(lane < HALO, has_right, jnp.where(lane >= LANES - HALO, has_left, 0)) > 0
    valid = (row_ok, row_ok & side_ok)

    def padded(ref, below_ref, above_ref, left_ref, right_ref):
        below, above = below_ref[...], above_ref[...]
        fill = jnp.zeros((LANES - left_ref.shape[0], LANES), F32)
        left = jnp.concatenate([left_ref[...], fill], axis=0).T[:tall]
        right = jnp.concatenate([right_ref[...], fill], axis=0).T[:tall]

        def one(c):
            middle = with_row_halo(ref[c], below, above, c)
            from_left = pltpu.roll(left, (LANES - HALO - 2 * HALO * c) % LANES, 1)
            from_right = pltpu.roll(right, (LANES - HALO - 2 * HALO * c) % LANES, 1)
            side = jnp.where(lane >= LANES - HALO, from_left, jnp.where(lane < HALO, from_right, 0.0))
            return (middle, side)

        return one

    def pairs(f, *operands):
        return tuple(f(*parts) for parts in zip(*operands))

    def below_of(v):
        return pairs(lambda x: pltpu.roll(x, tall - 1, 0), v)

    def above_of(v):
        return pairs(lambda x: pltpu.roll(x, 1, 0), v)

    def right_of(v):
        a, b = (pltpu.roll(x, LANES - 1, 1) for x in v)
        end = lane == LANES - 1
        return (jnp.where(end, b, a), jnp.where(end, a, b))

    def left_of(v):
        a, b = (pltpu.roll(x, 1, 1) for x in v)
        end = lane == 0
        return (jnp.where(end, b, a), jnp.where(end, a, b))

    field = padded(field_ref, f_below_ref, f_above_ref, f_left_ref, f_right_ref)
    grid = padded(grid_ref, g_below_ref, g_above_ref, g_left_ref, g_right_ref)
    bond_x, bond_y = field(7), field(8)
    low_x, low_y = above_of(bond_x), left_of(bond_y)
    scale = pairs(lambda a, b, c, d, e: a + b + c + d + e, bond_x, low_x, bond_y, low_y, field(6))

    def neighbours(v):
        return pairs(
            lambda bx, vb, lx, va, by, vr, ly, vl: bx * vb + lx * va + by * vr + ly * vl,
            bond_x, below_of(v), low_x, above_of(v), bond_y, right_of(v), low_y, left_of(v),
        )

    load = load_ref[0]
    sources = []
    for c in range(3):
        jump = field(c)
        external = field(3 + c)
        residual = pairs(
            lambda s, j, n, t, e: s * j - n + t - load * e, scale, jump, neighbours(jump), grid(c), external
        )
        sources.append((pairs(lambda r: -r, residual), external))

    def inverse_of(s, t00, t11, t22, t01, t02, t12, ok):
        d00, d11, d22 = s + t00, s + t11, s + t22
        c00 = d11 * d22 - t12 * t12
        c11 = d00 * d22 - t02 * t02
        c22 = d00 * d11 - t01 * t01
        c01 = t02 * t12 - t01 * d22
        c02 = t01 * t12 - t02 * d11
        c12 = t01 * t02 - d00 * t12
        determinant = d00 * c00 + t01 * c01 + t02 * c02
        over = jnp.where(ok, 1.0 / jnp.where(ok, determinant, 1.0), 0.0)
        return tuple(c * over for c in (c00, c11, c22, c01, c02, c12))

    both = pairs(inverse_of, scale, *(grid(3 + k) for k in range(6)), valid)
    i00, i11, i22, i01, i02, i12 = (tuple(both[t][k] for t in range(2)) for k in range(6))

    def dot3(a, x, b, y, c, z):
        return pairs(lambda a, x, b, y, c, z: a * x + b * y + c * z, a, x, b, y, c, z)

    def solve(w):
        return [
            dot3(i00, w[0], i01, w[1], i02, w[2]),
            dot3(i01, w[0], i11, w[1], i12, w[2]),
            dot3(i02, w[0], i12, w[1], i22, w[2]),
        ]

    done = []
    for half in range(2):
        source = [sources[c][half] for c in range(3)]
        iterate = solve(source)
        for _ in range(SWEEPS):
            iterate = solve([pairs(jnp.add, source[c], neighbours(iterate[c])) for c in range(3)])
        done.append([iterate[c][0][:rows] for c in range(3)])
    cross = square = 0.0
    for c in range(3):
        moved_ref[c] = done[0][c]
        moved_ref[3 + c] = done[1][c]
        cross = cross + done[0][c] * done[1][c]
        square = square + done[1][c] * done[1][c]
    half = iota(sums_ref.shape, 1) < LANES // 2
    sums_ref[...] = jnp.where(half, jnp.sum(cross), jnp.sum(square))


def finish_kernel(entries, load_ref, radius_ref, sums_ref, jump_ref, moved_ref, new_jump_ref, new_load_ref):
    whole = jnp.sum(sums_ref[...], axis=0, keepdims=True)
    half = iota(whole.shape, 1) < LANES // 2
    other = pltpu.roll(whole, LANES // 2, 1)
    cross, square = jnp.where(half, whole, other), jnp.where(half, other, whole)
    shifted = square + 0.25 * entries
    increment = (radius_ref[0] * (entries**0.5) * jnp.sqrt(shifted) - cross) / shifted
    for c in range(3):
        new_jump_ref[c] = jump_ref[c] + moved_ref[c] + increment * moved_ref[3 + c]
    new_load_ref[0] = load_ref[0] + jnp.max(increment)


def shape(*dims, dtype=F32):
    return jax.ShapeDtypeStruct(dims, dtype)


def call(kernel, outs, ins, out_specs, mib, scratch=(), cost=None, aliases=None):
    return pl.pallas_call(
        kernel,
        out_shape=outs,
        in_specs=ins,
        out_specs=out_specs,
        scratch_shapes=scratch,
        cost_estimate=cost,
        input_output_aliases=aliases or {},
        compiler_params=pltpu.CompilerParams(vmem_limit_bytes=mib * 1024 * 1024),
    )


def swap(first, last, axis):
    size = lax.axis_size(axis)
    up = [(i, i + 1) for i in range(size - 1)]
    down = [(i + 1, i) for i in range(size - 1)]
    above = lax.ppermute(last, axis, up)
    below = lax.ppermute(first, axis, down)
    return below, above


def on_device(
    jump, external, cohesive, bond_mask, load_factor, arc_radius, stiffness, coupling,
    old_state, old_history, newton_steps, point_ids,
):
    n_row, n_col = lax.axis_size("row"), lax.axis_size("col")
    devices = n_row * n_col
    row_at, col_at = lax.axis_index("row"), lax.axis_index("col")
    here = (row_at * n_col + col_at).astype(jnp.int32)
    slots, cells = old_state.shape
    _, rows, lanes = jump.shape
    edge = HALO * FIELDS
    blocks = shape(devices, 8, 2 * cells // 8)
    place = jnp.stack([row_at, col_at, n_row, n_col]).astype(jnp.int32)

    table = jnp.zeros((8, 256), jnp.int32)
    table = table.at[0, :slots].set(point_ids).at[1, :slots].set(newton_steps)

    def lane_edges(fields, below, above):
        return call(lane_edges_kernel, shape(2 * edge, LANES), [VMEM] * 3, VMEM, 4)(fields, below, above)

    live = jnp.sum((newton_steps > 0).astype(F32))
    counts = lax.all_to_all(jnp.broadcast_to(live, (devices, LANES)), ROWS_COLS, 0, 0, tiled=True)
    fields, first, last = call(
        fields_kernel,
        (shape(FIELDS, rows, lanes), shape(edge, LANES), shape(edge, LANES)),
        [VMEM] * 5,
        (VMEM,) * 3,
        4,
    )(jump, external, cohesive, bond_mask, table)
    f_below, f_above = swap(first, last, "row")
    turned = lane_edges(fields, f_below, f_above)
    f_right, f_left = swap(turned, turned, "col")
    packed_history, plan = call(
        pack_history_kernel,
        (blocks, shape(8, LANES, dtype=jnp.int32)),
        [SMEM, SMEM, VMEM, VMEM],
        (VMEM, VMEM),
        6,
    )(here[None], newton_steps, counts, old_history)
    history = lax.all_to_all(packed_history, ROWS_COLS, 0, 0, tiled=True)
    state, grid, first, last = call(
        newton_kernel,
        (shape(slots, cells), shape(FIELDS, rows, lanes), shape(edge, LANES), shape(edge, LANES)),
        [VMEM] * 6,
        (VMEM,) * 4,
        28,
        scratch=(
            pltpu.VMEM((slots, cells), F32),
            pltpu.VMEM((slots, cells), F32),
            pltpu.VMEM((1, cells), F32),
            pltpu.VMEM((2, slots, cells), BF16),
        ),
        cost=pl.CostEstimate(
            flops=2 * MAX_STEPS * slots * cells * cells,
            transcendentals=2 * MAX_STEPS * slots * cells,
            bytes_accessed=2 * cells * cells + 12 * slots * cells,
        ),
    )(table, jump, stiffness, coupling, old_state, old_history)
    g_below, g_above = swap(first, last, "row")
    packed_state = call(pack_state_kernel, blocks, [SMEM, SMEM, VMEM], VMEM, 6)(plan, newton_steps, state)
    turned = lane_edges(grid, g_below, g_above)
    g_right, g_left = swap(turned, turned, "col")
    packed_state = call(after_kernel, blocks, [ANY] * 3, ANY, 1, aliases={0: 0})(packed_state, g_right, g_left)
    arrived = lax.all_to_all(packed_state, ROWS_COLS, 0, 0, tiled=True)
    moved, sums = call(
        macro_kernel,
        (shape(6, rows, lanes), shape(devices, LANES)),
        [SMEM, SMEM] + [VMEM] * 10,
        (VMEM, VMEM),
        12,
        cost=pl.CostEstimate(flops=200_000_000, transcendentals=0, bytes_accessed=2_000_000),
    )(
        place, load_factor,
        fields, f_below, f_above, f_left, f_right,
        grid, g_below, g_above, g_left, g_right,
    )
    sums = lax.all_to_all(sums, ROWS_COLS, 0, 0, tiled=True)
    new_state, new_history = call(
        unpack_kernel,
        (shape(slots // 2, cells), shape(slots // 2, cells)),
        [SMEM, VMEM, VMEM],
        (VMEM, VMEM),
        8,
    )(plan, arrived, history)
    new_jump, new_load = call(
        functools.partial(finish_kernel, 3.0 * rows * lanes * devices),
        (shape(3, rows, lanes), shape(1)),
        [SMEM, SMEM, VMEM, VMEM, VMEM],
        (VMEM, SMEM),
        4,
    )(load_factor, arc_radius, sums, jump, moved)
    return (new_jump, new_load, new_state, new_history)


def solution(mesh):
    whole = P(None, "row", "col")
    slot_rows = P(ROWS_COLS, None)
    return jax.shard_map(
        on_device,
        mesh=mesh,
        in_specs=(
            whole, whole, P("row", "col"), whole, P(), P(), P(), P(),
            slot_rows, slot_rows, P(ROWS_COLS), P(ROWS_COLS),
        ),
        out_specs=(whole, P(), slot_rows, slot_rows),
        check_vma=False,
    )
```

```python
import functools

import jax
import jax.numpy as jnp
from jax import lax
from jax.experimental import pallas as pl
from jax.experimental.pallas import tpu as pltpu
from jax.sharding import PartitionSpec as P


MAX_STEPS = 9
SWEEPS = 3
HALO = 4
INPUT_FIELDS = 9
FIELDS = 18
LANES = 128
ROWS_COLS = ("row", "col")
VMEM = pl.BlockSpec(memory_space=pltpu.VMEM)
SMEM = pl.BlockSpec(memory_space=pltpu.SMEM)
HBM = pl.BlockSpec(memory_space=pltpu.HBM)
F32 = jnp.float32
BF16 = jnp.bfloat16


def iota(shape, dim):
    return lax.broadcasted_iota(jnp.int32, shape, dim)


def three_parts(x):
    high = x.astype(BF16)
    rest = x - high.astype(F32)
    middle = rest.astype(BF16)
    low = (rest - middle.astype(F32)).astype(BF16)
    return high, middle, low


def times_transposed(a, b):
    return lax.dot_general(a, b, (((1,), (1,)), ((), ())), preferred_element_type=F32)


def put_row_edges(field_ref, first_ref, last_ref):
    fields, rows, _ = field_ref.shape
    for c in range(fields):
        first_ref[HALO * c : HALO * (c + 1), :] = field_ref[c, :HALO, :]
        last_ref[HALO * c : HALO * (c + 1), :] = field_ref[c, rows - HALO :, :]


def with_row_halo(field, below, above, c):
    part = slice(HALO * c, HALO * (c + 1))
    return jnp.concatenate([field, below[part], above[part]], axis=0)


def count_kernel(steps_ref, out_ref):
    live = jnp.sum((steps_ref[...] > 0).astype(F32), axis=1, keepdims=True)
    out_ref[...] = jnp.broadcast_to(live[None], out_ref.shape)


def lane_edges_kernel(field_ref, below_ref, above_ref, to_left_ref, to_right_ref):
    below, above = below_ref[...], above_ref[...]
    fields, rows, lanes = field_ref.shape
    tall = rows + 2 * HALO
    group = iota((tall, lanes), 1) // HALO
    heads = tails = jnp.zeros((tall, lanes), F32)
    for c in range(fields):
        whole = with_row_halo(field_ref[c], below, above, c)
        heads = jnp.where(group == c, pltpu.roll(whole, HALO * c, 1) if c else whole, heads)
        tails = jnp.where(group == c, pltpu.roll(whole, HALO * (c + 1), 1), tails)
    fill = jnp.zeros((lanes - tall, lanes), F32)
    to_left_ref[...] = jnp.concatenate([heads, fill], axis=0).T[: HALO * fields]
    to_right_ref[...] = jnp.concatenate([tails, fill], axis=0).T[: HALO * fields]


def newton_kernel(
    ids_ref, steps_ref, jump_ref, stiffness_ref, coupling_ref, old_state_ref, history_ref,
    state_ref, grid_ref,
    damage_ref, load_ref, diagonal_ref, rounded_ref,
):
    slots, cells = state_ref.shape
    _, rows, lanes = jump_ref.shape
    wide = 2 * lanes
    fill = jnp.zeros((1, wide - slots), jnp.int32)
    ids_row = jnp.concatenate([ids_ref[...], fill], axis=1)
    steps_row = jnp.concatenate([steps_ref[...], fill], axis=1)
    own = iota((slots, wide), 0) == iota((slots, wide), 1)

    def column(values):
        return jnp.sum(jnp.where(own, values, 0.0), axis=1, keepdims=True)

    steps = column(steps_row.astype(F32))
    at_x = column((ids_row // lanes).astype(F32))
    at_y = column((ids_row % lanes).astype(F32))
    pick_x = (iota((slots, rows), 1).astype(F32) == at_x).astype(F32).astype(BF16)
    pick_y = iota((slots, lanes), 1).astype(F32) == at_y
    at_row = iota((rows, wide), 0) == ids_row // lanes
    at_lane = (iota((lanes, wide), 0) == ids_row % lanes).astype(F32).astype(BF16)
    drive = []
    for c in range(3):
        parts = three_parts(jump_ref[c])
        picked = [jnp.dot(pick_x, part, preferred_element_type=F32) for part in parts]
        whole = (picked[0] + picked[1]) + picked[2]
        drive.append(jnp.sum(jnp.where(pick_y, whole, 0.0), axis=1, keepdims=True))
    load_ref[...] = (
        drive[0] * coupling_ref[0:1, :] + drive[1] * coupling_ref[1:2, :] + drive[2] * coupling_ref[2:3, :]
    )
    damage_ref[...] = jnp.exp(-history_ref[...])
    first_state = old_state_ref[...]
    state_ref[...] = first_state
    rounded_ref[0] = first_state.astype(BF16)
    eye = iota((LANES, LANES), 0) == iota((LANES, LANES), 1)
    for t in range(cells // LANES):
        part = slice(t * LANES, (t + 1) * LANES)
        block = stiffness_ref[part, part].astype(F32)
        diagonal_ref[:, part] = jnp.sum(jnp.where(eye, block, 0.0), axis=0, keepdims=True)
    width = 256

    def advance(count, carry):
        now = lax.rem(count, 2)
        rounded = rounded_ref[now]
        moving = count.astype(F32) < steps
        for t in range(cells // width):
            part = slice(t * width, (t + 1) * width)
            force = jnp.dot(rounded, stiffness_ref[:, part], preferred_element_type=F32)
            current = state_ref[:, part]
            bent = jnp.tanh(current)
            damage = damage_ref[:, part]
            misfit = force + damage * bent - load_ref[:, part]
            slope = diagonal_ref[:, part] + damage * (1.0 - bent * bent)
            current = jnp.where(moving, current - misfit / slope, current)
            state_ref[:, part] = current
            rounded_ref[1 - now, :, part] = current.astype(BF16)
        return carry

    lax.fori_loop(0, MAX_STEPS, advance, 0)
    bent = jnp.tanh(state_ref[...])
    damage = damage_ref[...]
    pull = damage * bent
    weight = damage * (1.0 - bent * bent)
    c0, c1, c2 = (coupling_ref[k : k + 1, :] for k in range(3))
    sums = [jnp.sum(pull * c, axis=1, keepdims=True) for c in (c0, c1, c2)]
    sums += [
        jnp.sum(weight * c, axis=1, keepdims=True)
        for c in (c0 * c0, c1 * c1, c2 * c2, c0 * c1, c0 * c2, c1 * c2)
    ]
    lane = iota((slots, LANES), 1)
    table = jnp.zeros((slots, LANES), F32)
    for k, value in enumerate(sums):
        table = jnp.where(lane == k, value * (1.0 / cells), table)
    table = jnp.where(steps > 0.0, table, 0.0)
    table = jnp.concatenate([table, jnp.zeros((wide - slots, LANES), F32)], axis=0).T
    pieces = []
    for c in range(len(sums)):
        placed = jnp.where(at_row, table[c : c + 1, :], 0.0)
        pieces.extend(three_parts(placed))
    spread = times_transposed(jnp.concatenate(pieces, axis=0), at_lane)
    for c in range(len(sums)):
        at = 3 * c * rows
        grid_ref[c] = spread[at : at + rows] + spread[at + rows : at + 2 * rows] + spread[at + 2 * rows : at + 3 * rows]


def fields_kernel(
    ids_ref, steps_ref, jump_ref, external_ref, cohesive_ref, mask_ref, grid_ref, field_ref, first_ref, last_ref
):
    rows, lanes = cohesive_ref.shape
    slots = ids_ref.shape[1]
    ids = ids_ref[...]
    at_row = ((iota((rows, slots), 0) == ids // lanes) & (steps_ref[...] > 0)).astype(F32).astype(BF16)
    at_lane = (iota((lanes, slots), 0) == ids % lanes).astype(F32).astype(BF16)
    soft = times_transposed(at_row, at_lane)
    for c in range(3):
        field_ref[c] = jump_ref[c]
        field_ref[3 + c] = external_ref[c]
    field_ref[6] = (1.0 - soft) * cohesive_ref[...]
    field_ref[7] = 0.25 + 0.75 * mask_ref[0].astype(F32)
    field_ref[8] = 0.25 + 0.75 * mask_ref[1].astype(F32)
    for c in range(FIELDS - INPUT_FIELDS):
        field_ref[INPUT_FIELDS + c] = grid_ref[c]
    put_row_edges(field_ref, first_ref, last_ref)


def pack_kernel(here_ref, steps_ref, counts_ref, state_ref, history_ref, out_ref, plan_ref):
    slots, cells = state_ref.shape
    devices = counts_ref.shape[0]
    here = here_ref[0]
    counts = counts_ref[...]
    before = (iota((devices, devices), 1) < iota((devices, devices), 0)).astype(F32).astype(BF16)
    starts = jnp.dot(before, counts.astype(BF16), preferred_element_type=F32)
    row = iota((devices, LANES), 0)
    start = jnp.sum(jnp.where(row < here, counts, 0.0)[:, 0:1]).astype(jnp.int32)
    total = jnp.sum(counts, axis=0, keepdims=True)
    slot = iota((1, LANES), 1)
    wanted = (2 * (here + devices * (slot // 2)) + slot % 2).astype(F32)
    source = jnp.sum(jnp.where(starts <= wanted, 1.0, 0.0), axis=0, keepdims=True) - 1.0
    index = jnp.where(wanted < total, 2.0 * source + (slot % 2).astype(F32), -1.0).astype(jnp.int32)
    plan_ref[...] = jnp.broadcast_to(index, plan_ref.shape)
    places = out_ref.shape[0]
    unused = lax.rem(2 * (start // 2) + places - 2, places)
    group = 8

    def one(block, rank):
        at = pl.multiple_of(block * group, group)
        state = state_ref[pl.ds(at, group), :]
        history = history_ref[pl.ds(at, group), :]
        for k in range(group):
            alive = steps_ref[at + k] > 0
            to = jnp.where(alive, lax.rem(rank, places), unused)
            out_ref[pl.ds(to, 1), 0, :cells] = state[k : k + 1]
            out_ref[pl.ds(to, 1), 0, cells : 2 * cells] = history[k : k + 1]
            rank = rank + alive.astype(jnp.int32)
        return rank

    lax.fori_loop(0, slots // group, one, start)


def macro_kernel(
    place_ref, load_ref, field_ref, below_ref, above_ref, left_ref, right_ref, packed_hbm,
    moved_ref, packed_out, sums_ref, sem,
):
    del packed_hbm
    rows = field_ref.shape[1]
    tall = rows + 2 * HALO
    lane = iota((tall, LANES), 1)
    line = iota((tall, LANES), 0)
    row_at, col_at = place_ref[0], place_ref[1]
    has_above = (row_at > 0).astype(jnp.int32)
    has_below = (row_at < place_ref[2] - 1).astype(jnp.int32)
    has_left = (col_at > 0).astype(jnp.int32)
    has_right = (col_at < place_ref[3] - 1).astype(jnp.int32)
    row_ok = jnp.where(line < rows, 1, jnp.where(line < rows + HALO, has_below, has_above)) > 0
    side_ok = jnp.where(lane < HALO, has_right, jnp.where(lane >= LANES - HALO, has_left, 0)) > 0
    valid = (row_ok, row_ok & side_ok)
    below, above = below_ref[...], above_ref[...]
    fill = jnp.zeros((LANES - left_ref.shape[0], LANES), F32)
    left = jnp.concatenate([left_ref[...], fill], axis=0).T[:tall]
    right = jnp.concatenate([right_ref[...], fill], axis=0).T[:tall]

    def field(c):
        middle = with_row_halo(field_ref[c], below, above, c)
        from_left = pltpu.roll(left, (LANES - HALO - HALO * c) % LANES, 1)
        from_right = pltpu.roll(right, (LANES - HALO * c) % LANES, 1) if c else right
        side = jnp.where(lane >= LANES - HALO, from_left, jnp.where(lane < HALO, from_right, 0.0))
        return (middle, side)

    def grid(c):
        return field(INPUT_FIELDS + c)

    def pairs(f, *operands):
        return tuple(f(*parts) for parts in zip(*operands))

    def below_of(v):
        return pairs(lambda x: pltpu.roll(x, tall - 1, 0), v)

    def above_of(v):
        return pairs(lambda x: pltpu.roll(x, 1, 0), v)

    def right_of(v):
        a, b = (pltpu.roll(x, LANES - 1, 1) for x in v)
        end = lane == LANES - 1
        return (jnp.where(end, b, a), jnp.where(end, a, b))

    def left_of(v):
        a, b = (pltpu.roll(x, 1, 1) for x in v)
        end = lane == 0
        return (jnp.where(end, b, a), jnp.where(end, a, b))

    bond_x, bond_y = field(7), field(8)
    low_x, low_y = above_of(bond_x), left_of(bond_y)
    scale = pairs(lambda a, b, c, d, e: a + b + c + d + e, bond_x, low_x, bond_y, low_y, field(6))

    def neighbours(v):
        return pairs(
            lambda bx, vb, lx, va, by, vr, ly, vl: bx * vb + lx * va + by * vr + ly * vl,
            bond_x, below_of(v), low_x, above_of(v), bond_y, right_of(v), low_y, left_of(v),
        )

    load = load_ref[0]
    sources = []
    for c in range(3):
        jump = field(c)
        external = field(3 + c)
        residual = pairs(
            lambda s, j, n, t, e: s * j - n + t - load * e, scale, jump, neighbours(jump), grid(c), external
        )
        sources.append((pairs(lambda r: -r, residual), external))

    def inverse_of(s, t00, t11, t22, t01, t02, t12, ok):
        d00, d11, d22 = s + t00, s + t11, s + t22
        c00 = d11 * d22 - t12 * t12
        c11 = d00 * d22 - t02 * t02
        c22 = d00 * d11 - t01 * t01
        c01 = t02 * t12 - t01 * d22
        c02 = t01 * t12 - t02 * d11
        c12 = t01 * t02 - d00 * t12
        determinant = d00 * c00 + t01 * c01 + t02 * c02
        over = jnp.where(ok, 1.0 / jnp.where(ok, determinant, 1.0), 0.0)
        return tuple(c * over for c in (c00, c11, c22, c01, c02, c12))

    both = pairs(inverse_of, scale, *(grid(3 + k) for k in range(6)), valid)
    i00, i11, i22, i01, i02, i12 = (tuple(both[t][k] for t in range(2)) for k in range(6))

    def dot3(a, x, b, y, c, z):
        return pairs(lambda a, x, b, y, c, z: a * x + b * y + c * z, a, x, b, y, c, z)

    def solve(w):
        return [
            dot3(i00, w[0], i01, w[1], i02, w[2]),
            dot3(i01, w[0], i11, w[1], i12, w[2]),
            dot3(i02, w[0], i12, w[1], i22, w[2]),
        ]

    done = []
    for half in range(2):
        source = [sources[c][half] for c in range(3)]
        iterate = solve(source)
        for _ in range(SWEEPS):
            iterate = solve([pairs(jnp.add, source[c], neighbours(iterate[c])) for c in range(3)])
        done.append([iterate[c][0][:rows] for c in range(3)])
    cross = square = 0.0
    for c in range(3):
        moved_ref[c] = field_ref[c] + done[0][c]
        moved_ref[3 + c] = done[1][c]
        cross = cross + done[0][c] * done[1][c]
        square = square + done[1][c] * done[1][c]
    half = iota((1, 1, LANES), 2) < LANES // 2
    sums_ref[...] = jnp.broadcast_to(jnp.where(half, jnp.sum(cross), jnp.sum(square)), sums_ref.shape)
    copy = pltpu.make_async_copy(sums_ref, packed_out.at[:, :, packed_out.shape[2] - LANES :], sem)
    copy.start()
    copy.wait()


def last_kernel(
    entries, plan_ref, load_ref, radius_ref, arrived_ref, moved_ref,
    new_jump_ref, new_load_ref, new_state_ref, new_history_ref,
):
    new_cap, cells = new_state_ref.shape
    whole = 0.5 * jnp.sum(arrived_ref[:, 0, 2 * cells :], axis=0, keepdims=True)
    half = iota(whole.shape, 1) < LANES // 2
    other = pltpu.roll(whole, LANES // 2, 1)
    cross, square = jnp.where(half, whole, other), jnp.where(half, other, whole)
    shifted = square + 0.25 * entries
    increment = (radius_ref[0] * (entries**0.5) * jnp.sqrt(shifted) - cross) / shifted
    for c in range(3):
        new_jump_ref[c] = moved_ref[c] + increment * moved_ref[3 + c]
    new_load_ref[0] = load_ref[0] + jnp.max(increment)
    group = 8

    def one(block, carry):
        at = pl.multiple_of(block * group, group)
        for k in range(group):
            index = plan_ref[0, at + k]
            valid = index >= 0
            source = jnp.maximum(index, 0)
            state = arrived_ref[pl.ds(source, 1), 0, :cells]
            history = arrived_ref[pl.ds(source, 1), 0, cells : 2 * cells]
            new_state_ref[pl.ds(at + k, 1), :] = jnp.where(valid, state, 0.0)
            new_history_ref[pl.ds(at + k, 1), :] = jnp.where(valid, jnp.maximum(history, jnp.abs(state)), 0.0)
        return carry

    lax.fori_loop(0, new_cap // group, one, 0)


LONG = pl.CostEstimate(flops=10_000_000_000, transcendentals=0, bytes_accessed=60_000_000)


def shape(*dims, dtype=F32):
    return jax.ShapeDtypeStruct(dims, dtype)


def call(kernel, outs, ins, out_specs, mib, scratch=(), cost=None, aliases=None):
    return pl.pallas_call(
        kernel,
        out_shape=outs,
        in_specs=ins,
        out_specs=out_specs,
        scratch_shapes=scratch,
        cost_estimate=cost,
        input_output_aliases=aliases or {},
        compiler_params=pltpu.CompilerParams(vmem_limit_bytes=mib * 1024 * 1024),
    )


def swap(first, last, axis):
    size = lax.axis_size(axis)
    up = [(i, i + 1) for i in range(size - 1)]
    down = [(i + 1, i) for i in range(size - 1)]
    above = lax.ppermute(last, axis, up)
    below = lax.ppermute(first, axis, down)
    return below, above


def on_device(
    jump, external, cohesive, bond_mask, load_factor, arc_radius, stiffness, coupling,
    old_state, old_history, newton_steps, point_ids,
):
    n_row, n_col = lax.axis_size("row"), lax.axis_size("col")
    devices = n_row * n_col
    row_at, col_at = lax.axis_index("row"), lax.axis_index("col")
    here = (row_at * n_col + col_at).astype(jnp.int32)
    slots, cells = old_state.shape
    _, rows, lanes = jump.shape
    edge = HALO * FIELDS
    width = 2 * cells + LANES
    packed_shape = shape(2 * devices, 1, width)
    place = jnp.stack([row_at, col_at, n_row, n_col]).astype(jnp.int32)
    ids_row = point_ids.reshape(1, slots)
    steps_row = newton_steps.reshape(1, slots)

    mine = call(count_kernel, shape(devices, 1, LANES), [VMEM], VMEM, 2, cost=LONG)(steps_row)
    counts = lax.all_to_all(mine, ROWS_COLS, 0, 0, tiled=True).reshape(devices, LANES)
    state, grid = call(
        newton_kernel,
        (shape(slots, cells), shape(FIELDS - INPUT_FIELDS, rows, lanes)),
        [VMEM] * 7,
        (VMEM, VMEM),
        24,
        scratch=(
            pltpu.VMEM((slots, cells), F32),
            pltpu.VMEM((slots, cells), F32),
            pltpu.VMEM((1, cells), F32),
            pltpu.VMEM((2, slots, cells), BF16),
        ),
        cost=pl.CostEstimate(
            flops=2 * MAX_STEPS * slots * cells * cells,
            transcendentals=2 * MAX_STEPS * slots * cells,
            bytes_accessed=2 * cells * cells + 12 * slots * cells,
        ),
    )(ids_row, steps_row, jump, stiffness, coupling, old_state, old_history)
    fields, first, last = call(
        fields_kernel,
        (shape(FIELDS, rows, lanes), shape(edge, lanes), shape(edge, lanes)),
        [VMEM] * 7,
        (VMEM,) * 3,
        4,
    )(ids_row, steps_row, jump, external, cohesive, bond_mask, grid)
    below, above = swap(first, last, "row")
    packed, plan = call(
        pack_kernel,
        (packed_shape, shape(8, LANES, dtype=jnp.int32)),
        [SMEM, SMEM, VMEM, VMEM, VMEM],
        (VMEM, VMEM),
        12,
    )(here[None], newton_steps, counts, state, old_history)
    to_left, to_right = call(
        lane_edges_kernel, (shape(edge, lanes), shape(edge, lanes)), [VMEM] * 3, (VMEM, VMEM), 4
    )(fields, below, above)
    right, left = swap(to_left, to_right, "col")
    moved, packed = call(
        macro_kernel,
        (shape(6, rows, lanes), packed_shape),
        [SMEM, SMEM] + [VMEM] * 5 + [HBM],
        (VMEM, HBM),
        12,
        scratch=(pltpu.VMEM((2 * devices, 1, LANES), F32), pltpu.SemaphoreType.DMA),
        cost=pl.CostEstimate(flops=200_000_000, transcendentals=0, bytes_accessed=2_000_000),
        aliases={7: 1},
    )(place, load_factor, fields, below, above, left, right, packed)
    arrived = lax.all_to_all(packed.reshape(devices, 1, 2 * width), ROWS_COLS, 0, 0, tiled=True)
    arrived = arrived.reshape(2 * devices, 1, width)
    new_jump, new_load, new_state, new_history = call(
        functools.partial(last_kernel, 3.0 * rows * lanes * devices),
        (shape(3, rows, lanes), shape(1), shape(slots // 2, cells), shape(slots // 2, cells)),
        [SMEM, SMEM, SMEM, VMEM, VMEM],
        (VMEM, SMEM, VMEM, VMEM),
        12,
    )(plan, load_factor, arc_radius, arrived, moved)
    return (new_jump, new_load, new_state, new_history)


def solution(mesh):
    whole = P(None, "row", "col")
    slot_rows = P(ROWS_COLS, None)
    return jax.shard_map(
        on_device,
        mesh=mesh,
        in_specs=(
            whole, whole, P("row", "col"), whole, P(), P(), P(), P(),
            slot_rows, slot_rows, P(ROWS_COLS), P(ROWS_COLS),
        ),
        out_specs=(whole, P(), slot_rows, slot_rows),
        check_vma=False,
    )
```

```python
import functools

import jax
import jax.numpy as jnp
from jax import lax
from jax.experimental import pallas as pl
from jax.experimental.pallas import tpu as pltpu
from jax.sharding import PartitionSpec as P


MAX_STEPS = 9
SWEEPS = 3
HALO = 4
INPUT_FIELDS = 9
FIELDS = 18
EARLY = 1152
NEWTON_MIB = 52
LANES = 128
ROWS_COLS = ("row", "col")
VMEM = pl.BlockSpec(memory_space=pltpu.VMEM)
SMEM = pl.BlockSpec(memory_space=pltpu.SMEM)
HBM = pl.BlockSpec(memory_space=pltpu.HBM)
F32 = jnp.float32
BF16 = jnp.bfloat16


def iota(shape, dim):
    return lax.broadcasted_iota(jnp.int32, shape, dim)


def three_parts(x):
    high = x.astype(BF16)
    rest = x - high.astype(F32)
    middle = rest.astype(BF16)
    low = (rest - middle.astype(F32)).astype(BF16)
    return high, middle, low


def times_transposed(a, b):
    return lax.dot_general(a, b, (((1,), (1,)), ((), ())), preferred_element_type=F32)


def put_row_edges(field_ref, first_ref, last_ref):
    fields, rows, _ = field_ref.shape
    for c in range(fields):
        first_ref[HALO * c : HALO * (c + 1), :] = field_ref[c, :HALO, :]
        last_ref[HALO * c : HALO * (c + 1), :] = field_ref[c, rows - HALO :, :]


def with_row_halo(field, below, above, c):
    part = slice(HALO * c, HALO * (c + 1))
    return jnp.concatenate([field, below[part], above[part]], axis=0)


def count_kernel(steps_ref, out_ref):
    live = jnp.sum((steps_ref[...] > 0).astype(F32), axis=1, keepdims=True)
    out_ref[...] = jnp.broadcast_to(live[None], out_ref.shape)


def lane_edges_kernel(field_ref, below_ref, above_ref, to_left_ref, to_right_ref):
    below, above = below_ref[...], above_ref[...]
    fields, rows, lanes = field_ref.shape
    tall = rows + 2 * HALO
    group = iota((tall, lanes), 1) // HALO
    heads = tails = jnp.zeros((tall, lanes), F32)
    for c in range(fields):
        whole = with_row_halo(field_ref[c], below, above, c)
        heads = jnp.where(group == c, pltpu.roll(whole, HALO * c, 1) if c else whole, heads)
        tails = jnp.where(group == c, pltpu.roll(whole, HALO * (c + 1), 1), tails)
    fill = jnp.zeros((lanes - tall, lanes), F32)
    to_left_ref[...] = jnp.concatenate([heads, fill], axis=0).T[: HALO * fields]
    to_right_ref[...] = jnp.concatenate([tails, fill], axis=0).T[: HALO * fields]


def newton_kernel(
    ids_ref, steps_ref, jump_ref, stiffness_hbm, coupling_ref, old_state_hbm, history_hbm,
    state_ref, grid_ref,
    stiffness_ref, damage_ref, load_ref, diagonal_ref, rounded_ref, sems,
):
    width = 256
    cuts = [slice(t * width, (t + 1) * width) for t in range(stiffness_hbm.shape[1] // width)]
    copies = [
        pltpu.make_async_copy(stiffness_hbm.at[:, part], stiffness_ref.at[:, part], sems.at[t])
        for t, part in enumerate(cuts)
    ]
    get_history = pltpu.make_async_copy(history_hbm, damage_ref, sems.at[len(cuts)])
    get_state = pltpu.make_async_copy(old_state_hbm, state_ref, sems.at[len(cuts) + 1])
    for copy in (get_history, get_state, *copies):
        copy.start()
    slots, cells = state_ref.shape
    _, rows, lanes = jump_ref.shape
    wide = 2 * lanes
    fill = jnp.zeros((1, wide - slots), jnp.int32)
    ids_row = jnp.concatenate([ids_ref[...], fill], axis=1)
    steps_row = jnp.concatenate([steps_ref[...], fill], axis=1)
    own = iota((slots, wide), 0) == iota((slots, wide), 1)

    def column(values):
        return jnp.sum(jnp.where(own, values, 0.0), axis=1, keepdims=True)

    steps = column(steps_row.astype(F32))
    at_x = column((ids_row // lanes).astype(F32))
    at_y = column((ids_row % lanes).astype(F32))
    pick_x = (iota((slots, rows), 1).astype(F32) == at_x).astype(F32).astype(BF16)
    pick_y = iota((slots, lanes), 1).astype(F32) == at_y
    at_row = iota((rows, wide), 0) == ids_row // lanes
    at_lane = (iota((lanes, wide), 0) == ids_row % lanes).astype(F32).astype(BF16)
    drive = []
    for c in range(3):
        parts = three_parts(jump_ref[c])
        picked = [jnp.dot(pick_x, part, preferred_element_type=F32) for part in parts]
        whole = (picked[0] + picked[1]) + picked[2]
        drive.append(jnp.sum(jnp.where(pick_y, whole, 0.0), axis=1, keepdims=True))
    load_ref[...] = (
        drive[0] * coupling_ref[0:1, :] + drive[1] * coupling_ref[1:2, :] + drive[2] * coupling_ref[2:3, :]
    )
    get_history.wait()
    damage_ref[...] = jnp.exp(-damage_ref[...])
    get_state.wait()
    rounded_ref[0] = state_ref[...].astype(BF16)
    eye = iota((width, width), 0) == iota((width, width), 1)

    def advance(count, carry, waiting=False):
        now = count % 2 if waiting else lax.rem(count, 2)
        rounded = rounded_ref[now]
        moving = steps > jnp.asarray(count, jnp.int32).astype(F32)
        for t, part in enumerate(cuts):
            if waiting:
                copies[t].wait()
                block = stiffness_ref[part, part].astype(F32)
                diagonal_ref[:, part] = jnp.sum(jnp.where(eye, block, 0.0), axis=0, keepdims=True)
            force = jnp.dot(rounded, stiffness_ref[:, part], preferred_element_type=F32)
            current = state_ref[:, part]
            bent = jnp.tanh(current)
            damage = damage_ref[:, part]
            misfit = force + damage * bent - load_ref[:, part]
            slope = diagonal_ref[:, part] + damage * (1.0 - bent * bent)
            current = jnp.where(moving, current - misfit / slope, current)
            state_ref[:, part] = current
            rounded_ref[1 - now, :, part] = current.astype(BF16)
        return carry

    advance(0, 0, waiting=True)
    lax.fori_loop(1, MAX_STEPS, advance, 0)
    bent = jnp.tanh(state_ref[...])
    damage = damage_ref[...]
    pull = damage * bent
    weight = damage * (1.0 - bent * bent)
    c0, c1, c2 = (coupling_ref[k : k + 1, :] for k in range(3))
    sums = [jnp.sum(pull * c, axis=1, keepdims=True) for c in (c0, c1, c2)]
    sums += [
        jnp.sum(weight * c, axis=1, keepdims=True)
        for c in (c0 * c0, c1 * c1, c2 * c2, c0 * c1, c0 * c2, c1 * c2)
    ]
    lane = iota((slots, LANES), 1)
    table = jnp.zeros((slots, LANES), F32)
    for k, value in enumerate(sums):
        table = jnp.where(lane == k, value * (1.0 / cells), table)
    table = jnp.where(steps > 0.0, table, 0.0)
    table = jnp.concatenate([table, jnp.zeros((wide - slots, LANES), F32)], axis=0).T
    pieces = []
    for c in range(len(sums)):
        placed = jnp.where(at_row, table[c : c + 1, :], 0.0)
        pieces.extend(three_parts(placed))
    spread = times_transposed(jnp.concatenate(pieces, axis=0), at_lane)
    for c in range(len(sums)):
        at = 3 * c * rows
        grid_ref[c] = spread[at : at + rows] + spread[at + rows : at + 2 * rows] + spread[at + 2 * rows : at + 3 * rows]


def fields_kernel(
    ids_ref, steps_ref, jump_ref, external_ref, cohesive_ref, mask_ref, grid_ref, field_ref, first_ref, last_ref
):
    rows, lanes = cohesive_ref.shape
    slots = ids_ref.shape[1]
    ids = ids_ref[...]
    at_row = ((iota((rows, slots), 0) == ids // lanes) & (steps_ref[...] > 0)).astype(F32).astype(BF16)
    at_lane = (iota((lanes, slots), 0) == ids % lanes).astype(F32).astype(BF16)
    soft = times_transposed(at_row, at_lane)
    for c in range(3):
        field_ref[c] = jump_ref[c]
        field_ref[3 + c] = external_ref[c]
    field_ref[6] = (1.0 - soft) * cohesive_ref[...]
    field_ref[7] = 0.25 + 0.75 * mask_ref[0].astype(F32)
    field_ref[8] = 0.25 + 0.75 * mask_ref[1].astype(F32)
    for c in range(FIELDS - INPUT_FIELDS):
        field_ref[INPUT_FIELDS + c] = grid_ref[c]
    put_row_edges(field_ref, first_ref, last_ref)


def pack_rows(pieces, out_ref, steps_ref, start):
    slots, places = pieces[0][0].shape[0], out_ref.shape[0]
    unused = lax.rem(2 * (start // 2) + places - 2, places)
    group = 8

    def one(block, rank):
        at = pl.multiple_of(block * group, group)
        rows = [(ref[pl.ds(at, group), low:high], to) for ref, low, high, to in pieces]
        for k in range(group):
            alive = steps_ref[at + k] > 0
            place = jnp.where(alive, lax.rem(rank, places), unused)
            for values, to in rows:
                out_ref[pl.ds(place, 1), 0, to : to + values.shape[1]] = values[k : k + 1]
            rank = rank + alive.astype(jnp.int32)
        return rank

    lax.fori_loop(0, slots // group, one, start)


def pack_history_kernel(here_ref, steps_ref, counts_ref, history_ref, out_ref, plan_ref):
    devices = counts_ref.shape[0]
    here = here_ref[0]
    counts = counts_ref[...]
    before = (iota((devices, devices), 1) < iota((devices, devices), 0)).astype(F32).astype(BF16)
    starts = jnp.dot(before, counts.astype(BF16), preferred_element_type=F32)
    row = iota((devices, LANES), 0)
    start = jnp.sum(jnp.where(row < here, counts, 0.0)[:, 0:1]).astype(jnp.int32)
    total = jnp.sum(counts, axis=0, keepdims=True)
    slot = iota((1, LANES), 1)
    wanted = (2 * (here + devices * (slot // 2)) + slot % 2).astype(F32)
    source = jnp.sum(jnp.where(starts <= wanted, 1.0, 0.0), axis=0, keepdims=True) - 1.0
    index = jnp.where(wanted < total, 2.0 * source + (slot % 2).astype(F32), -1.0).astype(jnp.int32)
    line = iota(plan_ref.shape, 0)
    plan_ref[...] = jnp.where(line == 0, index, start)
    pack_rows([(history_ref, 0, EARLY, 0)], out_ref, steps_ref, start)


def pack_state_kernel(plan_ref, steps_ref, state_ref, history_ref, out_ref):
    cells = state_ref.shape[1]
    pieces = [(state_ref, 0, cells, 0)]
    if EARLY < cells:
        pieces.append((history_ref, EARLY, cells, cells))
    pack_rows(pieces, out_ref, steps_ref, plan_ref[1, 0])


def macro_kernel(
    place_ref, load_ref, field_ref, below_ref, above_ref, left_ref, right_ref, packed_hbm,
    moved_ref, packed_out, sums_ref, sem,
):
    del packed_hbm
    rows = field_ref.shape[1]
    tall = rows + 2 * HALO
    lane = iota((tall, LANES), 1)
    line = iota((tall, LANES), 0)
    row_at, col_at = place_ref[0], place_ref[1]
    has_above = (row_at > 0).astype(jnp.int32)
    has_below = (row_at < place_ref[2] - 1).astype(jnp.int32)
    has_left = (col_at > 0).astype(jnp.int32)
    has_right = (col_at < place_ref[3] - 1).astype(jnp.int32)
    row_ok = jnp.where(line < rows, 1, jnp.where(line < rows + HALO, has_below, has_above)) > 0
    side_ok = jnp.where(lane < HALO, has_right, jnp.where(lane >= LANES - HALO, has_left, 0)) > 0
    valid = (row_ok, row_ok & side_ok)
    below, above = below_ref[...], above_ref[...]
    fill = jnp.zeros((LANES - left_ref.shape[0], LANES), F32)
    left = jnp.concatenate([left_ref[...], fill], axis=0).T[:tall]
    right = jnp.concatenate([right_ref[...], fill], axis=0).T[:tall]

    def field(c):
        middle = with_row_halo(field_ref[c], below, above, c)
        from_left = pltpu.roll(left, (LANES - HALO - HALO * c) % LANES, 1)
        from_right = pltpu.roll(right, (LANES - HALO * c) % LANES, 1) if c else right
        side = jnp.where(lane >= LANES - HALO, from_left, jnp.where(lane < HALO, from_right, 0.0))
        return (middle, side)

    def grid(c):
        return field(INPUT_FIELDS + c)

    def pairs(f, *operands):
        return tuple(f(*parts) for parts in zip(*operands))

    def below_of(v):
        return pairs(lambda x: pltpu.roll(x, tall - 1, 0), v)

    def above_of(v):
        return pairs(lambda x: pltpu.roll(x, 1, 0), v)

    def right_of(v):
        a, b = (pltpu.roll(x, LANES - 1, 1) for x in v)
        end = lane == LANES - 1
        return (jnp.where(end, b, a), jnp.where(end, a, b))

    def left_of(v):
        a, b = (pltpu.roll(x, 1, 1) for x in v)
        end = lane == 0
        return (jnp.where(end, b, a), jnp.where(end, a, b))

    bond_x, bond_y = field(7), field(8)
    low_x, low_y = above_of(bond_x), left_of(bond_y)
    scale = pairs(lambda a, b, c, d, e: a + b + c + d + e, bond_x, low_x, bond_y, low_y, field(6))

    def neighbours(v):
        return pairs(
            lambda bx, vb, lx, va, by, vr, ly, vl: bx * vb + lx * va + by * vr + ly * vl,
            bond_x, below_of(v), low_x, above_of(v), bond_y, right_of(v), low_y, left_of(v),
        )

    load = load_ref[0]
    sources = []
    for c in range(3):
        jump = field(c)
        external = field(3 + c)
        residual = pairs(
            lambda s, j, n, t, e: s * j - n + t - load * e, scale, jump, neighbours(jump), grid(c), external
        )
        sources.append((pairs(lambda r: -r, residual), external))

    def inverse_of(s, t00, t11, t22, t01, t02, t12, ok):
        d00, d11, d22 = s + t00, s + t11, s + t22
        c00 = d11 * d22 - t12 * t12
        c11 = d00 * d22 - t02 * t02
        c22 = d00 * d11 - t01 * t01
        c01 = t02 * t12 - t01 * d22
        c02 = t01 * t12 - t02 * d11
        c12 = t01 * t02 - d00 * t12
        determinant = d00 * c00 + t01 * c01 + t02 * c02
        over = jnp.where(ok, 1.0 / jnp.where(ok, determinant, 1.0), 0.0)
        return tuple(c * over for c in (c00, c11, c22, c01, c02, c12))

    both = pairs(inverse_of, scale, *(grid(3 + k) for k in range(6)), valid)
    i00, i11, i22, i01, i02, i12 = (tuple(both[t][k] for t in range(2)) for k in range(6))

    def dot3(a, x, b, y, c, z):
        return pairs(lambda a, x, b, y, c, z: a * x + b * y + c * z, a, x, b, y, c, z)

    def solve(w):
        return [
            dot3(i00, w[0], i01, w[1], i02, w[2]),
            dot3(i01, w[0], i11, w[1], i12, w[2]),
            dot3(i02, w[0], i12, w[1], i22, w[2]),
        ]

    done = []
    for half in range(2):
        source = [sources[c][half] for c in range(3)]
        iterate = solve(source)
        for _ in range(SWEEPS):
            iterate = solve([pairs(jnp.add, source[c], neighbours(iterate[c])) for c in range(3)])
        done.append([iterate[c][0][:rows] for c in range(3)])
    cross = square = 0.0
    for c in range(3):
        moved_ref[c] = field_ref[c] + done[0][c]
        moved_ref[3 + c] = done[1][c]
        cross = cross + done[0][c] * done[1][c]
        square = square + done[1][c] * done[1][c]
    half = iota((1, 1, LANES), 2) < LANES // 2
    sums_ref[...] = jnp.broadcast_to(jnp.where(half, jnp.sum(cross), jnp.sum(square)), sums_ref.shape)
    copy = pltpu.make_async_copy(sums_ref, packed_out.at[:, :, packed_out.shape[2] - LANES :], sem)
    copy.start()
    copy.wait()


def last_kernel(
    entries, plan_ref, load_ref, radius_ref, early_ref, arrived_ref, moved_ref,
    new_jump_ref, new_load_ref, new_state_ref, new_history_ref,
):
    new_cap, cells = new_state_ref.shape
    whole = 0.5 * jnp.sum(arrived_ref[:, 0, arrived_ref.shape[2] - LANES :], axis=0, keepdims=True)
    half = iota(whole.shape, 1) < LANES // 2
    other = pltpu.roll(whole, LANES // 2, 1)
    cross, square = jnp.where(half, whole, other), jnp.where(half, other, whole)
    shifted = square + 0.25 * entries
    increment = (radius_ref[0] * (entries**0.5) * jnp.sqrt(shifted) - cross) / shifted
    for c in range(3):
        new_jump_ref[c] = moved_ref[c] + increment * moved_ref[3 + c]
    new_load_ref[0] = load_ref[0] + jnp.max(increment)
    group = 8

    def one(block, carry):
        at = pl.multiple_of(block * group, group)
        for k in range(group):
            index = plan_ref[0, at + k]
            valid = index >= 0
            source = jnp.maximum(index, 0)
            state = arrived_ref[pl.ds(source, 1), 0, :cells]
            early = early_ref[pl.ds(source, 1), 0, :]
            new_state_ref[pl.ds(at + k, 1), :] = jnp.where(valid, state, 0.0)
            size = jnp.abs(state)
            new_history_ref[pl.ds(at + k, 1), :EARLY] = jnp.where(valid, jnp.maximum(early, size[:, :EARLY]), 0.0)
            if EARLY < cells:
                late = arrived_ref[pl.ds(source, 1), 0, cells : 2 * cells - EARLY]
                new_history_ref[pl.ds(at + k, 1), EARLY:] = jnp.where(valid, jnp.maximum(late, size[:, EARLY:]), 0.0)
        return carry

    lax.fori_loop(0, new_cap // group, one, 0)


LONG = pl.CostEstimate(flops=10_000_000_000, transcendentals=0, bytes_accessed=60_000_000)


def shape(*dims, dtype=F32):
    return jax.ShapeDtypeStruct(dims, dtype)


def call(kernel, outs, ins, out_specs, mib, scratch=(), cost=None, aliases=None):
    return pl.pallas_call(
        kernel,
        out_shape=outs,
        in_specs=ins,
        out_specs=out_specs,
        scratch_shapes=scratch,
        cost_estimate=cost,
        input_output_aliases=aliases or {},
        compiler_params=pltpu.CompilerParams(vmem_limit_bytes=mib * 1024 * 1024),
    )


def swap(first, last, axis):
    size = lax.axis_size(axis)
    up = [(i, i + 1) for i in range(size - 1)]
    down = [(i + 1, i) for i in range(size - 1)]
    above = lax.ppermute(last, axis, up)
    below = lax.ppermute(first, axis, down)
    return below, above


def on_device(
    jump, external, cohesive, bond_mask, load_factor, arc_radius, stiffness, coupling,
    old_state, old_history, newton_steps, point_ids,
):
    n_row, n_col = lax.axis_size("row"), lax.axis_size("col")
    devices = n_row * n_col
    row_at, col_at = lax.axis_index("row"), lax.axis_index("col")
    here = (row_at * n_col + col_at).astype(jnp.int32)
    slots, cells = old_state.shape
    _, rows, lanes = jump.shape
    edge = HALO * FIELDS
    width = 2 * cells - EARLY + LANES
    early_shape = shape(2 * devices, 1, EARLY)
    packed_shape = shape(2 * devices, 1, width)
    place = jnp.stack([row_at, col_at, n_row, n_col]).astype(jnp.int32)
    ids_row = point_ids.reshape(1, slots)
    steps_row = newton_steps.reshape(1, slots)

    mine = call(count_kernel, shape(devices, 1, LANES), [VMEM], VMEM, 2, cost=LONG)(steps_row)
    counts = lax.all_to_all(mine, ROWS_COLS, 0, 0, tiled=True).reshape(devices, LANES)
    early, plan = call(
        pack_history_kernel,
        (early_shape, shape(8, LANES, dtype=jnp.int32)),
        [SMEM, SMEM, VMEM, VMEM],
        (VMEM, VMEM),
        6,
    )(here[None], newton_steps, counts, old_history)
    early = lax.all_to_all(early.reshape(devices, 1, 2 * EARLY), ROWS_COLS, 0, 0, tiled=True)
    early = early.reshape(early_shape.shape)
    state, grid = call(
        newton_kernel,
        (shape(slots, cells), shape(FIELDS - INPUT_FIELDS, rows, lanes)),
        [VMEM] * 3 + [HBM, VMEM, HBM, HBM],
        (VMEM, VMEM),
        NEWTON_MIB,
        scratch=(
            pltpu.VMEM(stiffness.shape, BF16),
            pltpu.VMEM((slots, cells), F32),
            pltpu.VMEM((slots, cells), F32),
            pltpu.VMEM((1, cells), F32),
            pltpu.VMEM((2, slots, cells), BF16),
            pltpu.SemaphoreType.DMA((cells // 256 + 2,)),
        ),
        cost=pl.CostEstimate(
            flops=2 * MAX_STEPS * slots * cells * cells,
            transcendentals=2 * MAX_STEPS * slots * cells,
            bytes_accessed=2 * cells * cells + 12 * slots * cells,
        ),
    )(ids_row, steps_row, jump, stiffness, coupling, old_state, old_history)
    fields, first, last = call(
        fields_kernel,
        (shape(FIELDS, rows, lanes), shape(edge, lanes), shape(edge, lanes)),
        [VMEM] * 7,
        (VMEM,) * 3,
        4,
    )(ids_row, steps_row, jump, external, cohesive, bond_mask, grid)
    below, above = swap(first, last, "row")
    packed = call(pack_state_kernel, packed_shape, [SMEM, SMEM, VMEM, VMEM], VMEM, 8)(
        plan, newton_steps, state, old_history
    )
    to_left, to_right = call(
        lane_edges_kernel, (shape(edge, lanes), shape(edge, lanes)), [VMEM] * 3, (VMEM, VMEM), 4
    )(fields, below, above)
    right, left = swap(to_left, to_right, "col")
    moved, packed = call(
        macro_kernel,
        (shape(6, rows, lanes), packed_shape),
        [SMEM, SMEM] + [VMEM] * 5 + [HBM],
        (VMEM, HBM),
        12,
        scratch=(pltpu.VMEM((2 * devices, 1, LANES), F32), pltpu.SemaphoreType.DMA),
        cost=pl.CostEstimate(flops=200_000_000, transcendentals=0, bytes_accessed=2_000_000),
        aliases={7: 1},
    )(place, load_factor, fields, below, above, left, right, packed)
    arrived = lax.all_to_all(packed.reshape(devices, 1, 2 * width), ROWS_COLS, 0, 0, tiled=True)
    arrived = arrived.reshape(2 * devices, 1, width)
    new_jump, new_load, new_state, new_history = call(
        functools.partial(last_kernel, 3.0 * rows * lanes * devices),
        (shape(3, rows, lanes), shape(1), shape(slots // 2, cells), shape(slots // 2, cells)),
        [SMEM, SMEM, SMEM, VMEM, VMEM, VMEM],
        (VMEM, SMEM, VMEM, VMEM),
        12,
    )(plan, load_factor, arc_radius, early, arrived, moved)
    return (new_jump, new_load, new_state, new_history)


def solution(mesh):
    whole = P(None, "row", "col")
    slot_rows = P(ROWS_COLS, None)
    return jax.shard_map(
        on_device,
        mesh=mesh,
        in_specs=(
            whole, whole, P("row", "col"), whole, P(), P(), P(), P(),
            slot_rows, slot_rows, P(ROWS_COLS), P(ROWS_COLS),
        ),
        out_specs=(whole, P(), slot_rows, slot_rows),
        check_vma=False,
    )
```

```python
import functools

import jax
import jax.numpy as jnp
from jax import lax
from jax.experimental import pallas as pl
from jax.experimental.pallas import tpu as pltpu
from jax.sharding import PartitionSpec as P


MAX_STEPS = 9
SWEEPS = 3
HALO = 4
INPUT_FIELDS = 9
FIELDS = 18
NEWTON_MIB = 52
LANES = 128
ROWS_COLS = ("row", "col")
VMEM = pl.BlockSpec(memory_space=pltpu.VMEM)
SMEM = pl.BlockSpec(memory_space=pltpu.SMEM)
HBM = pl.BlockSpec(memory_space=pltpu.HBM)
F32 = jnp.float32
BF16 = jnp.bfloat16


def iota(shape, dim):
    return lax.broadcasted_iota(jnp.int32, shape, dim)


def three_parts(x):
    high = x.astype(BF16)
    rest = x - high.astype(F32)
    middle = rest.astype(BF16)
    low = (rest - middle.astype(F32)).astype(BF16)
    return high, middle, low


def times_transposed(a, b):
    return lax.dot_general(a, b, (((1,), (1,)), ((), ())), preferred_element_type=F32)


def put_row_edges(field_ref, first_ref, last_ref):
    fields, rows, _ = field_ref.shape
    for c in range(fields):
        first_ref[HALO * c : HALO * (c + 1), :] = field_ref[c, :HALO, :]
        last_ref[HALO * c : HALO * (c + 1), :] = field_ref[c, rows - HALO :, :]


def with_row_halo(field, below, above, c):
    part = slice(HALO * c, HALO * (c + 1))
    return jnp.concatenate([field, below[part], above[part]], axis=0)


def count_kernel(steps_ref, out_ref):
    live = jnp.sum((steps_ref[...] > 0).astype(F32), axis=1, keepdims=True)
    out_ref[...] = jnp.broadcast_to(live[None], out_ref.shape)


def lane_edges_kernel(field_ref, below_ref, above_ref, to_left_ref, to_right_ref):
    below, above = below_ref[...], above_ref[...]
    fields, rows, lanes = field_ref.shape
    tall = rows + 2 * HALO
    group = iota((tall, lanes), 1) // HALO
    heads = tails = jnp.zeros((tall, lanes), F32)
    for c in range(fields):
        whole = with_row_halo(field_ref[c], below, above, c)
        heads = jnp.where(group == c, pltpu.roll(whole, HALO * c, 1) if c else whole, heads)
        tails = jnp.where(group == c, pltpu.roll(whole, HALO * (c + 1), 1), tails)
    fill = jnp.zeros((lanes - tall, lanes), F32)
    to_left_ref[...] = jnp.concatenate([heads, fill], axis=0).T[: HALO * fields]
    to_right_ref[...] = jnp.concatenate([tails, fill], axis=0).T[: HALO * fields]


def newton_kernel(
    ids_ref, steps_ref, jump_ref, stiffness_hbm, coupling_ref, old_state_hbm, history_hbm,
    state_ref, grid_ref,
    stiffness_ref, damage_ref, load_ref, diagonal_ref, rounded_ref, sems,
):
    width = 256
    cuts = [slice(t * width, (t + 1) * width) for t in range(stiffness_hbm.shape[1] // width)]
    copies = [
        pltpu.make_async_copy(stiffness_hbm.at[:, part], stiffness_ref.at[:, part], sems.at[t])
        for t, part in enumerate(cuts)
    ]
    get_history = pltpu.make_async_copy(history_hbm, damage_ref, sems.at[len(cuts)])
    get_state = pltpu.make_async_copy(old_state_hbm, state_ref, sems.at[len(cuts) + 1])
    ahead = 3
    for copy in (get_history, get_state):
        copy.start()
    slots, cells = state_ref.shape
    _, rows, lanes = jump_ref.shape
    wide = 2 * lanes
    fill = jnp.zeros((1, wide - slots), jnp.int32)
    ids_row = jnp.concatenate([ids_ref[...], fill], axis=1)
    steps_row = jnp.concatenate([steps_ref[...], fill], axis=1)
    own = iota((slots, wide), 0) == iota((slots, wide), 1)

    def column(values):
        return jnp.sum(jnp.where(own, values, 0.0), axis=1, keepdims=True)

    steps = column(steps_row.astype(F32))
    at_x = column((ids_row // lanes).astype(F32))
    at_y = column((ids_row % lanes).astype(F32))
    pick_x = (iota((slots, rows), 1).astype(F32) == at_x).astype(F32).astype(BF16)
    pick_y = iota((slots, lanes), 1).astype(F32) == at_y
    at_row = iota((rows, wide), 0) == ids_row // lanes
    at_lane = (iota((lanes, wide), 0) == ids_row % lanes).astype(F32).astype(BF16)
    drive = []
    for c in range(3):
        parts = three_parts(jump_ref[c])
        picked = [jnp.dot(pick_x, part, preferred_element_type=F32) for part in parts]
        whole = (picked[0] + picked[1]) + picked[2]
        drive.append(jnp.sum(jnp.where(pick_y, whole, 0.0), axis=1, keepdims=True))
    load_ref[...] = (
        drive[0] * coupling_ref[0:1, :] + drive[1] * coupling_ref[1:2, :] + drive[2] * coupling_ref[2:3, :]
    )
    get_history.wait()
    for copy in copies[:ahead]:
        copy.start()
    damage_ref[...] = jnp.exp(-damage_ref[...])
    get_state.wait()
    rounded_ref[0] = state_ref[...].astype(BF16)
    eye = iota((width, width), 0) == iota((width, width), 1)

    def advance(count, carry, waiting=False):
        now = count % 2 if waiting else lax.rem(count, 2)
        rounded = rounded_ref[now]
        moving = steps > jnp.asarray(count, jnp.int32).astype(F32)
        for t, part in enumerate(cuts):
            if waiting:
                copies[t].wait()
                if t + ahead < len(copies):
                    copies[t + ahead].start()
                block = stiffness_ref[part, part].astype(F32)
                diagonal_ref[:, part] = jnp.sum(jnp.where(eye, block, 0.0), axis=0, keepdims=True)
            force = jnp.dot(rounded, stiffness_ref[:, part], preferred_element_type=F32)
            current = state_ref[:, part]
            bent = jnp.tanh(current)
            damage = damage_ref[:, part]
            misfit = force + damage * bent - load_ref[:, part]
            slope = diagonal_ref[:, part] + damage * (1.0 - bent * bent)
            current = jnp.where(moving, current - misfit / slope, current)
            state_ref[:, part] = current
            rounded_ref[1 - now, :, part] = current.astype(BF16)
        return carry

    advance(0, 0, waiting=True)
    lax.fori_loop(1, MAX_STEPS, advance, 0)
    bent = jnp.tanh(state_ref[...])
    damage = damage_ref[...]
    pull = damage * bent
    weight = damage * (1.0 - bent * bent)
    c0, c1, c2 = (coupling_ref[k : k + 1, :] for k in range(3))
    sums = [jnp.sum(pull * c, axis=1, keepdims=True) for c in (c0, c1, c2)]
    sums += [
        jnp.sum(weight * c, axis=1, keepdims=True)
        for c in (c0 * c0, c1 * c1, c2 * c2, c0 * c1, c0 * c2, c1 * c2)
    ]
    lane = iota((slots, LANES), 1)
    table = jnp.zeros((slots, LANES), F32)
    for k, value in enumerate(sums):
        table = jnp.where(lane == k, value * (1.0 / cells), table)
    table = jnp.where(steps > 0.0, table, 0.0)
    table = jnp.concatenate([table, jnp.zeros((wide - slots, LANES), F32)], axis=0).T
    pieces = []
    for c in range(len(sums)):
        placed = jnp.where(at_row, table[c : c + 1, :], 0.0)
        pieces.extend(three_parts(placed))
    spread = times_transposed(jnp.concatenate(pieces, axis=0), at_lane)
    for c in range(len(sums)):
        at = 3 * c * rows
        grid_ref[c] = spread[at : at + rows] + spread[at + rows : at + 2 * rows] + spread[at + 2 * rows : at + 3 * rows]


def fields_kernel(
    ids_ref, steps_ref, jump_ref, external_ref, cohesive_ref, mask_ref, grid_ref, field_ref, first_ref, last_ref
):
    rows, lanes = cohesive_ref.shape
    slots = ids_ref.shape[1]
    ids = ids_ref[...]
    at_row = ((iota((rows, slots), 0) == ids // lanes) & (steps_ref[...] > 0)).astype(F32).astype(BF16)
    at_lane = (iota((lanes, slots), 0) == ids % lanes).astype(F32).astype(BF16)
    soft = times_transposed(at_row, at_lane)
    for c in range(3):
        field_ref[c] = jump_ref[c]
        field_ref[3 + c] = external_ref[c]
    field_ref[6] = (1.0 - soft) * cohesive_ref[...]
    field_ref[7] = 0.25 + 0.75 * mask_ref[0].astype(F32)
    field_ref[8] = 0.25 + 0.75 * mask_ref[1].astype(F32)
    for c in range(FIELDS - INPUT_FIELDS):
        field_ref[INPUT_FIELDS + c] = grid_ref[c]
    put_row_edges(field_ref, first_ref, last_ref)


def pack_kernel(here_ref, steps_ref, counts_ref, state_ref, history_ref, out_ref, plan_ref):
    slots, cells = state_ref.shape
    devices = counts_ref.shape[0]
    here = here_ref[0]
    counts = counts_ref[...]
    before = (iota((devices, devices), 1) < iota((devices, devices), 0)).astype(F32).astype(BF16)
    starts = jnp.dot(before, counts.astype(BF16), preferred_element_type=F32)
    row = iota((devices, LANES), 0)
    start = jnp.sum(jnp.where(row < here, counts, 0.0)[:, 0:1]).astype(jnp.int32)
    total = jnp.sum(counts, axis=0, keepdims=True)
    slot = iota((1, LANES), 1)
    wanted = (2 * (here + devices * (slot // 2)) + slot % 2).astype(F32)
    source = jnp.sum(jnp.where(starts <= wanted, 1.0, 0.0), axis=0, keepdims=True) - 1.0
    index = jnp.where(wanted < total, 2.0 * source + (slot % 2).astype(F32), -1.0).astype(jnp.int32)
    plan_ref[...] = jnp.broadcast_to(index, plan_ref.shape)
    places = 2 * out_ref.shape[0]
    unused = lax.rem(2 * (start // 2) + places - 2, places)
    group = 8

    def one(block, rank):
        at = pl.multiple_of(block * group, group)
        state = state_ref[pl.ds(at, group), :]
        history = history_ref[pl.ds(at, group), :]
        for k in range(group):
            alive = steps_ref[at + k] > 0
            to = jnp.where(alive, lax.rem(rank, places), unused)
            at_lane = pl.multiple_of(lax.rem(to, 2) * (2 * cells), LANES)
            out_ref[pl.ds(to // 2, 1), 0, pl.ds(at_lane, cells)] = state[k : k + 1]
            out_ref[pl.ds(to // 2, 1), 0, pl.ds(at_lane + cells, cells)] = history[k : k + 1]
            rank = rank + alive.astype(jnp.int32)
        return rank

    lax.fori_loop(0, slots // group, one, start)


def macro_kernel(
    place_ref, load_ref, field_ref, below_ref, above_ref, left_ref, right_ref, packed_hbm,
    moved_ref, packed_out, sums_ref, sem,
):
    del packed_hbm
    rows = field_ref.shape[1]
    tall = rows + 2 * HALO
    lane = iota((tall, LANES), 1)
    line = iota((tall, LANES), 0)
    row_at, col_at = place_ref[0], place_ref[1]
    has_above = (row_at > 0).astype(jnp.int32)
    has_below = (row_at < place_ref[2] - 1).astype(jnp.int32)
    has_left = (col_at > 0).astype(jnp.int32)
    has_right = (col_at < place_ref[3] - 1).astype(jnp.int32)
    row_ok = jnp.where(line < rows, 1, jnp.where(line < rows + HALO, has_below, has_above)) > 0
    side_ok = jnp.where(lane < HALO, has_right, jnp.where(lane >= LANES - HALO, has_left, 0)) > 0
    valid = (row_ok, row_ok & side_ok)
    below, above = below_ref[...], above_ref[...]
    fill = jnp.zeros((LANES - left_ref.shape[0], LANES), F32)
    left = jnp.concatenate([left_ref[...], fill], axis=0).T[:tall]
    right = jnp.concatenate([right_ref[...], fill], axis=0).T[:tall]

    def field(c):
        middle = with_row_halo(field_ref[c], below, above, c)
        from_left = pltpu.roll(left, (LANES - HALO - HALO * c) % LANES, 1)
        from_right = pltpu.roll(right, (LANES - HALO * c) % LANES, 1) if c else right
        side = jnp.where(lane >= LANES - HALO, from_left, jnp.where(lane < HALO, from_right, 0.0))
        return (middle, side)

    def grid(c):
        return field(INPUT_FIELDS + c)

    def pairs(f, *operands):
        return tuple(f(*parts) for parts in zip(*operands))

    def below_of(v):
        return pairs(lambda x: pltpu.roll(x, tall - 1, 0), v)

    def above_of(v):
        return pairs(lambda x: pltpu.roll(x, 1, 0), v)

    def right_of(v):
        a, b = (pltpu.roll(x, LANES - 1, 1) for x in v)
        end = lane == LANES - 1
        return (jnp.where(end, b, a), jnp.where(end, a, b))

    def left_of(v):
        a, b = (pltpu.roll(x, 1, 1) for x in v)
        end = lane == 0
        return (jnp.where(end, b, a), jnp.where(end, a, b))

    bond_x, bond_y = field(7), field(8)
    low_x, low_y = above_of(bond_x), left_of(bond_y)
    scale = pairs(lambda a, b, c, d, e: a + b + c + d + e, bond_x, low_x, bond_y, low_y, field(6))

    def neighbours(v):
        return pairs(
            lambda bx, vb, lx, va, by, vr, ly, vl: bx * vb + lx * va + by * vr + ly * vl,
            bond_x, below_of(v), low_x, above_of(v), bond_y, right_of(v), low_y, left_of(v),
        )

    load = load_ref[0]
    sources = []
    for c in range(3):
        jump = field(c)
        external = field(3 + c)
        residual = pairs(
            lambda s, j, n, t, e: s * j - n + t - load * e, scale, jump, neighbours(jump), grid(c), external
        )
        sources.append((pairs(lambda r: -r, residual), external))

    def inverse_of(s, t00, t11, t22, t01, t02, t12, ok):
        d00, d11, d22 = s + t00, s + t11, s + t22
        c00 = d11 * d22 - t12 * t12
        c11 = d00 * d22 - t02 * t02
        c22 = d00 * d11 - t01 * t01
        c01 = t02 * t12 - t01 * d22
        c02 = t01 * t12 - t02 * d11
        c12 = t01 * t02 - d00 * t12
        determinant = d00 * c00 + t01 * c01 + t02 * c02
        over = jnp.where(ok, 1.0 / jnp.where(ok, determinant, 1.0), 0.0)
        return tuple(c * over for c in (c00, c11, c22, c01, c02, c12))

    both = pairs(inverse_of, scale, *(grid(3 + k) for k in range(6)), valid)
    i00, i11, i22, i01, i02, i12 = (tuple(both[t][k] for t in range(2)) for k in range(6))

    def dot3(a, x, b, y, c, z):
        return pairs(lambda a, x, b, y, c, z: a * x + b * y + c * z, a, x, b, y, c, z)

    def solve(w):
        return [
            dot3(i00, w[0], i01, w[1], i02, w[2]),
            dot3(i01, w[0], i11, w[1], i12, w[2]),
            dot3(i02, w[0], i12, w[1], i22, w[2]),
        ]

    done = []
    for half in range(2):
        source = [sources[c][half] for c in range(3)]
        iterate = solve(source)
        for _ in range(SWEEPS):
            iterate = solve([pairs(jnp.add, source[c], neighbours(iterate[c])) for c in range(3)])
        done.append([iterate[c][0][:rows] for c in range(3)])
    cross = square = 0.0
    for c in range(3):
        moved_ref[c] = field_ref[c] + done[0][c]
        moved_ref[3 + c] = done[1][c]
        cross = cross + done[0][c] * done[1][c]
        square = square + done[1][c] * done[1][c]
    half = iota((1, 1, LANES), 2) < LANES // 2
    sums_ref[...] = jnp.broadcast_to(jnp.where(half, jnp.sum(cross), jnp.sum(square)), sums_ref.shape)
    copy = pltpu.make_async_copy(sums_ref, packed_out.at[:, :, packed_out.shape[2] - LANES :], sem)
    copy.start()
    copy.wait()


def last_kernel(
    entries, plan_ref, load_ref, radius_ref, arrived_ref, moved_ref,
    new_jump_ref, new_load_ref, new_state_ref, new_history_ref,
):
    new_cap, cells = new_state_ref.shape
    whole = jnp.sum(arrived_ref[:, 0, 4 * cells :], axis=0, keepdims=True)
    half = iota(whole.shape, 1) < LANES // 2
    other = pltpu.roll(whole, LANES // 2, 1)
    cross, square = jnp.where(half, whole, other), jnp.where(half, other, whole)
    shifted = square + 0.25 * entries
    increment = (radius_ref[0] * (entries**0.5) * jnp.sqrt(shifted) - cross) / shifted
    for c in range(3):
        new_jump_ref[c] = moved_ref[c] + increment * moved_ref[3 + c]
    new_load_ref[0] = load_ref[0] + jnp.max(increment)
    group = 8

    def one(block, carry):
        at = pl.multiple_of(block * group, group)
        for k in range(group):
            index = plan_ref[0, at + k]
            valid = index >= 0
            source = jnp.maximum(index, 0)
            at_lane = pl.multiple_of(lax.rem(source, 2) * (2 * cells), LANES)
            state = arrived_ref[pl.ds(source // 2, 1), 0, pl.ds(at_lane, cells)]
            history = arrived_ref[pl.ds(source // 2, 1), 0, pl.ds(at_lane + cells, cells)]
            new_state_ref[pl.ds(at + k, 1), :] = jnp.where(valid, state, 0.0)
            new_history_ref[pl.ds(at + k, 1), :] = jnp.where(valid, jnp.maximum(history, jnp.abs(state)), 0.0)
        return carry

    lax.fori_loop(0, new_cap // group, one, 0)


LONG = pl.CostEstimate(flops=10_000_000_000, transcendentals=0, bytes_accessed=60_000_000)


def shape(*dims, dtype=F32):
    return jax.ShapeDtypeStruct(dims, dtype)


def call(kernel, outs, ins, out_specs, mib, scratch=(), cost=None, aliases=None):
    return pl.pallas_call(
        kernel,
        out_shape=outs,
        in_specs=ins,
        out_specs=out_specs,
        scratch_shapes=scratch,
        cost_estimate=cost,
        input_output_aliases=aliases or {},
        compiler_params=pltpu.CompilerParams(vmem_limit_bytes=mib * 1024 * 1024),
    )


def swap(first, last, axis):
    size = lax.axis_size(axis)
    up = [(i, i + 1) for i in range(size - 1)]
    down = [(i + 1, i) for i in range(size - 1)]
    above = lax.ppermute(last, axis, up)
    below = lax.ppermute(first, axis, down)
    return below, above


def on_device(
    jump, external, cohesive, bond_mask, load_factor, arc_radius, stiffness, coupling,
    old_state, old_history, newton_steps, point_ids,
):
    n_row, n_col = lax.axis_size("row"), lax.axis_size("col")
    devices = n_row * n_col
    row_at, col_at = lax.axis_index("row"), lax.axis_index("col")
    here = (row_at * n_col + col_at).astype(jnp.int32)
    slots, cells = old_state.shape
    _, rows, lanes = jump.shape
    edge = HALO * FIELDS
    packed_shape = shape(devices, 1, 4 * cells + LANES)
    place = jnp.stack([row_at, col_at, n_row, n_col]).astype(jnp.int32)
    ids_row = point_ids.reshape(1, slots)
    steps_row = newton_steps.reshape(1, slots)

    mine = call(count_kernel, shape(devices, 1, LANES), [VMEM], VMEM, 2, cost=LONG)(steps_row)
    counts = lax.all_to_all(mine, ROWS_COLS, 0, 0, tiled=True).reshape(devices, LANES)
    state, grid = call(
        newton_kernel,
        (shape(slots, cells), shape(FIELDS - INPUT_FIELDS, rows, lanes)),
        [VMEM] * 3 + [HBM, VMEM, HBM, HBM],
        (VMEM, VMEM),
        NEWTON_MIB,
        scratch=(
            pltpu.VMEM(stiffness.shape, BF16),
            pltpu.VMEM((slots, cells), F32),
            pltpu.VMEM((slots, cells), F32),
            pltpu.VMEM((1, cells), F32),
            pltpu.VMEM((2, slots, cells), BF16),
            pltpu.SemaphoreType.DMA((cells // 256 + 2,)),
        ),
        cost=pl.CostEstimate(
            flops=2 * MAX_STEPS * slots * cells * cells,
            transcendentals=2 * MAX_STEPS * slots * cells,
            bytes_accessed=2 * cells * cells + 12 * slots * cells,
        ),
    )(ids_row, steps_row, jump, stiffness, coupling, old_state, old_history)
    fields, first, last = call(
        fields_kernel,
        (shape(FIELDS, rows, lanes), shape(edge, lanes), shape(edge, lanes)),
        [VMEM] * 7,
        (VMEM,) * 3,
        4,
    )(ids_row, steps_row, jump, external, cohesive, bond_mask, grid)
    below, above = swap(first, last, "row")
    packed, plan = call(
        pack_kernel,
        (packed_shape, shape(8, LANES, dtype=jnp.int32)),
        [SMEM, SMEM, VMEM, VMEM, VMEM],
        (VMEM, VMEM),
        12,
    )(here[None], newton_steps, counts, state, old_history)
    to_left, to_right = call(
        lane_edges_kernel, (shape(edge, lanes), shape(edge, lanes)), [VMEM] * 3, (VMEM, VMEM), 4
    )(fields, below, above)
    right, left = swap(to_left, to_right, "col")
    moved, packed = call(
        macro_kernel,
        (shape(6, rows, lanes), packed_shape),
        [SMEM, SMEM] + [VMEM] * 5 + [HBM],
        (VMEM, HBM),
        12,
        scratch=(pltpu.VMEM((devices, 1, LANES), F32), pltpu.SemaphoreType.DMA),
        cost=pl.CostEstimate(flops=200_000_000, transcendentals=0, bytes_accessed=2_000_000),
        aliases={7: 1},
    )(place, load_factor, fields, below, above, left, right, packed)
    arrived = lax.all_to_all(packed, ROWS_COLS, 0, 0, tiled=True)
    new_jump, new_load, new_state, new_history = call(
        functools.partial(last_kernel, 3.0 * rows * lanes * devices),
        (shape(3, rows, lanes), shape(1), shape(slots // 2, cells), shape(slots // 2, cells)),
        [SMEM, SMEM, SMEM, VMEM, VMEM],
        (VMEM, SMEM, VMEM, VMEM),
        12,
    )(plan, load_factor, arc_radius, arrived, moved)
    return (new_jump, new_load, new_state, new_history)


def solution(mesh):
    whole = P(None, "row", "col")
    slot_rows = P(ROWS_COLS, None)
    return jax.shard_map(
        on_device,
        mesh=mesh,
        in_specs=(
            whole, whole, P("row", "col"), whole, P(), P(), P(), P(),
            slot_rows, slot_rows, P(ROWS_COLS), P(ROWS_COLS),
        ),
        out_specs=(whole, P(), slot_rows, slot_rows),
        check_vma=False,
    )
```

```python
import functools

import jax
import jax.numpy as jnp
from jax import lax
from jax.experimental import pallas as pl
from jax.experimental.pallas import tpu as pltpu
from jax.sharding import PartitionSpec as P


MAX_STEPS = 9
SWEEPS = 3
HALO = 4
INPUT_FIELDS = 9
FIELDS = 18
NEWTON_MIB = 52
LANES = 128
ROWS_COLS = ("row", "col")
VMEM = pl.BlockSpec(memory_space=pltpu.VMEM)
SMEM = pl.BlockSpec(memory_space=pltpu.SMEM)
HBM = pl.BlockSpec(memory_space=pltpu.HBM)
F32 = jnp.float32
BF16 = jnp.bfloat16


def iota(shape, dim):
    return lax.broadcasted_iota(jnp.int32, shape, dim)


def three_parts(x):
    high = x.astype(BF16)
    rest = x - high.astype(F32)
    middle = rest.astype(BF16)
    low = (rest - middle.astype(F32)).astype(BF16)
    return high, middle, low


def times_transposed(a, b):
    return lax.dot_general(a, b, (((1,), (1,)), ((), ())), preferred_element_type=F32)


def put_row_edges(field_ref, first_ref, last_ref):
    fields, rows, _ = field_ref.shape
    for c in range(fields):
        first_ref[HALO * c : HALO * (c + 1), :] = field_ref[c, :HALO, :]
        last_ref[HALO * c : HALO * (c + 1), :] = field_ref[c, rows - HALO :, :]


def with_row_halo(field, below, above, c):
    part = slice(HALO * c, HALO * (c + 1))
    return jnp.concatenate([field, below[part], above[part]], axis=0)


def count_kernel(steps_ref, out_ref):
    live = jnp.sum((steps_ref[...] > 0).astype(F32), axis=1, keepdims=True)
    out_ref[...] = jnp.broadcast_to(live[None], out_ref.shape)


def lane_edges_kernel(field_ref, below_ref, above_ref, to_left_ref, to_right_ref):
    below, above = below_ref[...], above_ref[...]
    fields, rows, lanes = field_ref.shape
    tall = rows + 2 * HALO
    group = iota((tall, lanes), 1) // HALO
    heads = tails = jnp.zeros((tall, lanes), F32)
    for c in range(fields):
        whole = with_row_halo(field_ref[c], below, above, c)
        heads = jnp.where(group == c, pltpu.roll(whole, HALO * c, 1) if c else whole, heads)
        tails = jnp.where(group == c, pltpu.roll(whole, HALO * (c + 1), 1), tails)
    fill = jnp.zeros((lanes - tall, lanes), F32)
    to_left_ref[...] = jnp.concatenate([heads, fill], axis=0).T[: HALO * fields]
    to_right_ref[...] = jnp.concatenate([tails, fill], axis=0).T[: HALO * fields]


def newton_kernel(
    ids_ref, steps_ref, jump_ref, stiffness_hbm, coupling_ref, old_state_hbm, history_hbm,
    state_ref, grid_ref,
    stiffness_ref, damage_ref, load_ref, diagonal_ref, rounded_ref, sems,
):
    width = 256
    cuts = [slice(t * width, (t + 1) * width) for t in range(stiffness_hbm.shape[1] // width)]
    copies = [
        pltpu.make_async_copy(stiffness_hbm.at[:, part], stiffness_ref.at[:, part], sems.at[t])
        for t, part in enumerate(cuts)
    ]
    get_history = pltpu.make_async_copy(history_hbm, damage_ref, sems.at[len(cuts)])
    get_state = pltpu.make_async_copy(old_state_hbm, state_ref, sems.at[len(cuts) + 1])
    for copy in (get_history, get_state):
        copy.start()
    slots, cells = state_ref.shape
    _, rows, lanes = jump_ref.shape
    wide = 2 * lanes
    fill = jnp.zeros((1, wide - slots), jnp.int32)
    ids_row = jnp.concatenate([ids_ref[...], fill], axis=1)
    steps_row = jnp.concatenate([steps_ref[...], fill], axis=1)
    own = iota((slots, wide), 0) == iota((slots, wide), 1)

    def column(values):
        return jnp.sum(jnp.where(own, values, 0.0), axis=1, keepdims=True)

    steps = column(steps_row.astype(F32))
    at_x = column((ids_row // lanes).astype(F32))
    at_y = column((ids_row % lanes).astype(F32))
    pick_x = (iota((slots, rows), 1).astype(F32) == at_x).astype(F32).astype(BF16)
    pick_y = iota((slots, lanes), 1).astype(F32) == at_y
    at_row = iota((rows, wide), 0) == ids_row // lanes
    at_lane = (iota((lanes, wide), 0) == ids_row % lanes).astype(F32).astype(BF16)
    drive = []
    for c in range(3):
        parts = three_parts(jump_ref[c])
        picked = [jnp.dot(pick_x, part, preferred_element_type=F32) for part in parts]
        whole = (picked[0] + picked[1]) + picked[2]
        drive.append(jnp.sum(jnp.where(pick_y, whole, 0.0), axis=1, keepdims=True))
    load_ref[...] = (
        drive[0] * coupling_ref[0:1, :] + drive[1] * coupling_ref[1:2, :] + drive[2] * coupling_ref[2:3, :]
    )
    for copy in copies:
        copy.start()
    get_history.wait()
    damage_ref[...] = jnp.exp(-damage_ref[...])
    get_state.wait()
    rounded_ref[0] = state_ref[...].astype(BF16)
    eye = iota((width, width), 0) == iota((width, width), 1)

    def advance(count, carry, waiting=False):
        now = count % 2 if waiting else lax.rem(count, 2)
        rounded = rounded_ref[now]
        moving = steps > jnp.asarray(count, jnp.int32).astype(F32)
        for t, part in enumerate(cuts):
            if waiting:
                copies[t].wait()
                block = stiffness_ref[part, part].astype(F32)
                diagonal_ref[:, part] = jnp.sum(jnp.where(eye, block, 0.0), axis=0, keepdims=True)
            force = jnp.dot(rounded, stiffness_ref[:, part], preferred_element_type=F32)
            current = state_ref[:, part]
            bent = jnp.tanh(current)
            damage = damage_ref[:, part]
            misfit = force + damage * bent - load_ref[:, part]
            slope = diagonal_ref[:, part] + damage * (1.0 - bent * bent)
            current = jnp.where(moving, current - misfit / slope, current)
            state_ref[:, part] = current
            rounded_ref[1 - now, :, part] = current.astype(BF16)
        return carry

    advance(0, 0, waiting=True)
    lax.fori_loop(1, MAX_STEPS, advance, 0)
    bent = jnp.tanh(state_ref[...])
    damage = damage_ref[...]
    pull = damage * bent
    weight = damage * (1.0 - bent * bent)
    c0, c1, c2 = (coupling_ref[k : k + 1, :] for k in range(3))
    sums = [jnp.sum(pull * c, axis=1, keepdims=True) for c in (c0, c1, c2)]
    sums += [
        jnp.sum(weight * c, axis=1, keepdims=True)
        for c in (c0 * c0, c1 * c1, c2 * c2, c0 * c1, c0 * c2, c1 * c2)
    ]
    lane = iota((slots, LANES), 1)
    table = jnp.zeros((slots, LANES), F32)
    for k, value in enumerate(sums):
        table = jnp.where(lane == k, value * (1.0 / cells), table)
    table = jnp.where(steps > 0.0, table, 0.0)
    table = jnp.concatenate([table, jnp.zeros((wide - slots, LANES), F32)], axis=0).T
    pieces = []
    for c in range(len(sums)):
        placed = jnp.where(at_row, table[c : c + 1, :], 0.0)
        pieces.extend(three_parts(placed))
    spread = times_transposed(jnp.concatenate(pieces, axis=0), at_lane)
    for c in range(len(sums)):
        at = 3 * c * rows
        grid_ref[c] = spread[at : at + rows] + spread[at + rows : at + 2 * rows] + spread[at + 2 * rows : at + 3 * rows]


def fields_kernel(
    ids_ref, steps_ref, jump_ref, external_ref, cohesive_ref, mask_ref, grid_ref, counts_ref,
    field_ref, first_ref, last_ref, line_ref,
):
    counts = counts_ref[:, 0, :]
    line = jnp.sum(jnp.where(iota(counts.shape, 0) == iota(counts.shape, 1), counts, 0.0), axis=0, keepdims=True)
    line_ref[...] = jnp.broadcast_to(line[None], line_ref.shape)
    rows, lanes = cohesive_ref.shape
    slots = ids_ref.shape[1]
    ids = ids_ref[...]
    at_row = ((iota((rows, slots), 0) == ids // lanes) & (steps_ref[...] > 0)).astype(F32).astype(BF16)
    at_lane = (iota((lanes, slots), 0) == ids % lanes).astype(F32).astype(BF16)
    soft = times_transposed(at_row, at_lane)
    for c in range(3):
        field_ref[c] = jump_ref[c]
        field_ref[3 + c] = external_ref[c]
    field_ref[6] = (1.0 - soft) * cohesive_ref[...]
    field_ref[7] = 0.25 + 0.75 * mask_ref[0].astype(F32)
    field_ref[8] = 0.25 + 0.75 * mask_ref[1].astype(F32)
    for c in range(FIELDS - INPUT_FIELDS):
        field_ref[INPUT_FIELDS + c] = grid_ref[c]
    put_row_edges(field_ref, first_ref, last_ref)


def pack_kernel(here_ref, steps_ref, counts_ref, state_ref, history_ref, out_ref, plan_ref):
    slots, cells = state_ref.shape
    devices = out_ref.shape[0]
    here = here_ref[0]
    lines = counts_ref[:, 0, :]
    n_row = lines.shape[0]
    n_col = devices // n_row
    pick = (iota((devices, n_row), 0) // n_col == iota((devices, n_row), 1)).astype(F32).astype(BF16)
    spread = jnp.dot(pick, lines.astype(BF16), preferred_element_type=F32)
    mine = iota(spread.shape, 0) % n_col == iota(spread.shape, 1)
    counts = jnp.broadcast_to(jnp.sum(jnp.where(mine, spread, 0.0), axis=1, keepdims=True), (devices, LANES))
    before = (iota((devices, devices), 1) < iota((devices, devices), 0)).astype(F32).astype(BF16)
    starts = jnp.dot(before, counts.astype(BF16), preferred_element_type=F32)
    row = iota((devices, LANES), 0)
    start = jnp.sum(jnp.where(row < here, counts, 0.0)[:, 0:1]).astype(jnp.int32)
    total = jnp.sum(counts, axis=0, keepdims=True)
    slot = iota((1, LANES), 1)
    wanted = (2 * (here + devices * (slot // 2)) + slot % 2).astype(F32)
    source = jnp.sum(jnp.where(starts <= wanted, 1.0, 0.0), axis=0, keepdims=True) - 1.0
    index = jnp.where(wanted < total, 2.0 * source + (slot % 2).astype(F32), -1.0).astype(jnp.int32)
    plan_ref[...] = jnp.broadcast_to(index, plan_ref.shape)
    places = 2 * out_ref.shape[0]
    unused = lax.rem(2 * (start // 2) + places - 2, places)
    group = 8

    def one(block, rank):
        at = pl.multiple_of(block * group, group)
        state = state_ref[pl.ds(at, group), :]
        history = history_ref[pl.ds(at, group), :]
        for k in range(group):
            alive = steps_ref[at + k] > 0
            to = jnp.where(alive, lax.rem(rank, places), unused)
            at_lane = pl.multiple_of(lax.rem(to, 2) * (2 * cells), LANES)
            out_ref[pl.ds(to // 2, 1), 0, pl.ds(at_lane, cells)] = state[k : k + 1]
            out_ref[pl.ds(to // 2, 1), 0, pl.ds(at_lane + cells, cells)] = history[k : k + 1]
            rank = rank + alive.astype(jnp.int32)
        return rank

    lax.fori_loop(0, slots // group, one, start)


def macro_kernel(
    place_ref, load_ref, field_ref, below_ref, above_ref, left_ref, right_ref, packed_hbm,
    moved_ref, packed_out, sums_ref, sem,
):
    del packed_hbm
    rows = field_ref.shape[1]
    tall = rows + 2 * HALO
    lane = iota((tall, LANES), 1)
    line = iota((tall, LANES), 0)
    row_at, col_at = place_ref[0], place_ref[1]
    has_above = (row_at > 0).astype(jnp.int32)
    has_below = (row_at < place_ref[2] - 1).astype(jnp.int32)
    has_left = (col_at > 0).astype(jnp.int32)
    has_right = (col_at < place_ref[3] - 1).astype(jnp.int32)
    row_ok = jnp.where(line < rows, 1, jnp.where(line < rows + HALO, has_below, has_above)) > 0
    side_ok = jnp.where(lane < HALO, has_right, jnp.where(lane >= LANES - HALO, has_left, 0)) > 0
    valid = (row_ok, row_ok & side_ok)
    below, above = below_ref[...], above_ref[...]
    fill = jnp.zeros((LANES - left_ref.shape[0], LANES), F32)
    left = jnp.concatenate([left_ref[...], fill], axis=0).T[:tall]
    right = jnp.concatenate([right_ref[...], fill], axis=0).T[:tall]

    def field(c):
        middle = with_row_halo(field_ref[c], below, above, c)
        from_left = pltpu.roll(left, (LANES - HALO - HALO * c) % LANES, 1)
        from_right = pltpu.roll(right, (LANES - HALO * c) % LANES, 1) if c else right
        side = jnp.where(lane >= LANES - HALO, from_left, jnp.where(lane < HALO, from_right, 0.0))
        return (middle, side)

    def grid(c):
        return field(INPUT_FIELDS + c)

    def pairs(f, *operands):
        return tuple(f(*parts) for parts in zip(*operands))

    def below_of(v):
        return pairs(lambda x: pltpu.roll(x, tall - 1, 0), v)

    def above_of(v):
        return pairs(lambda x: pltpu.roll(x, 1, 0), v)

    def right_of(v):
        a, b = (pltpu.roll(x, LANES - 1, 1) for x in v)
        end = lane == LANES - 1
        return (jnp.where(end, b, a), jnp.where(end, a, b))

    def left_of(v):
        a, b = (pltpu.roll(x, 1, 1) for x in v)
        end = lane == 0
        return (jnp.where(end, b, a), jnp.where(end, a, b))

    bond_x, bond_y = field(7), field(8)
    low_x, low_y = above_of(bond_x), left_of(bond_y)
    scale = pairs(lambda a, b, c, d, e: a + b + c + d + e, bond_x, low_x, bond_y, low_y, field(6))

    def neighbours(v):
        return pairs(
            lambda bx, vb, lx, va, by, vr, ly, vl: bx * vb + lx * va + by * vr + ly * vl,
            bond_x, below_of(v), low_x, above_of(v), bond_y, right_of(v), low_y, left_of(v),
        )

    load = load_ref[0]
    sources = []
    for c in range(3):
        jump = field(c)
        external = field(3 + c)
        residual = pairs(
            lambda s, j, n, t, e: s * j - n + t - load * e, scale, jump, neighbours(jump), grid(c), external
        )
        sources.append((pairs(lambda r: -r, residual), external))

    def inverse_of(s, t00, t11, t22, t01, t02, t12, ok):
        d00, d11, d22 = s + t00, s + t11, s + t22
        c00 = d11 * d22 - t12 * t12
        c11 = d00 * d22 - t02 * t02
        c22 = d00 * d11 - t01 * t01
        c01 = t02 * t12 - t01 * d22
        c02 = t01 * t12 - t02 * d11
        c12 = t01 * t02 - d00 * t12
        determinant = d00 * c00 + t01 * c01 + t02 * c02
        over = jnp.where(ok, 1.0 / jnp.where(ok, determinant, 1.0), 0.0)
        return tuple(c * over for c in (c00, c11, c22, c01, c02, c12))

    both = pairs(inverse_of, scale, *(grid(3 + k) for k in range(6)), valid)
    i00, i11, i22, i01, i02, i12 = (tuple(both[t][k] for t in range(2)) for k in range(6))

    def dot3(a, x, b, y, c, z):
        return pairs(lambda a, x, b, y, c, z: a * x + b * y + c * z, a, x, b, y, c, z)

    def solve(w):
        return [
            dot3(i00, w[0], i01, w[1], i02, w[2]),
            dot3(i01, w[0], i11, w[1], i12, w[2]),
            dot3(i02, w[0], i12, w[1], i22, w[2]),
        ]

    done = []
    for half in range(2):
        source = [sources[c][half] for c in range(3)]
        iterate = solve(source)
        for _ in range(SWEEPS):
            iterate = solve([pairs(jnp.add, source[c], neighbours(iterate[c])) for c in range(3)])
        done.append([iterate[c][0][:rows] for c in range(3)])
    cross = square = 0.0
    for c in range(3):
        moved_ref[c] = field_ref[c] + done[0][c]
        moved_ref[3 + c] = done[1][c]
        cross = cross + done[0][c] * done[1][c]
        square = square + done[1][c] * done[1][c]
    half = iota((1, 1, LANES), 2) < LANES // 2
    sums_ref[...] = jnp.broadcast_to(jnp.where(half, jnp.sum(cross), jnp.sum(square)), sums_ref.shape)
    copy = pltpu.make_async_copy(sums_ref, packed_out.at[:, :, packed_out.shape[2] - LANES :], sem)
    copy.start()
    copy.wait()


def last_kernel(
    entries, plan_ref, load_ref, radius_ref, arrived_ref, moved_ref,
    new_jump_ref, new_load_ref, new_state_ref, new_history_ref,
):
    new_cap, cells = new_state_ref.shape
    whole = jnp.sum(arrived_ref[:, 0, 4 * cells :], axis=0, keepdims=True)
    half = iota(whole.shape, 1) < LANES // 2
    other = pltpu.roll(whole, LANES // 2, 1)
    cross, square = jnp.where(half, whole, other), jnp.where(half, other, whole)
    shifted = square + 0.25 * entries
    increment = (radius_ref[0] * (entries**0.5) * jnp.sqrt(shifted) - cross) / shifted
    for c in range(3):
        new_jump_ref[c] = moved_ref[c] + increment * moved_ref[3 + c]
    new_load_ref[0] = load_ref[0] + jnp.max(increment)
    group = 8

    def one(block, carry):
        at = pl.multiple_of(block * group, group)
        for k in range(group):
            index = plan_ref[0, at + k]
            valid = index >= 0
            source = jnp.maximum(index, 0)
            at_lane = pl.multiple_of(lax.rem(source, 2) * (2 * cells), LANES)
            state = arrived_ref[pl.ds(source // 2, 1), 0, pl.ds(at_lane, cells)]
            history = arrived_ref[pl.ds(source // 2, 1), 0, pl.ds(at_lane + cells, cells)]
            new_state_ref[pl.ds(at + k, 1), :] = jnp.where(valid, state, 0.0)
            new_history_ref[pl.ds(at + k, 1), :] = jnp.where(valid, jnp.maximum(history, jnp.abs(state)), 0.0)
        return carry

    lax.fori_loop(0, new_cap // group, one, 0)


LONG = pl.CostEstimate(flops=10_000_000_000, transcendentals=0, bytes_accessed=60_000_000)


def shape(*dims, dtype=F32):
    return jax.ShapeDtypeStruct(dims, dtype)


def call(kernel, outs, ins, out_specs, mib, scratch=(), cost=None, aliases=None):
    return pl.pallas_call(
        kernel,
        out_shape=outs,
        in_specs=ins,
        out_specs=out_specs,
        scratch_shapes=scratch,
        cost_estimate=cost,
        input_output_aliases=aliases or {},
        compiler_params=pltpu.CompilerParams(vmem_limit_bytes=mib * 1024 * 1024),
    )


def swap(first, last, axis):
    size = lax.axis_size(axis)
    up = [(i, i + 1) for i in range(size - 1)]
    down = [(i + 1, i) for i in range(size - 1)]
    above = lax.ppermute(last, axis, up)
    below = lax.ppermute(first, axis, down)
    return below, above


def on_device(
    jump, external, cohesive, bond_mask, load_factor, arc_radius, stiffness, coupling,
    old_state, old_history, newton_steps, point_ids,
):
    n_row, n_col = lax.axis_size("row"), lax.axis_size("col")
    devices = n_row * n_col
    row_at, col_at = lax.axis_index("row"), lax.axis_index("col")
    here = (row_at * n_col + col_at).astype(jnp.int32)
    slots, cells = old_state.shape
    _, rows, lanes = jump.shape
    edge = HALO * FIELDS
    packed_shape = shape(devices, 1, 4 * cells + LANES)
    place = jnp.stack([row_at, col_at, n_row, n_col]).astype(jnp.int32)
    ids_row = point_ids.reshape(1, slots)
    steps_row = newton_steps.reshape(1, slots)

    mine = call(count_kernel, shape(n_col, 1, LANES), [VMEM], VMEM, 2, cost=LONG)(steps_row)
    counts = lax.all_to_all(mine, "col", 0, 0, tiled=True)
    state, grid = call(
        newton_kernel,
        (shape(slots, cells), shape(FIELDS - INPUT_FIELDS, rows, lanes)),
        [VMEM] * 3 + [HBM, VMEM, HBM, HBM],
        (VMEM, VMEM),
        NEWTON_MIB,
        scratch=(
            pltpu.VMEM(stiffness.shape, BF16),
            pltpu.VMEM((slots, cells), F32),
            pltpu.VMEM((slots, cells), F32),
            pltpu.VMEM((1, cells), F32),
            pltpu.VMEM((2, slots, cells), BF16),
            pltpu.SemaphoreType.DMA((cells // 256 + 2,)),
        ),
        cost=pl.CostEstimate(
            flops=2 * MAX_STEPS * slots * cells * cells,
            transcendentals=2 * MAX_STEPS * slots * cells,
            bytes_accessed=2 * cells * cells + 12 * slots * cells,
        ),
    )(ids_row, steps_row, jump, stiffness, coupling, old_state, old_history)
    fields, first, last, line = call(
        fields_kernel,
        (shape(FIELDS, rows, lanes), shape(edge, lanes), shape(edge, lanes), shape(n_row, 1, LANES)),
        [VMEM] * 8,
        (VMEM,) * 4,
        4,
    )(ids_row, steps_row, jump, external, cohesive, bond_mask, grid, counts)
    below, above = swap(first, last, "row")
    counts = lax.all_to_all(line, "row", 0, 0, tiled=True)
    packed, plan = call(
        pack_kernel,
        (packed_shape, shape(8, LANES, dtype=jnp.int32)),
        [SMEM, SMEM, VMEM, VMEM, VMEM],
        (VMEM, VMEM),
        12,
    )(here[None], newton_steps, counts, state, old_history)
    to_left, to_right = call(
        lane_edges_kernel, (shape(edge, lanes), shape(edge, lanes)), [VMEM] * 3, (VMEM, VMEM), 4
    )(fields, below, above)
    right, left = swap(to_left, to_right, "col")
    moved, packed = call(
        macro_kernel,
        (shape(6, rows, lanes), packed_shape),
        [SMEM, SMEM] + [VMEM] * 5 + [HBM],
        (VMEM, HBM),
        12,
        scratch=(pltpu.VMEM((devices, 1, LANES), F32), pltpu.SemaphoreType.DMA),
        cost=pl.CostEstimate(flops=200_000_000, transcendentals=0, bytes_accessed=2_000_000),
        aliases={7: 1},
    )(place, load_factor, fields, below, above, left, right, packed)
    arrived = lax.all_to_all(packed, ROWS_COLS, 0, 0, tiled=True)
    new_jump, new_load, new_state, new_history = call(
        functools.partial(last_kernel, 3.0 * rows * lanes * devices),
        (shape(3, rows, lanes), shape(1), shape(slots // 2, cells), shape(slots // 2, cells)),
        [SMEM, SMEM, SMEM, VMEM, VMEM],
        (VMEM, SMEM, VMEM, VMEM),
        12,
    )(plan, load_factor, arc_radius, arrived, moved)
    return (new_jump, new_load, new_state, new_history)


def solution(mesh):
    whole = P(None, "row", "col")
    slot_rows = P(ROWS_COLS, None)
    return jax.shard_map(
        on_device,
        mesh=mesh,
        in_specs=(
            whole, whole, P("row", "col"), whole, P(), P(), P(), P(),
            slot_rows, slot_rows, P(ROWS_COLS), P(ROWS_COLS),
        ),
        out_specs=(whole, P(), slot_rows, slot_rows),
        check_vma=False,
    )
```

```python
import functools

import jax
import jax.numpy as jnp
from jax import lax
from jax.experimental import pallas as pl
from jax.experimental.pallas import tpu as pltpu
from jax.sharding import PartitionSpec as P


MAX_STEPS = 9
SWEEPS = 3
HALO = 4
INPUT_FIELDS = 9
FIELDS = 18
NEWTON_MIB = 52
LANES = 128
ROWS_COLS = ("row", "col")
VMEM = pl.BlockSpec(memory_space=pltpu.VMEM)
SMEM = pl.BlockSpec(memory_space=pltpu.SMEM)
HBM = pl.BlockSpec(memory_space=pltpu.HBM)
F32 = jnp.float32
BF16 = jnp.bfloat16


def iota(shape, dim):
    return lax.broadcasted_iota(jnp.int32, shape, dim)


def three_parts(x):
    high = x.astype(BF16)
    rest = x - high.astype(F32)
    middle = rest.astype(BF16)
    low = (rest - middle.astype(F32)).astype(BF16)
    return high, middle, low


def times_transposed(a, b):
    return lax.dot_general(a, b, (((1,), (1,)), ((), ())), preferred_element_type=F32)


def put_row_edges(field_ref, first_ref, last_ref):
    fields, rows, _ = field_ref.shape
    for c in range(fields):
        first_ref[HALO * c : HALO * (c + 1), :] = field_ref[c, :HALO, :]
        last_ref[HALO * c : HALO * (c + 1), :] = field_ref[c, rows - HALO :, :]


def with_row_halo(field, below, above, c):
    part = slice(HALO * c, HALO * (c + 1))
    return jnp.concatenate([field, below[part], above[part]], axis=0)


def count_kernel(steps_ref, out_ref):
    live = jnp.sum((steps_ref[...] > 0).astype(F32), axis=1, keepdims=True)
    out_ref[...] = jnp.broadcast_to(live[None], out_ref.shape)


def lane_edges_kernel(field_ref, below_ref, above_ref, to_left_ref, to_right_ref):
    below, above = below_ref[...], above_ref[...]
    fields, rows, lanes = field_ref.shape
    tall = rows + 2 * HALO
    group = iota((tall, lanes), 1) // HALO
    heads = tails = jnp.zeros((tall, lanes), F32)
    for c in range(fields):
        whole = with_row_halo(field_ref[c], below, above, c)
        heads = jnp.where(group == c, pltpu.roll(whole, HALO * c, 1) if c else whole, heads)
        tails = jnp.where(group == c, pltpu.roll(whole, HALO * (c + 1), 1), tails)
    fill = jnp.zeros((lanes - tall, lanes), F32)
    to_left_ref[...] = jnp.concatenate([heads, fill], axis=0).T[: HALO * fields]
    to_right_ref[...] = jnp.concatenate([tails, fill], axis=0).T[: HALO * fields]


def newton_kernel(
    ids_ref, steps_ref, jump_ref, stiffness_hbm, coupling_ref, old_state_hbm, history_hbm, after_ref,
    state_ref, grid_ref,
    stiffness_ref, damage_ref, load_ref, diagonal_ref, rounded_ref, sems,
):
    del after_ref
    width = 256
    cuts = [slice(t * width, (t + 1) * width) for t in range(stiffness_hbm.shape[1] // width)]
    copies = [
        pltpu.make_async_copy(stiffness_hbm.at[:, part], stiffness_ref.at[:, part], sems.at[t])
        for t, part in enumerate(cuts)
    ]
    get_history = pltpu.make_async_copy(history_hbm, damage_ref, sems.at[len(cuts)])
    get_state = pltpu.make_async_copy(old_state_hbm, state_ref, sems.at[len(cuts) + 1])
    for copy in (get_history, get_state):
        copy.start()
    slots, cells = state_ref.shape
    _, rows, lanes = jump_ref.shape
    wide = 2 * lanes
    fill = jnp.zeros((1, wide - slots), jnp.int32)
    ids_row = jnp.concatenate([ids_ref[...], fill], axis=1)
    steps_row = jnp.concatenate([steps_ref[...], fill], axis=1)
    own = iota((slots, wide), 0) == iota((slots, wide), 1)

    def column(values):
        return jnp.sum(jnp.where(own, values, 0.0), axis=1, keepdims=True)

    steps = column(steps_row.astype(F32))
    at_x = column((ids_row // lanes).astype(F32))
    at_y = column((ids_row % lanes).astype(F32))
    pick_x = (iota((slots, rows), 1).astype(F32) == at_x).astype(F32).astype(BF16)
    pick_y = iota((slots, lanes), 1).astype(F32) == at_y
    at_row = iota((rows, wide), 0) == ids_row // lanes
    at_lane = (iota((lanes, wide), 0) == ids_row % lanes).astype(F32).astype(BF16)
    drive = []
    for c in range(3):
        parts = three_parts(jump_ref[c])
        picked = [jnp.dot(pick_x, part, preferred_element_type=F32) for part in parts]
        whole = (picked[0] + picked[1]) + picked[2]
        drive.append(jnp.sum(jnp.where(pick_y, whole, 0.0), axis=1, keepdims=True))
    load_ref[...] = (
        drive[0] * coupling_ref[0:1, :] + drive[1] * coupling_ref[1:2, :] + drive[2] * coupling_ref[2:3, :]
    )
    for copy in copies:
        copy.start()
    get_history.wait()
    damage_ref[...] = jnp.exp(-damage_ref[...])
    get_state.wait()
    rounded_ref[0] = state_ref[...].astype(BF16)
    eye = iota((width, width), 0) == iota((width, width), 1)

    def advance(count, carry, waiting=False):
        now = count % 2 if waiting else lax.rem(count, 2)
        rounded = rounded_ref[now]
        moving = steps > jnp.asarray(count, jnp.int32).astype(F32)
        for t, part in enumerate(cuts):
            if waiting:
                copies[t].wait()
                block = stiffness_ref[part, part].astype(F32)
                diagonal_ref[:, part] = jnp.sum(jnp.where(eye, block, 0.0), axis=0, keepdims=True)
            force = jnp.dot(rounded, stiffness_ref[:, part], preferred_element_type=F32)
            current = state_ref[:, part]
            bent = jnp.tanh(current)
            damage = damage_ref[:, part]
            misfit = force + damage * bent - load_ref[:, part]
            slope = diagonal_ref[:, part] + damage * (1.0 - bent * bent)
            current = jnp.where(moving, current - misfit / slope, current)
            state_ref[:, part] = current
            rounded_ref[1 - now, :, part] = current.astype(BF16)
        return carry

    advance(0, 0, waiting=True)
    lax.fori_loop(1, MAX_STEPS, advance, 0)
    bent = jnp.tanh(state_ref[...])
    damage = damage_ref[...]
    pull = damage * bent
    weight = damage * (1.0 - bent * bent)
    c0, c1, c2 = (coupling_ref[k : k + 1, :] for k in range(3))
    sums = [jnp.sum(pull * c, axis=1, keepdims=True) for c in (c0, c1, c2)]
    sums += [
        jnp.sum(weight * c, axis=1, keepdims=True)
        for c in (c0 * c0, c1 * c1, c2 * c2, c0 * c1, c0 * c2, c1 * c2)
    ]
    lane = iota((slots, LANES), 1)
    table = jnp.zeros((slots, LANES), F32)
    for k, value in enumerate(sums):
        table = jnp.where(lane == k, value * (1.0 / cells), table)
    table = jnp.where(steps > 0.0, table, 0.0)
    table = jnp.concatenate([table, jnp.zeros((wide - slots, LANES), F32)], axis=0).T
    pieces = []
    for c in range(len(sums)):
        placed = jnp.where(at_row, table[c : c + 1, :], 0.0)
        pieces.extend(three_parts(placed))
    spread = times_transposed(jnp.concatenate(pieces, axis=0), at_lane)
    for c in range(len(sums)):
        at = 3 * c * rows
        grid_ref[c] = spread[at : at + rows] + spread[at + rows : at + 2 * rows] + spread[at + 2 * rows : at + 3 * rows]


def fields_kernel(
    ids_ref, steps_ref, jump_ref, external_ref, cohesive_ref, mask_ref, grid_ref, field_ref, first_ref, last_ref
):
    rows, lanes = cohesive_ref.shape
    slots = ids_ref.shape[1]
    ids = ids_ref[...]
    at_row = ((iota((rows, slots), 0) == ids // lanes) & (steps_ref[...] > 0)).astype(F32).astype(BF16)
    at_lane = (iota((lanes, slots), 0) == ids % lanes).astype(F32).astype(BF16)
    soft = times_transposed(at_row, at_lane)
    for c in range(3):
        field_ref[c] = jump_ref[c]
        field_ref[3 + c] = external_ref[c]
    field_ref[6] = (1.0 - soft) * cohesive_ref[...]
    field_ref[7] = 0.25 + 0.75 * mask_ref[0].astype(F32)
    field_ref[8] = 0.25 + 0.75 * mask_ref[1].astype(F32)
    for c in range(FIELDS - INPUT_FIELDS):
        field_ref[INPUT_FIELDS + c] = grid_ref[c]
    put_row_edges(field_ref, first_ref, last_ref)


def pack_kernel(here_ref, steps_ref, counts_ref, state_ref, history_ref, out_ref, plan_ref):
    slots, cells = state_ref.shape
    devices = counts_ref.shape[0]
    here = here_ref[0]
    counts = counts_ref[...]
    before = (iota((devices, devices), 1) < iota((devices, devices), 0)).astype(F32).astype(BF16)
    starts = jnp.dot(before, counts.astype(BF16), preferred_element_type=F32)
    row = iota((devices, LANES), 0)
    start = jnp.sum(jnp.where(row < here, counts, 0.0)[:, 0:1]).astype(jnp.int32)
    total = jnp.sum(counts, axis=0, keepdims=True)
    slot = iota((1, LANES), 1)
    wanted = (2 * (here + devices * (slot // 2)) + slot % 2).astype(F32)
    source = jnp.sum(jnp.where(starts <= wanted, 1.0, 0.0), axis=0, keepdims=True) - 1.0
    index = jnp.where(wanted < total, 2.0 * source + (slot % 2).astype(F32), -1.0).astype(jnp.int32)
    plan_ref[...] = jnp.broadcast_to(index, plan_ref.shape)
    places = 2 * out_ref.shape[0]
    unused = lax.rem(2 * (start // 2) + places - 2, places)
    group = 8

    def one(block, rank):
        at = pl.multiple_of(block * group, group)
        state = state_ref[pl.ds(at, group), :]
        history = history_ref[pl.ds(at, group), :]
        for k in range(group):
            alive = steps_ref[at + k] > 0
            to = jnp.where(alive, lax.rem(rank, places), unused)
            at_lane = pl.multiple_of(lax.rem(to, 2) * (2 * cells), LANES)
            out_ref[pl.ds(to // 2, 1), 0, pl.ds(at_lane, cells)] = state[k : k + 1]
            out_ref[pl.ds(to // 2, 1), 0, pl.ds(at_lane + cells, cells)] = history[k : k + 1]
            rank = rank + alive.astype(jnp.int32)
        return rank

    lax.fori_loop(0, slots // group, one, start)


def macro_kernel(
    place_ref, load_ref, field_ref, below_ref, above_ref, left_ref, right_ref, packed_hbm,
    moved_ref, packed_out, sums_ref, sem,
):
    del packed_hbm
    rows = field_ref.shape[1]
    tall = rows + 2 * HALO
    lane = iota((tall, LANES), 1)
    line = iota((tall, LANES), 0)
    row_at, col_at = place_ref[0], place_ref[1]
    has_above = (row_at > 0).astype(jnp.int32)
    has_below = (row_at < place_ref[2] - 1).astype(jnp.int32)
    has_left = (col_at > 0).astype(jnp.int32)
    has_right = (col_at < place_ref[3] - 1).astype(jnp.int32)
    row_ok = jnp.where(line < rows, 1, jnp.where(line < rows + HALO, has_below, has_above)) > 0
    side_ok = jnp.where(lane < HALO, has_right, jnp.where(lane >= LANES - HALO, has_left, 0)) > 0
    valid = (row_ok, row_ok & side_ok)
    below, above = below_ref[...], above_ref[...]
    fill = jnp.zeros((LANES - left_ref.shape[0], LANES), F32)
    left = jnp.concatenate([left_ref[...], fill], axis=0).T[:tall]
    right = jnp.concatenate([right_ref[...], fill], axis=0).T[:tall]

    def field(c):
        middle = with_row_halo(field_ref[c], below, above, c)
        from_left = pltpu.roll(left, (LANES - HALO - HALO * c) % LANES, 1)
        from_right = pltpu.roll(right, (LANES - HALO * c) % LANES, 1) if c else right
        side = jnp.where(lane >= LANES - HALO, from_left, jnp.where(lane < HALO, from_right, 0.0))
        return (middle, side)

    def grid(c):
        return field(INPUT_FIELDS + c)

    def pairs(f, *operands):
        return tuple(f(*parts) for parts in zip(*operands))

    def below_of(v):
        return pairs(lambda x: pltpu.roll(x, tall - 1, 0), v)

    def above_of(v):
        return pairs(lambda x: pltpu.roll(x, 1, 0), v)

    def right_of(v):
        a, b = (pltpu.roll(x, LANES - 1, 1) for x in v)
        end = lane == LANES - 1
        return (jnp.where(end, b, a), jnp.where(end, a, b))

    def left_of(v):
        a, b = (pltpu.roll(x, 1, 1) for x in v)
        end = lane == 0
        return (jnp.where(end, b, a), jnp.where(end, a, b))

    bond_x, bond_y = field(7), field(8)
    low_x, low_y = above_of(bond_x), left_of(bond_y)
    scale = pairs(lambda a, b, c, d, e: a + b + c + d + e, bond_x, low_x, bond_y, low_y, field(6))

    def neighbours(v):
        return pairs(
            lambda bx, vb, lx, va, by, vr, ly, vl: bx * vb + lx * va + by * vr + ly * vl,
            bond_x, below_of(v), low_x, above_of(v), bond_y, right_of(v), low_y, left_of(v),
        )

    load = load_ref[0]
    sources = []
    for c in range(3):
        jump = field(c)
        external = field(3 + c)
        residual = pairs(
            lambda s, j, n, t, e: s * j - n + t - load * e, scale, jump, neighbours(jump), grid(c), external
        )
        sources.append((pairs(lambda r: -r, residual), external))

    def inverse_of(s, t00, t11, t22, t01, t02, t12, ok):
        d00, d11, d22 = s + t00, s + t11, s + t22
        c00 = d11 * d22 - t12 * t12
        c11 = d00 * d22 - t02 * t02
        c22 = d00 * d11 - t01 * t01
        c01 = t02 * t12 - t01 * d22
        c02 = t01 * t12 - t02 * d11
        c12 = t01 * t02 - d00 * t12
        determinant = d00 * c00 + t01 * c01 + t02 * c02
        over = jnp.where(ok, 1.0 / jnp.where(ok, determinant, 1.0), 0.0)
        return tuple(c * over for c in (c00, c11, c22, c01, c02, c12))

    both = pairs(inverse_of, scale, *(grid(3 + k) for k in range(6)), valid)
    i00, i11, i22, i01, i02, i12 = (tuple(both[t][k] for t in range(2)) for k in range(6))

    def dot3(a, x, b, y, c, z):
        return pairs(lambda a, x, b, y, c, z: a * x + b * y + c * z, a, x, b, y, c, z)

    def solve(w):
        return [
            dot3(i00, w[0], i01, w[1], i02, w[2]),
            dot3(i01, w[0], i11, w[1], i12, w[2]),
            dot3(i02, w[0], i12, w[1], i22, w[2]),
        ]

    done = []
    for half in range(2):
        source = [sources[c][half] for c in range(3)]
        iterate = solve(source)
        for _ in range(SWEEPS):
            iterate = solve([pairs(jnp.add, source[c], neighbours(iterate[c])) for c in range(3)])
        done.append([iterate[c][0][:rows] for c in range(3)])
    cross = square = 0.0
    for c in range(3):
        moved_ref[c] = field_ref[c] + done[0][c]
        moved_ref[3 + c] = done[1][c]
        cross = cross + done[0][c] * done[1][c]
        square = square + done[1][c] * done[1][c]
    half = iota((1, 1, LANES), 2) < LANES // 2
    sums_ref[...] = jnp.broadcast_to(jnp.where(half, jnp.sum(cross), jnp.sum(square)), sums_ref.shape)
    copy = pltpu.make_async_copy(sums_ref, packed_out.at[:, :, packed_out.shape[2] - LANES :], sem)
    copy.start()
    copy.wait()


def last_kernel(
    entries, plan_ref, load_ref, radius_ref, arrived_ref, moved_ref,
    new_jump_ref, new_load_ref, new_state_ref, new_history_ref,
):
    new_cap, cells = new_state_ref.shape
    whole = jnp.sum(arrived_ref[:, 0, 4 * cells :], axis=0, keepdims=True)
    half = iota(whole.shape, 1) < LANES // 2
    other = pltpu.roll(whole, LANES // 2, 1)
    cross, square = jnp.where(half, whole, other), jnp.where(half, other, whole)
    shifted = square + 0.25 * entries
    increment = (radius_ref[0] * (entries**0.5) * jnp.sqrt(shifted) - cross) / shifted
    for c in range(3):
        new_jump_ref[c] = moved_ref[c] + increment * moved_ref[3 + c]
    new_load_ref[0] = load_ref[0] + jnp.max(increment)
    group = 8

    def one(block, carry):
        at = pl.multiple_of(block * group, group)
        for k in range(group):
            index = plan_ref[0, at + k]
            valid = index >= 0
            source = jnp.maximum(index, 0)
            at_lane = pl.multiple_of(lax.rem(source, 2) * (2 * cells), LANES)
            state = arrived_ref[pl.ds(source // 2, 1), 0, pl.ds(at_lane, cells)]
            history = arrived_ref[pl.ds(source // 2, 1), 0, pl.ds(at_lane + cells, cells)]
            new_state_ref[pl.ds(at + k, 1), :] = jnp.where(valid, state, 0.0)
            new_history_ref[pl.ds(at + k, 1), :] = jnp.where(valid, jnp.maximum(history, jnp.abs(state)), 0.0)
        return carry

    lax.fori_loop(0, new_cap // group, one, 0)


LONG = pl.CostEstimate(flops=10_000_000_000, transcendentals=0, bytes_accessed=60_000_000)


def shape(*dims, dtype=F32):
    return jax.ShapeDtypeStruct(dims, dtype)


def call(kernel, outs, ins, out_specs, mib, scratch=(), cost=None, aliases=None):
    return pl.pallas_call(
        kernel,
        out_shape=outs,
        in_specs=ins,
        out_specs=out_specs,
        scratch_shapes=scratch,
        cost_estimate=cost,
        input_output_aliases=aliases or {},
        compiler_params=pltpu.CompilerParams(vmem_limit_bytes=mib * 1024 * 1024),
    )


def swap(first, last, axis):
    size = lax.axis_size(axis)
    up = [(i, i + 1) for i in range(size - 1)]
    down = [(i + 1, i) for i in range(size - 1)]
    above = lax.ppermute(last, axis, up)
    below = lax.ppermute(first, axis, down)
    return below, above


def on_device(
    jump, external, cohesive, bond_mask, load_factor, arc_radius, stiffness, coupling,
    old_state, old_history, newton_steps, point_ids,
):
    n_row, n_col = lax.axis_size("row"), lax.axis_size("col")
    devices = n_row * n_col
    row_at, col_at = lax.axis_index("row"), lax.axis_index("col")
    here = (row_at * n_col + col_at).astype(jnp.int32)
    slots, cells = old_state.shape
    _, rows, lanes = jump.shape
    edge = HALO * FIELDS
    packed_shape = shape(devices, 1, 4 * cells + LANES)
    place = jnp.stack([row_at, col_at, n_row, n_col]).astype(jnp.int32)
    ids_row = point_ids.reshape(1, slots)
    steps_row = newton_steps.reshape(1, slots)

    mine = call(count_kernel, shape(devices, 1, LANES), [VMEM], VMEM, 2, cost=LONG)(steps_row)
    state, grid = call(
        newton_kernel,
        (shape(slots, cells), shape(FIELDS - INPUT_FIELDS, rows, lanes)),
        [VMEM] * 3 + [HBM, VMEM, HBM, HBM, HBM],
        (VMEM, VMEM),
        NEWTON_MIB,
        scratch=(
            pltpu.VMEM(stiffness.shape, BF16),
            pltpu.VMEM((slots, cells), F32),
            pltpu.VMEM((slots, cells), F32),
            pltpu.VMEM((1, cells), F32),
            pltpu.VMEM((2, slots, cells), BF16),
            pltpu.SemaphoreType.DMA((cells // 256 + 2,)),
        ),
        cost=pl.CostEstimate(
            flops=2 * MAX_STEPS * slots * cells * cells,
            transcendentals=2 * MAX_STEPS * slots * cells,
            bytes_accessed=2 * cells * cells + 12 * slots * cells,
        ),
    )(ids_row, steps_row, jump, stiffness, coupling, old_state, old_history, mine)
    fields, first, last = call(
        fields_kernel,
        (shape(FIELDS, rows, lanes), shape(edge, lanes), shape(edge, lanes)),
        [VMEM] * 7,
        (VMEM,) * 3,
        4,
    )(ids_row, steps_row, jump, external, cohesive, bond_mask, grid)
    below, above = swap(first, last, "row")
    counts = lax.all_to_all(mine, ROWS_COLS, 0, 0, tiled=True).reshape(devices, LANES)
    packed, plan = call(
        pack_kernel,
        (packed_shape, shape(8, LANES, dtype=jnp.int32)),
        [SMEM, SMEM, VMEM, VMEM, VMEM],
        (VMEM, VMEM),
        12,
    )(here[None], newton_steps, counts, state, old_history)
    to_left, to_right = call(
        lane_edges_kernel, (shape(edge, lanes), shape(edge, lanes)), [VMEM] * 3, (VMEM, VMEM), 4
    )(fields, below, above)
    right, left = swap(to_left, to_right, "col")
    moved, packed = call(
        macro_kernel,
        (shape(6, rows, lanes), packed_shape),
        [SMEM, SMEM] + [VMEM] * 5 + [HBM],
        (VMEM, HBM),
        12,
        scratch=(pltpu.VMEM((devices, 1, LANES), F32), pltpu.SemaphoreType.DMA),
        cost=pl.CostEstimate(flops=200_000_000, transcendentals=0, bytes_accessed=2_000_000),
        aliases={7: 1},
    )(place, load_factor, fields, below, above, left, right, packed)
    arrived = lax.all_to_all(packed, ROWS_COLS, 0, 0, tiled=True)
    new_jump, new_load, new_state, new_history = call(
        functools.partial(last_kernel, 3.0 * rows * lanes * devices),
        (shape(3, rows, lanes), shape(1), shape(slots // 2, cells), shape(slots // 2, cells)),
        [SMEM, SMEM, SMEM, VMEM, VMEM],
        (VMEM, SMEM, VMEM, VMEM),
        12,
    )(plan, load_factor, arc_radius, arrived, moved)
    return (new_jump, new_load, new_state, new_history)


def solution(mesh):
    whole = P(None, "row", "col")
    slot_rows = P(ROWS_COLS, None)
    return jax.shard_map(
        on_device,
        mesh=mesh,
        in_specs=(
            whole, whole, P("row", "col"), whole, P(), P(), P(), P(),
            slot_rows, slot_rows, P(ROWS_COLS), P(ROWS_COLS),
        ),
        out_specs=(whole, P(), slot_rows, slot_rows),
        check_vma=False,
    )
```

```python
import functools

import jax
import jax.numpy as jnp
from jax import lax
from jax.experimental import pallas as pl
from jax.experimental.pallas import tpu as pltpu
from jax.sharding import PartitionSpec as P


MAX_STEPS = 9
SWEEPS = 3
HALO = 4
INPUT_FIELDS = 9
FIELDS = 18
NEWTON_MIB = 52
LANES = 128
ROWS_COLS = ("row", "col")
VMEM = pl.BlockSpec(memory_space=pltpu.VMEM)
SMEM = pl.BlockSpec(memory_space=pltpu.SMEM)
HBM = pl.BlockSpec(memory_space=pltpu.HBM)
F32 = jnp.float32
BF16 = jnp.bfloat16


def iota(shape, dim):
    return lax.broadcasted_iota(jnp.int32, shape, dim)


def three_parts(x):
    high = x.astype(BF16)
    rest = x - high.astype(F32)
    middle = rest.astype(BF16)
    low = (rest - middle.astype(F32)).astype(BF16)
    return high, middle, low


def times_transposed(a, b):
    return lax.dot_general(a, b, (((1,), (1,)), ((), ())), preferred_element_type=F32)


def put_row_edges(field_ref, first_ref, last_ref):
    fields, rows, _ = field_ref.shape
    for c in range(fields):
        first_ref[HALO * c : HALO * (c + 1), :] = field_ref[c, :HALO, :]
        last_ref[HALO * c : HALO * (c + 1), :] = field_ref[c, rows - HALO :, :]


def with_row_halo(field, below, above, c):
    part = slice(HALO * c, HALO * (c + 1))
    return jnp.concatenate([field, below[part], above[part]], axis=0)


def count_kernel(steps_ref, out_ref):
    live = jnp.sum((steps_ref[...] > 0).astype(F32), axis=1, keepdims=True)
    out_ref[...] = jnp.broadcast_to(live[None], out_ref.shape)


def lane_edges_kernel(field_ref, below_ref, above_ref, to_left_ref, to_right_ref):
    below, above = below_ref[...], above_ref[...]
    fields, rows, lanes = field_ref.shape
    tall = rows + 2 * HALO
    group = iota((tall, lanes), 1) // HALO
    heads = tails = jnp.zeros((tall, lanes), F32)
    for c in range(fields):
        whole = with_row_halo(field_ref[c], below, above, c)
        heads = jnp.where(group == c, pltpu.roll(whole, HALO * c, 1) if c else whole, heads)
        tails = jnp.where(group == c, pltpu.roll(whole, HALO * (c + 1), 1), tails)
    fill = jnp.zeros((lanes - tall, lanes), F32)
    to_left_ref[...] = jnp.concatenate([heads, fill], axis=0).T[: HALO * fields]
    to_right_ref[...] = jnp.concatenate([tails, fill], axis=0).T[: HALO * fields]


def newton_kernel(
    ids_ref, steps_ref, jump_ref, stiffness_hbm, coupling_ref, old_state_hbm, history_hbm, count_in,
    state_ref, grid_ref, count_out,
    stiffness_ref, damage_ref, load_ref, diagonal_ref, rounded_ref, sems,
):
    del count_in, count_out
    width = 256
    cuts = [slice(t * width, (t + 1) * width) for t in range(stiffness_hbm.shape[1] // width)]
    copies = [
        pltpu.make_async_copy(stiffness_hbm.at[:, part], stiffness_ref.at[:, part], sems.at[t])
        for t, part in enumerate(cuts)
    ]
    get_history = pltpu.make_async_copy(history_hbm, damage_ref, sems.at[len(cuts)])
    get_state = pltpu.make_async_copy(old_state_hbm, state_ref, sems.at[len(cuts) + 1])
    for copy in (get_history, get_state):
        copy.start()
    slots, cells = state_ref.shape
    _, rows, lanes = jump_ref.shape
    wide = 2 * lanes
    fill = jnp.zeros((1, wide - slots), jnp.int32)
    ids_row = jnp.concatenate([ids_ref[...], fill], axis=1)
    steps_row = jnp.concatenate([steps_ref[...], fill], axis=1)
    own = iota((slots, wide), 0) == iota((slots, wide), 1)

    def column(values):
        return jnp.sum(jnp.where(own, values, 0.0), axis=1, keepdims=True)

    steps = column(steps_row.astype(F32))
    at_x = column((ids_row // lanes).astype(F32))
    at_y = column((ids_row % lanes).astype(F32))
    pick_x = (iota((slots, rows), 1).astype(F32) == at_x).astype(F32).astype(BF16)
    pick_y = iota((slots, lanes), 1).astype(F32) == at_y
    at_row = iota((rows, wide), 0) == ids_row // lanes
    at_lane = (iota((lanes, wide), 0) == ids_row % lanes).astype(F32).astype(BF16)
    drive = []
    for c in range(3):
        parts = three_parts(jump_ref[c])
        picked = [jnp.dot(pick_x, part, preferred_element_type=F32) for part in parts]
        whole = (picked[0] + picked[1]) + picked[2]
        drive.append(jnp.sum(jnp.where(pick_y, whole, 0.0), axis=1, keepdims=True))
    load_ref[...] = (
        drive[0] * coupling_ref[0:1, :] + drive[1] * coupling_ref[1:2, :] + drive[2] * coupling_ref[2:3, :]
    )
    for copy in copies:
        copy.start()
    get_history.wait()
    damage_ref[...] = jnp.exp(-damage_ref[...])
    get_state.wait()
    rounded_ref[0] = state_ref[...].astype(BF16)
    eye = iota((width, width), 0) == iota((width, width), 1)

    def advance(count, carry, waiting=False):
        now = count % 2 if waiting else lax.rem(count, 2)
        rounded = rounded_ref[now]
        moving = steps > jnp.asarray(count, jnp.int32).astype(F32)
        for t, part in enumerate(cuts):
            if waiting:
                copies[t].wait()
                block = stiffness_ref[part, part].astype(F32)
                diagonal_ref[:, part] = jnp.sum(jnp.where(eye, block, 0.0), axis=0, keepdims=True)
            force = jnp.dot(rounded, stiffness_ref[:, part], preferred_element_type=F32)
            current = state_ref[:, part]
            bent = jnp.tanh(current)
            damage = damage_ref[:, part]
            misfit = force + damage * bent - load_ref[:, part]
            slope = diagonal_ref[:, part] + damage * (1.0 - bent * bent)
            current = jnp.where(moving, current - misfit / slope, current)
            state_ref[:, part] = current
            rounded_ref[1 - now, :, part] = current.astype(BF16)
        return carry

    advance(0, 0, waiting=True)
    lax.fori_loop(1, MAX_STEPS, advance, 0)
    bent = jnp.tanh(state_ref[...])
    damage = damage_ref[...]
    pull = damage * bent
    weight = damage * (1.0 - bent * bent)
    c0, c1, c2 = (coupling_ref[k : k + 1, :] for k in range(3))
    sums = [jnp.sum(pull * c, axis=1, keepdims=True) for c in (c0, c1, c2)]
    sums += [
        jnp.sum(weight * c, axis=1, keepdims=True)
        for c in (c0 * c0, c1 * c1, c2 * c2, c0 * c1, c0 * c2, c1 * c2)
    ]
    lane = iota((slots, LANES), 1)
    table = jnp.zeros((slots, LANES), F32)
    for k, value in enumerate(sums):
        table = jnp.where(lane == k, value * (1.0 / cells), table)
    table = jnp.where(steps > 0.0, table, 0.0)
    table = jnp.concatenate([table, jnp.zeros((wide - slots, LANES), F32)], axis=0).T
    pieces = []
    for c in range(len(sums)):
        placed = jnp.where(at_row, table[c : c + 1, :], 0.0)
        pieces.extend(three_parts(placed))
    spread = times_transposed(jnp.concatenate(pieces, axis=0), at_lane)
    for c in range(len(sums)):
        at = 3 * c * rows
        grid_ref[c] = spread[at : at + rows] + spread[at + rows : at + 2 * rows] + spread[at + 2 * rows : at + 3 * rows]


def fields_kernel(
    ids_ref, steps_ref, jump_ref, external_ref, cohesive_ref, mask_ref, grid_ref, field_ref, first_ref, last_ref
):
    rows, lanes = cohesive_ref.shape
    slots = ids_ref.shape[1]
    ids = ids_ref[...]
    at_row = ((iota((rows, slots), 0) == ids // lanes) & (steps_ref[...] > 0)).astype(F32).astype(BF16)
    at_lane = (iota((lanes, slots), 0) == ids % lanes).astype(F32).astype(BF16)
    soft = times_transposed(at_row, at_lane)
    for c in range(3):
        field_ref[c] = jump_ref[c]
        field_ref[3 + c] = external_ref[c]
    field_ref[6] = (1.0 - soft) * cohesive_ref[...]
    field_ref[7] = 0.25 + 0.75 * mask_ref[0].astype(F32)
    field_ref[8] = 0.25 + 0.75 * mask_ref[1].astype(F32)
    for c in range(FIELDS - INPUT_FIELDS):
        field_ref[INPUT_FIELDS + c] = grid_ref[c]
    put_row_edges(field_ref, first_ref, last_ref)


def pack_kernel(here_ref, steps_ref, counts_ref, state_ref, history_ref, out_ref, plan_ref):
    slots, cells = state_ref.shape
    devices = counts_ref.shape[0]
    here = here_ref[0]
    counts = counts_ref[...]
    before = (iota((devices, devices), 1) < iota((devices, devices), 0)).astype(F32).astype(BF16)
    starts = jnp.dot(before, counts.astype(BF16), preferred_element_type=F32)
    row = iota((devices, LANES), 0)
    start = jnp.sum(jnp.where(row < here, counts, 0.0)[:, 0:1]).astype(jnp.int32)
    total = jnp.sum(counts, axis=0, keepdims=True)
    slot = iota((1, LANES), 1)
    wanted = (2 * (here + devices * (slot // 2)) + slot % 2).astype(F32)
    source = jnp.sum(jnp.where(starts <= wanted, 1.0, 0.0), axis=0, keepdims=True) - 1.0
    index = jnp.where(wanted < total, 2.0 * source + (slot % 2).astype(F32), -1.0).astype(jnp.int32)
    plan_ref[...] = jnp.broadcast_to(index, plan_ref.shape)
    places = 2 * out_ref.shape[0]
    unused = lax.rem(2 * (start // 2) + places - 2, places)
    group = 8

    def one(block, rank):
        at = pl.multiple_of(block * group, group)
        state = state_ref[pl.ds(at, group), :]
        history = history_ref[pl.ds(at, group), :]
        for k in range(group):
            alive = steps_ref[at + k] > 0
            to = jnp.where(alive, lax.rem(rank, places), unused)
            at_lane = pl.multiple_of(lax.rem(to, 2) * (2 * cells), LANES)
            out_ref[pl.ds(to // 2, 1), 0, pl.ds(at_lane, cells)] = state[k : k + 1]
            out_ref[pl.ds(to // 2, 1), 0, pl.ds(at_lane + cells, cells)] = history[k : k + 1]
            rank = rank + alive.astype(jnp.int32)
        return rank

    lax.fori_loop(0, slots // group, one, start)


def macro_kernel(
    place_ref, load_ref, field_ref, below_ref, above_ref, left_ref, right_ref, packed_hbm,
    moved_ref, packed_out, sums_ref, sem,
):
    del packed_hbm
    rows = field_ref.shape[1]
    tall = rows + 2 * HALO
    lane = iota((tall, LANES), 1)
    line = iota((tall, LANES), 0)
    row_at, col_at = place_ref[0], place_ref[1]
    has_above = (row_at > 0).astype(jnp.int32)
    has_below = (row_at < place_ref[2] - 1).astype(jnp.int32)
    has_left = (col_at > 0).astype(jnp.int32)
    has_right = (col_at < place_ref[3] - 1).astype(jnp.int32)
    row_ok = jnp.where(line < rows, 1, jnp.where(line < rows + HALO, has_below, has_above)) > 0
    side_ok = jnp.where(lane < HALO, has_right, jnp.where(lane >= LANES - HALO, has_left, 0)) > 0
    valid = (row_ok, row_ok & side_ok)
    below, above = below_ref[...], above_ref[...]
    fill = jnp.zeros((LANES - left_ref.shape[0], LANES), F32)
    left = jnp.concatenate([left_ref[...], fill], axis=0).T[:tall]
    right = jnp.concatenate([right_ref[...], fill], axis=0).T[:tall]

    def field(c):
        middle = with_row_halo(field_ref[c], below, above, c)
        from_left = pltpu.roll(left, (LANES - HALO - HALO * c) % LANES, 1)
        from_right = pltpu.roll(right, (LANES - HALO * c) % LANES, 1) if c else right
        side = jnp.where(lane >= LANES - HALO, from_left, jnp.where(lane < HALO, from_right, 0.0))
        return (middle, side)

    def grid(c):
        return field(INPUT_FIELDS + c)

    def pairs(f, *operands):
        return tuple(f(*parts) for parts in zip(*operands))

    def below_of(v):
        return pairs(lambda x: pltpu.roll(x, tall - 1, 0), v)

    def above_of(v):
        return pairs(lambda x: pltpu.roll(x, 1, 0), v)

    def right_of(v):
        a, b = (pltpu.roll(x, LANES - 1, 1) for x in v)
        end = lane == LANES - 1
        return (jnp.where(end, b, a), jnp.where(end, a, b))

    def left_of(v):
        a, b = (pltpu.roll(x, 1, 1) for x in v)
        end = lane == 0
        return (jnp.where(end, b, a), jnp.where(end, a, b))

    bond_x, bond_y = field(7), field(8)
    low_x, low_y = above_of(bond_x), left_of(bond_y)
    scale = pairs(lambda a, b, c, d, e: a + b + c + d + e, bond_x, low_x, bond_y, low_y, field(6))

    def neighbours(v):
        return pairs(
            lambda bx, vb, lx, va, by, vr, ly, vl: bx * vb + lx * va + by * vr + ly * vl,
            bond_x, below_of(v), low_x, above_of(v), bond_y, right_of(v), low_y, left_of(v),
        )

    load = load_ref[0]
    sources = []
    for c in range(3):
        jump = field(c)
        external = field(3 + c)
        residual = pairs(
            lambda s, j, n, t, e: s * j - n + t - load * e, scale, jump, neighbours(jump), grid(c), external
        )
        sources.append((pairs(lambda r: -r, residual), external))

    def inverse_of(s, t00, t11, t22, t01, t02, t12, ok):
        d00, d11, d22 = s + t00, s + t11, s + t22
        c00 = d11 * d22 - t12 * t12
        c11 = d00 * d22 - t02 * t02
        c22 = d00 * d11 - t01 * t01
        c01 = t02 * t12 - t01 * d22
        c02 = t01 * t12 - t02 * d11
        c12 = t01 * t02 - d00 * t12
        determinant = d00 * c00 + t01 * c01 + t02 * c02
        over = jnp.where(ok, 1.0 / jnp.where(ok, determinant, 1.0), 0.0)
        return tuple(c * over for c in (c00, c11, c22, c01, c02, c12))

    both = pairs(inverse_of, scale, *(grid(3 + k) for k in range(6)), valid)
    i00, i11, i22, i01, i02, i12 = (tuple(both[t][k] for t in range(2)) for k in range(6))

    def dot3(a, x, b, y, c, z):
        return pairs(lambda a, x, b, y, c, z: a * x + b * y + c * z, a, x, b, y, c, z)

    def solve(w):
        return [
            dot3(i00, w[0], i01, w[1], i02, w[2]),
            dot3(i01, w[0], i11, w[1], i12, w[2]),
            dot3(i02, w[0], i12, w[1], i22, w[2]),
        ]

    done = []
    for half in range(2):
        source = [sources[c][half] for c in range(3)]
        iterate = solve(source)
        for _ in range(SWEEPS):
            iterate = solve([pairs(jnp.add, source[c], neighbours(iterate[c])) for c in range(3)])
        done.append([iterate[c][0][:rows] for c in range(3)])
    cross = square = 0.0
    for c in range(3):
        moved_ref[c] = field_ref[c] + done[0][c]
        moved_ref[3 + c] = done[1][c]
        cross = cross + done[0][c] * done[1][c]
        square = square + done[1][c] * done[1][c]
    half = iota((1, 1, LANES), 2) < LANES // 2
    sums_ref[...] = jnp.broadcast_to(jnp.where(half, jnp.sum(cross), jnp.sum(square)), sums_ref.shape)
    copy = pltpu.make_async_copy(sums_ref, packed_out.at[:, :, packed_out.shape[2] - LANES :], sem)
    copy.start()
    copy.wait()


def last_kernel(
    entries, plan_ref, load_ref, radius_ref, arrived_ref, moved_ref,
    new_jump_ref, new_load_ref, new_state_ref, new_history_ref,
):
    new_cap, cells = new_state_ref.shape
    whole = jnp.sum(arrived_ref[:, 0, 4 * cells :], axis=0, keepdims=True)
    half = iota(whole.shape, 1) < LANES // 2
    other = pltpu.roll(whole, LANES // 2, 1)
    cross, square = jnp.where(half, whole, other), jnp.where(half, other, whole)
    shifted = square + 0.25 * entries
    increment = (radius_ref[0] * (entries**0.5) * jnp.sqrt(shifted) - cross) / shifted
    for c in range(3):
        new_jump_ref[c] = moved_ref[c] + increment * moved_ref[3 + c]
    new_load_ref[0] = load_ref[0] + jnp.max(increment)
    group = 8

    def one(block, carry):
        at = pl.multiple_of(block * group, group)
        for k in range(group):
            index = plan_ref[0, at + k]
            valid = index >= 0
            source = jnp.maximum(index, 0)
            at_lane = pl.multiple_of(lax.rem(source, 2) * (2 * cells), LANES)
            state = arrived_ref[pl.ds(source // 2, 1), 0, pl.ds(at_lane, cells)]
            history = arrived_ref[pl.ds(source // 2, 1), 0, pl.ds(at_lane + cells, cells)]
            new_state_ref[pl.ds(at + k, 1), :] = jnp.where(valid, state, 0.0)
            new_history_ref[pl.ds(at + k, 1), :] = jnp.where(valid, jnp.maximum(history, jnp.abs(state)), 0.0)
        return carry

    lax.fori_loop(0, new_cap // group, one, 0)


LONG = pl.CostEstimate(flops=10_000_000_000, transcendentals=0, bytes_accessed=60_000_000)


def shape(*dims, dtype=F32):
    return jax.ShapeDtypeStruct(dims, dtype)


def call(kernel, outs, ins, out_specs, mib, scratch=(), cost=None, aliases=None):
    return pl.pallas_call(
        kernel,
        out_shape=outs,
        in_specs=ins,
        out_specs=out_specs,
        scratch_shapes=scratch,
        cost_estimate=cost,
        input_output_aliases=aliases or {},
        compiler_params=pltpu.CompilerParams(vmem_limit_bytes=mib * 1024 * 1024),
    )


def swap(first, last, axis):
    size = lax.axis_size(axis)
    up = [(i, i + 1) for i in range(size - 1)]
    down = [(i + 1, i) for i in range(size - 1)]
    above = lax.ppermute(last, axis, up)
    below = lax.ppermute(first, axis, down)
    return below, above


def on_device(
    jump, external, cohesive, bond_mask, load_factor, arc_radius, stiffness, coupling,
    old_state, old_history, newton_steps, point_ids,
):
    n_row, n_col = lax.axis_size("row"), lax.axis_size("col")
    devices = n_row * n_col
    row_at, col_at = lax.axis_index("row"), lax.axis_index("col")
    here = (row_at * n_col + col_at).astype(jnp.int32)
    slots, cells = old_state.shape
    _, rows, lanes = jump.shape
    edge = HALO * FIELDS
    packed_shape = shape(devices, 1, 4 * cells + LANES)
    place = jnp.stack([row_at, col_at, n_row, n_col]).astype(jnp.int32)
    ids_row = point_ids.reshape(1, slots)
    steps_row = newton_steps.reshape(1, slots)

    mine = call(count_kernel, shape(devices, 1, LANES), [VMEM], VMEM, 2, cost=LONG)(steps_row)
    state, grid, mine = call(
        newton_kernel,
        (shape(slots, cells), shape(FIELDS - INPUT_FIELDS, rows, lanes), shape(devices, 1, LANES)),
        [VMEM] * 3 + [HBM, VMEM, HBM, HBM, HBM],
        (VMEM, VMEM, HBM),
        NEWTON_MIB,
        scratch=(
            pltpu.VMEM(stiffness.shape, BF16),
            pltpu.VMEM((slots, cells), F32),
            pltpu.VMEM((slots, cells), F32),
            pltpu.VMEM((1, cells), F32),
            pltpu.VMEM((2, slots, cells), BF16),
            pltpu.SemaphoreType.DMA((cells // 256 + 2,)),
        ),
        cost=pl.CostEstimate(
            flops=2 * MAX_STEPS * slots * cells * cells,
            transcendentals=2 * MAX_STEPS * slots * cells,
            bytes_accessed=2 * cells * cells + 12 * slots * cells,
        ),
        aliases={7: 2},
    )(ids_row, steps_row, jump, stiffness, coupling, old_state, old_history, mine)
    fields, first, last = call(
        fields_kernel,
        (shape(FIELDS, rows, lanes), shape(edge, lanes), shape(edge, lanes)),
        [VMEM] * 7,
        (VMEM,) * 3,
        4,
    )(ids_row, steps_row, jump, external, cohesive, bond_mask, grid)
    below, above = swap(first, last, "row")
    counts = lax.all_to_all(mine, ROWS_COLS, 0, 0, tiled=True).reshape(devices, LANES)
    packed, plan = call(
        pack_kernel,
        (packed_shape, shape(8, LANES, dtype=jnp.int32)),
        [SMEM, SMEM, VMEM, VMEM, VMEM],
        (VMEM, VMEM),
        12,
    )(here[None], newton_steps, counts, state, old_history)
    to_left, to_right = call(
        lane_edges_kernel, (shape(edge, lanes), shape(edge, lanes)), [VMEM] * 3, (VMEM, VMEM), 4
    )(fields, below, above)
    right, left = swap(to_left, to_right, "col")
    moved, packed = call(
        macro_kernel,
        (shape(6, rows, lanes), packed_shape),
        [SMEM, SMEM] + [VMEM] * 5 + [HBM],
        (VMEM, HBM),
        12,
        scratch=(pltpu.VMEM((devices, 1, LANES), F32), pltpu.SemaphoreType.DMA),
        cost=pl.CostEstimate(flops=200_000_000, transcendentals=0, bytes_accessed=2_000_000),
        aliases={7: 1},
    )(place, load_factor, fields, below, above, left, right, packed)
    arrived = lax.all_to_all(packed, ROWS_COLS, 0, 0, tiled=True)
    new_jump, new_load, new_state, new_history = call(
        functools.partial(last_kernel, 3.0 * rows * lanes * devices),
        (shape(3, rows, lanes), shape(1), shape(slots // 2, cells), shape(slots // 2, cells)),
        [SMEM, SMEM, SMEM, VMEM, VMEM],
        (VMEM, SMEM, VMEM, VMEM),
        12,
    )(plan, load_factor, arc_radius, arrived, moved)
    return (new_jump, new_load, new_state, new_history)


def solution(mesh):
    whole = P(None, "row", "col")
    slot_rows = P(ROWS_COLS, None)
    return jax.shard_map(
        on_device,
        mesh=mesh,
        in_specs=(
            whole, whole, P("row", "col"), whole, P(), P(), P(), P(),
            slot_rows, slot_rows, P(ROWS_COLS), P(ROWS_COLS),
        ),
        out_specs=(whole, P(), slot_rows, slot_rows),
        check_vma=False,
    )
```

```python
import functools

import jax
import jax.numpy as jnp
from jax import lax
from jax.experimental import pallas as pl
from jax.experimental.pallas import tpu as pltpu
from jax.sharding import PartitionSpec as P


MAX_STEPS = 9
SWEEPS = 3
HALO = 4
INPUT_FIELDS = 9
FIELDS = 18
NEWTON_MIB = 52
LANES = 128
ROWS_COLS = ("row", "col")
VMEM = pl.BlockSpec(memory_space=pltpu.VMEM)
SMEM = pl.BlockSpec(memory_space=pltpu.SMEM)
HBM = pl.BlockSpec(memory_space=pltpu.HBM)
F32 = jnp.float32
BF16 = jnp.bfloat16


def iota(shape, dim):
    return lax.broadcasted_iota(jnp.int32, shape, dim)


def three_parts(x):
    high = x.astype(BF16)
    rest = x - high.astype(F32)
    middle = rest.astype(BF16)
    low = (rest - middle.astype(F32)).astype(BF16)
    return high, middle, low


def times_transposed(a, b):
    return lax.dot_general(a, b, (((1,), (1,)), ((), ())), preferred_element_type=F32)


def put_row_edges(field_ref, first_ref, last_ref):
    fields, rows, _ = field_ref.shape
    for c in range(fields):
        first_ref[HALO * c : HALO * (c + 1), :] = field_ref[c, :HALO, :]
        last_ref[HALO * c : HALO * (c + 1), :] = field_ref[c, rows - HALO :, :]


def with_row_halo(field, below, above, c):
    part = slice(HALO * c, HALO * (c + 1))
    return jnp.concatenate([field, below[part], above[part]], axis=0)


def count_kernel(steps_ref, out_ref):
    live = jnp.sum((steps_ref[...] > 0).astype(F32), axis=1, keepdims=True)
    out_ref[...] = jnp.broadcast_to(live[None], out_ref.shape)


def lane_edges_kernel(field_ref, below_ref, above_ref, to_left_ref, to_right_ref):
    below, above = below_ref[...], above_ref[...]
    fields, rows, lanes = field_ref.shape
    tall = rows + 2 * HALO
    group = iota((tall, lanes), 1) // HALO
    heads = tails = jnp.zeros((tall, lanes), F32)
    for c in range(fields):
        whole = with_row_halo(field_ref[c], below, above, c)
        heads = jnp.where(group == c, pltpu.roll(whole, HALO * c, 1) if c else whole, heads)
        tails = jnp.where(group == c, pltpu.roll(whole, HALO * (c + 1), 1), tails)
    fill = jnp.zeros((lanes - tall, lanes), F32)
    to_left_ref[...] = jnp.concatenate([heads, fill], axis=0).T[: HALO * fields]
    to_right_ref[...] = jnp.concatenate([tails, fill], axis=0).T[: HALO * fields]


def newton_kernel(
    ids_ref, steps_ref, jump_ref, stiffness_hbm, coupling_ref, old_state_hbm, history_hbm, after_ref,
    state_ref, grid_ref,
    stiffness_ref, damage_ref, load_ref, diagonal_ref, rounded_ref, sems,
):
    del after_ref
    width = 256
    cuts = [slice(t * width, (t + 1) * width) for t in range(stiffness_hbm.shape[1] // width)]
    copies = [
        pltpu.make_async_copy(stiffness_hbm.at[:, part], stiffness_ref.at[:, part], sems.at[t])
        for t, part in enumerate(cuts)
    ]
    get_history = pltpu.make_async_copy(history_hbm, damage_ref, sems.at[len(cuts)])
    get_state = pltpu.make_async_copy(old_state_hbm, state_ref, sems.at[len(cuts) + 1])
    for copy in (get_history, get_state):
        copy.start()
    slots, cells = state_ref.shape
    _, rows, lanes = jump_ref.shape
    wide = 2 * lanes
    fill = jnp.zeros((1, wide - slots), jnp.int32)
    ids_row = jnp.concatenate([ids_ref[...], fill], axis=1)
    steps_row = jnp.concatenate([steps_ref[...], fill], axis=1)
    own = iota((slots, wide), 0) == iota((slots, wide), 1)

    def column(values):
        return jnp.sum(jnp.where(own, values, 0.0), axis=1, keepdims=True)

    steps = column(steps_row.astype(F32))
    at_x = column((ids_row // lanes).astype(F32))
    at_y = column((ids_row % lanes).astype(F32))
    pick_x = (iota((slots, rows), 1).astype(F32) == at_x).astype(F32).astype(BF16)
    pick_y = iota((slots, lanes), 1).astype(F32) == at_y
    at_row = iota((rows, wide), 0) == ids_row // lanes
    at_lane = (iota((lanes, wide), 0) == ids_row % lanes).astype(F32).astype(BF16)
    drive = []
    for c in range(3):
        parts = three_parts(jump_ref[c])
        picked = [jnp.dot(pick_x, part, preferred_element_type=F32) for part in parts]
        whole = (picked[0] + picked[1]) + picked[2]
        drive.append(jnp.sum(jnp.where(pick_y, whole, 0.0), axis=1, keepdims=True))
    load_ref[...] = (
        drive[0] * coupling_ref[0:1, :] + drive[1] * coupling_ref[1:2, :] + drive[2] * coupling_ref[2:3, :]
    )
    for copy in copies:
        copy.start()
    get_history.wait()
    damage_ref[...] = jnp.exp(-damage_ref[...])
    get_state.wait()
    rounded_ref[0] = state_ref[...].astype(BF16)
    eye = iota((LANES, LANES), 0) == iota((LANES, LANES), 1)

    def advance(count, carry, waiting=False):
        now = count % 2 if waiting else lax.rem(count, 2)
        rounded = rounded_ref[now]
        moving = steps > jnp.asarray(count, jnp.int32).astype(F32)
        for t, part in enumerate(cuts):
            if waiting:
                copies[t].wait()
                for low in range(part.start, part.stop, LANES):
                    near = slice(low, low + LANES)
                    block = stiffness_ref[near, near].astype(F32)
                    diagonal_ref[:, near] = jnp.sum(jnp.where(eye, block, 0.0), axis=0, keepdims=True)
            force = jnp.dot(rounded, stiffness_ref[:, part], preferred_element_type=F32)
            current = state_ref[:, part]
            bent = jnp.tanh(current)
            damage = damage_ref[:, part]
            misfit = force + damage * bent - load_ref[:, part]
            slope = diagonal_ref[:, part] + damage * (1.0 - bent * bent)
            current = jnp.where(moving, current - misfit / slope, current)
            state_ref[:, part] = current
            rounded_ref[1 - now, :, part] = current.astype(BF16)
        return carry

    advance(0, 0, waiting=True)
    lax.fori_loop(1, MAX_STEPS, advance, 0)
    bent = jnp.tanh(state_ref[...])
    damage = damage_ref[...]
    pull = damage * bent
    weight = damage * (1.0 - bent * bent)
    c0, c1, c2 = (coupling_ref[k : k + 1, :] for k in range(3))
    sums = [jnp.sum(pull * c, axis=1, keepdims=True) for c in (c0, c1, c2)]
    sums += [
        jnp.sum(weight * c, axis=1, keepdims=True)
        for c in (c0 * c0, c1 * c1, c2 * c2, c0 * c1, c0 * c2, c1 * c2)
    ]
    lane = iota((slots, LANES), 1)
    table = jnp.zeros((slots, LANES), F32)
    for k, value in enumerate(sums):
        table = jnp.where(lane == k, value * (1.0 / cells), table)
    table = jnp.where(steps > 0.0, table, 0.0)
    table = jnp.concatenate([table, jnp.zeros((wide - slots, LANES), F32)], axis=0).T
    pieces = []
    for c in range(len(sums)):
        placed = jnp.where(at_row, table[c : c + 1, :], 0.0)
        pieces.extend(three_parts(placed))
    spread = times_transposed(jnp.concatenate(pieces, axis=0), at_lane)
    for c in range(len(sums)):
        at = 3 * c * rows
        grid_ref[c] = spread[at : at + rows] + spread[at + rows : at + 2 * rows] + spread[at + 2 * rows : at + 3 * rows]


def fields_kernel(
    ids_ref, steps_ref, jump_ref, external_ref, cohesive_ref, mask_ref, grid_ref, field_ref, first_ref, last_ref
):
    rows, lanes = cohesive_ref.shape
    slots = ids_ref.shape[1]
    ids = ids_ref[...]
    at_row = ((iota((rows, slots), 0) == ids // lanes) & (steps_ref[...] > 0)).astype(F32).astype(BF16)
    at_lane = (iota((lanes, slots), 0) == ids % lanes).astype(F32).astype(BF16)
    soft = times_transposed(at_row, at_lane)
    for c in range(3):
        field_ref[c] = jump_ref[c]
        field_ref[3 + c] = external_ref[c]
    field_ref[6] = (1.0 - soft) * cohesive_ref[...]
    field_ref[7] = 0.25 + 0.75 * mask_ref[0].astype(F32)
    field_ref[8] = 0.25 + 0.75 * mask_ref[1].astype(F32)
    for c in range(FIELDS - INPUT_FIELDS):
        field_ref[INPUT_FIELDS + c] = grid_ref[c]
    put_row_edges(field_ref, first_ref, last_ref)


def plan_kernel(here_ref, counts_ref, plan_ref):
    devices = counts_ref.shape[0]
    counts = counts_ref[...]
    before = (iota((devices, devices), 1) < iota((devices, devices), 0)).astype(F32).astype(BF16)
    starts = jnp.dot(before, counts.astype(BF16), preferred_element_type=F32)
    total = jnp.sum(counts, axis=0, keepdims=True)
    slot = iota((1, LANES), 1)
    wanted = (2 * (here_ref[0] + devices * (slot // 2)) + slot % 2).astype(F32)
    source = jnp.sum(jnp.where(starts <= wanted, 1.0, 0.0), axis=0, keepdims=True) - 1.0
    index = jnp.where(wanted < total, 2.0 * source + (slot % 2).astype(F32), -1.0).astype(jnp.int32)
    plan_ref[...] = jnp.broadcast_to(index, plan_ref.shape)


def pack_kernel(here_ref, steps_ref, counts_ref, state_ref, history_ref, out_ref):
    slots, cells = state_ref.shape
    counts = counts_ref[...]
    row = iota(counts.shape, 0)
    start = jnp.sum(jnp.where(row < here_ref[0], counts, 0.0)[:, 0:1]).astype(jnp.int32)
    places = 2 * out_ref.shape[0]
    assert places & (places - 1) == 0
    last = places - 1
    unused = (start - 2) & last & -2
    group = 8

    def one(block, rank):
        at = pl.multiple_of(block * group, group)
        state = state_ref[pl.ds(at, group), :]
        history = history_ref[pl.ds(at, group), :]
        for k in range(group):
            alive = steps_ref[at + k] > 0
            to = jnp.where(alive, rank & last, unused)
            at_lane = pl.multiple_of((to & 1) * (2 * cells), LANES)
            out_ref[pl.ds(to >> 1, 1), 0, pl.ds(at_lane, cells)] = state[k : k + 1]
            out_ref[pl.ds(to >> 1, 1), 0, pl.ds(at_lane + cells, cells)] = history[k : k + 1]
            rank = rank + alive.astype(jnp.int32)
        return rank

    lax.fori_loop(0, slots // group, one, start)


def macro_kernel(
    place_ref, load_ref, field_ref, below_ref, above_ref, left_ref, right_ref, packed_hbm,
    moved_ref, packed_out, sums_ref, sem,
):
    del packed_hbm
    rows = field_ref.shape[1]
    tall = rows + 2 * HALO
    lane = iota((tall, LANES), 1)
    line = iota((tall, LANES), 0)
    row_at, col_at = place_ref[0], place_ref[1]
    has_above = (row_at > 0).astype(jnp.int32)
    has_below = (row_at < place_ref[2] - 1).astype(jnp.int32)
    has_left = (col_at > 0).astype(jnp.int32)
    has_right = (col_at < place_ref[3] - 1).astype(jnp.int32)
    row_ok = jnp.where(line < rows, 1, jnp.where(line < rows + HALO, has_below, has_above)) > 0
    side_ok = jnp.where(lane < HALO, has_right, jnp.where(lane >= LANES - HALO, has_left, 0)) > 0
    valid = (row_ok, row_ok & side_ok)
    below, above = below_ref[...], above_ref[...]
    fill = jnp.zeros((LANES - left_ref.shape[0], LANES), F32)
    left = jnp.concatenate([left_ref[...], fill], axis=0).T[:tall]
    right = jnp.concatenate([right_ref[...], fill], axis=0).T[:tall]

    def field(c):
        middle = with_row_halo(field_ref[c], below, above, c)
        from_left = pltpu.roll(left, (LANES - HALO - HALO * c) % LANES, 1)
        from_right = pltpu.roll(right, (LANES - HALO * c) % LANES, 1) if c else right
        side = jnp.where(lane >= LANES - HALO, from_left, jnp.where(lane < HALO, from_right, 0.0))
        return (middle, side)

    def grid(c):
        return field(INPUT_FIELDS + c)

    def pairs(f, *operands):
        return tuple(f(*parts) for parts in zip(*operands))

    def below_of(v):
        return pairs(lambda x: pltpu.roll(x, tall - 1, 0), v)

    def above_of(v):
        return pairs(lambda x: pltpu.roll(x, 1, 0), v)

    def right_of(v):
        a, b = (pltpu.roll(x, LANES - 1, 1) for x in v)
        end = lane == LANES - 1
        return (jnp.where(end, b, a), jnp.where(end, a, b))

    def left_of(v):
        a, b = (pltpu.roll(x, 1, 1) for x in v)
        end = lane == 0
        return (jnp.where(end, b, a), jnp.where(end, a, b))

    bond_x, bond_y = field(7), field(8)
    low_x, low_y = above_of(bond_x), left_of(bond_y)
    scale = pairs(lambda a, b, c, d, e: a + b + c + d + e, bond_x, low_x, bond_y, low_y, field(6))

    def neighbours(v):
        return pairs(
            lambda bx, vb, lx, va, by, vr, ly, vl: bx * vb + lx * va + by * vr + ly * vl,
            bond_x, below_of(v), low_x, above_of(v), bond_y, right_of(v), low_y, left_of(v),
        )

    load = load_ref[0]
    sources = []
    for c in range(3):
        jump = field(c)
        external = field(3 + c)
        residual = pairs(
            lambda s, j, n, t, e: s * j - n + t - load * e, scale, jump, neighbours(jump), grid(c), external
        )
        sources.append((pairs(lambda r: -r, residual), external))

    def inverse_of(s, t00, t11, t22, t01, t02, t12, ok):
        d00, d11, d22 = s + t00, s + t11, s + t22
        c00 = d11 * d22 - t12 * t12
        c11 = d00 * d22 - t02 * t02
        c22 = d00 * d11 - t01 * t01
        c01 = t02 * t12 - t01 * d22
        c02 = t01 * t12 - t02 * d11
        c12 = t01 * t02 - d00 * t12
        determinant = d00 * c00 + t01 * c01 + t02 * c02
        over = jnp.where(ok, 1.0 / jnp.where(ok, determinant, 1.0), 0.0)
        return tuple(c * over for c in (c00, c11, c22, c01, c02, c12))

    both = pairs(inverse_of, scale, *(grid(3 + k) for k in range(6)), valid)
    i00, i11, i22, i01, i02, i12 = (tuple(both[t][k] for t in range(2)) for k in range(6))

    def dot3(a, x, b, y, c, z):
        return pairs(lambda a, x, b, y, c, z: a * x + b * y + c * z, a, x, b, y, c, z)

    def solve(w):
        return [
            dot3(i00, w[0], i01, w[1], i02, w[2]),
            dot3(i01, w[0], i11, w[1], i12, w[2]),
            dot3(i02, w[0], i12, w[1], i22, w[2]),
        ]

    done = []
    for half in range(2):
        source = [sources[c][half] for c in range(3)]
        iterate = solve(source)
        for _ in range(SWEEPS):
            iterate = solve([pairs(jnp.add, source[c], neighbours(iterate[c])) for c in range(3)])
        done.append([iterate[c][0][:rows] for c in range(3)])
    cross = square = 0.0
    for c in range(3):
        moved_ref[c] = field_ref[c] + done[0][c]
        moved_ref[3 + c] = done[1][c]
        cross = cross + done[0][c] * done[1][c]
        square = square + done[1][c] * done[1][c]
    half = iota((1, 1, LANES), 2) < LANES // 2
    sums_ref[...] = jnp.broadcast_to(jnp.where(half, jnp.sum(cross), jnp.sum(square)), sums_ref.shape)
    copy = pltpu.make_async_copy(sums_ref, packed_out.at[:, :, packed_out.shape[2] - LANES :], sem)
    copy.start()
    copy.wait()


def last_kernel(
    entries, plan_ref, load_ref, radius_ref, arrived_ref, moved_ref,
    new_jump_ref, new_load_ref, new_state_ref, new_history_ref,
):
    new_cap, cells = new_state_ref.shape
    whole = jnp.sum(arrived_ref[:, 0, 4 * cells :], axis=0, keepdims=True)
    half = iota(whole.shape, 1) < LANES // 2
    other = pltpu.roll(whole, LANES // 2, 1)
    cross, square = jnp.where(half, whole, other), jnp.where(half, other, whole)
    shifted = square + 0.25 * entries
    increment = (radius_ref[0] * (entries**0.5) * jnp.sqrt(shifted) - cross) / shifted
    for c in range(3):
        new_jump_ref[c] = moved_ref[c] + increment * moved_ref[3 + c]
    new_load_ref[0] = load_ref[0] + jnp.max(increment)
    group = 8

    def one(block, carry):
        at = pl.multiple_of(block * group, group)
        for k in range(group):
            index = plan_ref[0, at + k]
            valid = index >= 0
            source = jnp.maximum(index, 0)
            at_lane = pl.multiple_of((source & 1) * (2 * cells), LANES)
            state = arrived_ref[pl.ds(source >> 1, 1), 0, pl.ds(at_lane, cells)]
            history = arrived_ref[pl.ds(source >> 1, 1), 0, pl.ds(at_lane + cells, cells)]
            new_state_ref[pl.ds(at + k, 1), :] = jnp.where(valid, state, 0.0)
            new_history_ref[pl.ds(at + k, 1), :] = jnp.where(valid, jnp.maximum(history, jnp.abs(state)), 0.0)
        return carry

    lax.fori_loop(0, new_cap // group, one, 0)


LONG = pl.CostEstimate(flops=10_000_000_000, transcendentals=0, bytes_accessed=60_000_000)


def shape(*dims, dtype=F32):
    return jax.ShapeDtypeStruct(dims, dtype)


def call(kernel, outs, ins, out_specs, mib, scratch=(), cost=None, aliases=None):
    return pl.pallas_call(
        kernel,
        out_shape=outs,
        in_specs=ins,
        out_specs=out_specs,
        scratch_shapes=scratch,
        cost_estimate=cost,
        input_output_aliases=aliases or {},
        compiler_params=pltpu.CompilerParams(vmem_limit_bytes=mib * 1024 * 1024),
    )


def swap(first, last, axis):
    size = lax.axis_size(axis)
    up = [(i, i + 1) for i in range(size - 1)]
    down = [(i + 1, i) for i in range(size - 1)]
    above = lax.ppermute(last, axis, up)
    below = lax.ppermute(first, axis, down)
    return below, above


def on_device(
    jump, external, cohesive, bond_mask, load_factor, arc_radius, stiffness, coupling,
    old_state, old_history, newton_steps, point_ids,
):
    n_row, n_col = lax.axis_size("row"), lax.axis_size("col")
    devices = n_row * n_col
    row_at, col_at = lax.axis_index("row"), lax.axis_index("col")
    here = (row_at * n_col + col_at).astype(jnp.int32)
    slots, cells = old_state.shape
    _, rows, lanes = jump.shape
    edge = HALO * FIELDS
    packed_shape = shape(devices, 1, 4 * cells + LANES)
    place = jnp.stack([row_at, col_at, n_row, n_col]).astype(jnp.int32)
    ids_row = point_ids.reshape(1, slots)
    steps_row = newton_steps.reshape(1, slots)

    mine = call(count_kernel, shape(devices, 1, LANES), [VMEM], VMEM, 2, cost=LONG)(steps_row)
    state, grid = call(
        newton_kernel,
        (shape(slots, cells), shape(FIELDS - INPUT_FIELDS, rows, lanes)),
        [VMEM] * 3 + [HBM, VMEM, HBM, HBM, HBM],
        (VMEM, VMEM),
        NEWTON_MIB,
        scratch=(
            pltpu.VMEM(stiffness.shape, BF16),
            pltpu.VMEM((slots, cells), F32),
            pltpu.VMEM((slots, cells), F32),
            pltpu.VMEM((1, cells), F32),
            pltpu.VMEM((2, slots, cells), BF16),
            pltpu.SemaphoreType.DMA((cells // 256 + 2,)),
        ),
        cost=pl.CostEstimate(
            flops=2 * MAX_STEPS * slots * cells * cells,
            transcendentals=2 * MAX_STEPS * slots * cells,
            bytes_accessed=2 * cells * cells + 12 * slots * cells,
        ),
    )(ids_row, steps_row, jump, stiffness, coupling, old_state, old_history, mine)
    fields, first, last = call(
        fields_kernel,
        (shape(FIELDS, rows, lanes), shape(edge, lanes), shape(edge, lanes)),
        [VMEM] * 7,
        (VMEM,) * 3,
        4,
    )(ids_row, steps_row, jump, external, cohesive, bond_mask, grid)
    below, above = swap(first, last, "row")
    counts = lax.all_to_all(mine, ROWS_COLS, 0, 0, tiled=True).reshape(devices, LANES)
    packed = call(pack_kernel, packed_shape, [SMEM, SMEM, VMEM, VMEM, VMEM], VMEM, 12)(
        here[None], newton_steps, counts, state, old_history
    )
    to_left, to_right = call(
        lane_edges_kernel, (shape(edge, lanes), shape(edge, lanes)), [VMEM] * 3, (VMEM, VMEM), 4
    )(fields, below, above)
    right, left = swap(to_left, to_right, "col")
    moved, packed = call(
        macro_kernel,
        (shape(6, rows, lanes), packed_shape),
        [SMEM, SMEM] + [VMEM] * 5 + [HBM],
        (VMEM, HBM),
        12,
        scratch=(pltpu.VMEM((devices, 1, LANES), F32), pltpu.SemaphoreType.DMA),
        cost=pl.CostEstimate(flops=200_000_000, transcendentals=0, bytes_accessed=2_000_000),
        aliases={7: 1},
    )(place, load_factor, fields, below, above, left, right, packed)
    arrived = lax.all_to_all(packed, ROWS_COLS, 0, 0, tiled=True)
    plan = call(plan_kernel, shape(8, LANES, dtype=jnp.int32), [SMEM, VMEM], VMEM, 2)(here[None], counts)
    new_jump, new_load, new_state, new_history = call(
        functools.partial(last_kernel, 3.0 * rows * lanes * devices),
        (shape(3, rows, lanes), shape(1), shape(slots // 2, cells), shape(slots // 2, cells)),
        [SMEM, SMEM, SMEM, VMEM, VMEM],
        (VMEM, SMEM, VMEM, VMEM),
        12,
    )(plan, load_factor, arc_radius, arrived, moved)
    return (new_jump, new_load, new_state, new_history)


def solution(mesh):
    whole = P(None, "row", "col")
    slot_rows = P(ROWS_COLS, None)
    return jax.shard_map(
        on_device,
        mesh=mesh,
        in_specs=(
            whole, whole, P("row", "col"), whole, P(), P(), P(), P(),
            slot_rows, slot_rows, P(ROWS_COLS), P(ROWS_COLS),
        ),
        out_specs=(whole, P(), slot_rows, slot_rows),
        check_vma=False,
    )
```

```python
import functools

import jax
import jax.numpy as jnp
from jax import lax
from jax.experimental import pallas as pl
from jax.experimental.pallas import tpu as pltpu
from jax.sharding import PartitionSpec as P


MAX_STEPS = 9
SWEEPS = 3
HALO = 4
INPUT_FIELDS = 9
FIELDS = 18
NEWTON_MIB = 52
LANES = 128
ROWS_COLS = ("row", "col")
VMEM = pl.BlockSpec(memory_space=pltpu.VMEM)
SMEM = pl.BlockSpec(memory_space=pltpu.SMEM)
HBM = pl.BlockSpec(memory_space=pltpu.HBM)
F32 = jnp.float32
BF16 = jnp.bfloat16


def iota(shape, dim):
    return lax.broadcasted_iota(jnp.int32, shape, dim)


def three_parts(x):
    high = x.astype(BF16)
    rest = x - high.astype(F32)
    middle = rest.astype(BF16)
    low = (rest - middle.astype(F32)).astype(BF16)
    return high, middle, low


def times_transposed(a, b):
    return lax.dot_general(a, b, (((1,), (1,)), ((), ())), preferred_element_type=F32)


def even_on(axis):
    return lax.rem(lax.axis_index(axis), 2) == 0


def by_parity(even, first, second):
    return jnp.where(even, first, second), jnp.where(even, second, first)


def put_row_edges(field_ref, near_ref, far_ref):
    fields, rows, _ = field_ref.shape
    even = even_on("row")
    for c in range(fields):
        part = slice(HALO * c, HALO * (c + 1))
        near_ref[part, :], far_ref[part, :] = by_parity(even, field_ref[c, rows - HALO :, :], field_ref[c, :HALO, :])


def with_row_halo(field, below, above, c):
    part = slice(HALO * c, HALO * (c + 1))
    return jnp.concatenate([field, below[part], above[part]], axis=0)


def count_kernel(steps_ref, out_ref):
    live = jnp.sum((steps_ref[...] > 0).astype(F32), axis=1, keepdims=True)
    out_ref[...] = jnp.broadcast_to(live[None], out_ref.shape)


def lane_edges_kernel(field_ref, row_near_ref, row_far_ref, near_ref, far_ref):
    below, above = by_parity(even_on("row"), row_near_ref[...], row_far_ref[...])
    fields, rows, lanes = field_ref.shape
    tall = rows + 2 * HALO
    group = iota((tall, lanes), 1) // HALO
    heads = tails = jnp.zeros((tall, lanes), F32)
    for c in range(fields):
        whole = with_row_halo(field_ref[c], below, above, c)
        heads = jnp.where(group == c, pltpu.roll(whole, HALO * c, 1) if c else whole, heads)
        tails = jnp.where(group == c, pltpu.roll(whole, HALO * (c + 1), 1), tails)
    fill = jnp.zeros((lanes - tall, lanes), F32)
    to_left = jnp.concatenate([heads, fill], axis=0).T[: HALO * fields]
    to_right = jnp.concatenate([tails, fill], axis=0).T[: HALO * fields]
    near_ref[...], far_ref[...] = by_parity(even_on("col"), to_right, to_left)


def newton_kernel(
    ids_ref, steps_ref, jump_ref, stiffness_hbm, coupling_ref, old_state_hbm, history_hbm, after_ref,
    state_ref, grid_ref,
    stiffness_ref, damage_ref, load_ref, diagonal_ref, rounded_ref, sems,
):
    del after_ref
    width = 256
    cuts = [slice(t * width, (t + 1) * width) for t in range(stiffness_hbm.shape[1] // width)]
    copies = [
        pltpu.make_async_copy(stiffness_hbm.at[:, part], stiffness_ref.at[:, part], sems.at[t])
        for t, part in enumerate(cuts)
    ]
    get_history = pltpu.make_async_copy(history_hbm, damage_ref, sems.at[len(cuts)])
    get_state = pltpu.make_async_copy(old_state_hbm, state_ref, sems.at[len(cuts) + 1])
    for copy in (get_history, get_state):
        copy.start()
    slots, cells = state_ref.shape
    _, rows, lanes = jump_ref.shape
    wide = 2 * lanes
    fill = jnp.zeros((1, wide - slots), jnp.int32)
    ids_row = jnp.concatenate([ids_ref[...], fill], axis=1)
    steps_row = jnp.concatenate([steps_ref[...], fill], axis=1)
    own = iota((slots, wide), 0) == iota((slots, wide), 1)

    def column(values):
        return jnp.sum(jnp.where(own, values, 0.0), axis=1, keepdims=True)

    steps = column(steps_row.astype(F32))
    at_x = column((ids_row // lanes).astype(F32))
    at_y = column((ids_row % lanes).astype(F32))
    pick_x = (iota((slots, rows), 1).astype(F32) == at_x).astype(F32).astype(BF16)
    pick_y = iota((slots, lanes), 1).astype(F32) == at_y
    at_row = iota((rows, wide), 0) == ids_row // lanes
    at_lane = (iota((lanes, wide), 0) == ids_row % lanes).astype(F32).astype(BF16)
    drive = []
    for c in range(3):
        parts = three_parts(jump_ref[c])
        picked = [jnp.dot(pick_x, part, preferred_element_type=F32) for part in parts]
        whole = (picked[0] + picked[1]) + picked[2]
        drive.append(jnp.sum(jnp.where(pick_y, whole, 0.0), axis=1, keepdims=True))
    load_ref[...] = (
        drive[0] * coupling_ref[0:1, :] + drive[1] * coupling_ref[1:2, :] + drive[2] * coupling_ref[2:3, :]
    )
    for copy in copies:
        copy.start()
    get_history.wait()
    damage_ref[...] = jnp.exp(-damage_ref[...])
    get_state.wait()
    rounded_ref[0] = state_ref[...].astype(BF16)
    eye = iota((LANES, LANES), 0) == iota((LANES, LANES), 1)

    def advance(count, carry, waiting=False):
        now = count % 2 if waiting else lax.rem(count, 2)
        rounded = rounded_ref[now]
        moving = steps > jnp.asarray(count, jnp.int32).astype(F32)
        for t, part in enumerate(cuts):
            if waiting:
                copies[t].wait()
                for low in range(part.start, part.stop, LANES):
                    near = slice(low, low + LANES)
                    block = stiffness_ref[near, near].astype(F32)
                    diagonal_ref[:, near] = jnp.sum(jnp.where(eye, block, 0.0), axis=0, keepdims=True)
            force = jnp.dot(rounded, stiffness_ref[:, part], preferred_element_type=F32)
            current = state_ref[:, part]
            bent = jnp.tanh(current)
            damage = damage_ref[:, part]
            misfit = force + damage * bent - load_ref[:, part]
            slope = diagonal_ref[:, part] + damage * (1.0 - bent * bent)
            current = jnp.where(moving, current - misfit / slope, current)
            state_ref[:, part] = current
            rounded_ref[1 - now, :, part] = current.astype(BF16)
        return carry

    advance(0, 0, waiting=True)
    lax.fori_loop(1, MAX_STEPS, advance, 0)
    bent = jnp.tanh(state_ref[...])
    damage = damage_ref[...]
    pull = damage * bent
    weight = damage * (1.0 - bent * bent)
    c0, c1, c2 = (coupling_ref[k : k + 1, :] for k in range(3))
    sums = [jnp.sum(pull * c, axis=1, keepdims=True) for c in (c0, c1, c2)]
    sums += [
        jnp.sum(weight * c, axis=1, keepdims=True)
        for c in (c0 * c0, c1 * c1, c2 * c2, c0 * c1, c0 * c2, c1 * c2)
    ]
    lane = iota((slots, LANES), 1)
    table = jnp.zeros((slots, LANES), F32)
    for k, value in enumerate(sums):
        table = jnp.where(lane == k, value * (1.0 / cells), table)
    table = jnp.where(steps > 0.0, table, 0.0)
    table = jnp.concatenate([table, jnp.zeros((wide - slots, LANES), F32)], axis=0).T
    pieces = []
    for c in range(len(sums)):
        placed = jnp.where(at_row, table[c : c + 1, :], 0.0)
        pieces.extend(three_parts(placed))
    spread = times_transposed(jnp.concatenate(pieces, axis=0), at_lane)
    for c in range(len(sums)):
        at = 3 * c * rows
        grid_ref[c] = spread[at : at + rows] + spread[at + rows : at + 2 * rows] + spread[at + 2 * rows : at + 3 * rows]


def fields_kernel(
    ids_ref, steps_ref, jump_ref, external_ref, cohesive_ref, mask_ref, grid_ref, field_ref, near_ref, far_ref
):
    rows, lanes = cohesive_ref.shape
    slots = ids_ref.shape[1]
    ids = ids_ref[...]
    at_row = ((iota((rows, slots), 0) == ids // lanes) & (steps_ref[...] > 0)).astype(F32).astype(BF16)
    at_lane = (iota((lanes, slots), 0) == ids % lanes).astype(F32).astype(BF16)
    soft = times_transposed(at_row, at_lane)
    for c in range(3):
        field_ref[c] = jump_ref[c]
        field_ref[3 + c] = external_ref[c]
    field_ref[6] = (1.0 - soft) * cohesive_ref[...]
    field_ref[7] = 0.25 + 0.75 * mask_ref[0].astype(F32)
    field_ref[8] = 0.25 + 0.75 * mask_ref[1].astype(F32)
    for c in range(FIELDS - INPUT_FIELDS):
        field_ref[INPUT_FIELDS + c] = grid_ref[c]
    put_row_edges(field_ref, near_ref, far_ref)


def plan_kernel(here_ref, counts_ref, plan_ref):
    devices = counts_ref.shape[0]
    counts = counts_ref[...]
    before = (iota((devices, devices), 1) < iota((devices, devices), 0)).astype(F32).astype(BF16)
    starts = jnp.dot(before, counts.astype(BF16), preferred_element_type=F32)
    total = jnp.sum(counts, axis=0, keepdims=True)
    slot = iota((1, LANES), 1)
    wanted = (2 * (here_ref[0] + devices * (slot // 2)) + slot % 2).astype(F32)
    source = jnp.sum(jnp.where(starts <= wanted, 1.0, 0.0), axis=0, keepdims=True) - 1.0
    index = jnp.where(wanted < total, 2.0 * source + (slot % 2).astype(F32), -1.0).astype(jnp.int32)
    plan_ref[...] = jnp.broadcast_to(index, plan_ref.shape)


def pack_kernel(here_ref, steps_ref, counts_ref, state_ref, history_ref, out_ref):
    slots, cells = state_ref.shape
    counts = counts_ref[...]
    row = iota(counts.shape, 0)
    start = jnp.sum(jnp.where(row < here_ref[0], counts, 0.0)[:, 0:1]).astype(jnp.int32)
    places = 2 * out_ref.shape[0]
    assert places & (places - 1) == 0
    last = places - 1
    unused = (start - 2) & last & -2
    group = 8

    def one(block, rank):
        at = pl.multiple_of(block * group, group)
        state = state_ref[pl.ds(at, group), :]
        history = history_ref[pl.ds(at, group), :]
        for k in range(group):
            alive = steps_ref[at + k] > 0
            to = jnp.where(alive, rank & last, unused)
            at_lane = pl.multiple_of((to & 1) * (2 * cells), LANES)
            out_ref[pl.ds(to >> 1, 1), 0, pl.ds(at_lane, cells)] = state[k : k + 1]
            out_ref[pl.ds(to >> 1, 1), 0, pl.ds(at_lane + cells, cells)] = history[k : k + 1]
            rank = rank + alive.astype(jnp.int32)
        return rank

    lax.fori_loop(0, slots // group, one, start)


def macro_kernel(
    place_ref, load_ref, field_ref, row_near_ref, row_far_ref, col_near_ref, col_far_ref, packed_hbm,
    moved_ref, packed_out, sums_ref, sem,
):
    del packed_hbm
    rows = field_ref.shape[1]
    tall = rows + 2 * HALO
    lane = iota((tall, LANES), 1)
    line = iota((tall, LANES), 0)
    row_at, col_at = place_ref[0], place_ref[1]
    has_above = (row_at > 0).astype(jnp.int32)
    has_below = (row_at < place_ref[2] - 1).astype(jnp.int32)
    has_left = (col_at > 0).astype(jnp.int32)
    has_right = (col_at < place_ref[3] - 1).astype(jnp.int32)
    row_ok = jnp.where(line < rows, 1, jnp.where(line < rows + HALO, has_below, has_above)) > 0
    side_ok = jnp.where(lane < HALO, has_right, jnp.where(lane >= LANES - HALO, has_left, 0)) > 0
    valid = (row_ok, row_ok & side_ok)
    below, above = by_parity(even_on("row"), row_near_ref[...], row_far_ref[...])
    right, left = by_parity(even_on("col"), col_near_ref[...], col_far_ref[...])
    fill = jnp.zeros((LANES - left.shape[0], LANES), F32)
    left = jnp.concatenate([left, fill], axis=0).T[:tall]
    right = jnp.concatenate([right, fill], axis=0).T[:tall]

    def field(c):
        middle = with_row_halo(field_ref[c], below, above, c)
        from_left = pltpu.roll(left, (LANES - HALO - HALO * c) % LANES, 1)
        from_right = pltpu.roll(right, (LANES - HALO * c) % LANES, 1) if c else right
        side = jnp.where(lane >= LANES - HALO, from_left, jnp.where(lane < HALO, from_right, 0.0))
        return (middle, side)

    def grid(c):
        return field(INPUT_FIELDS + c)

    def pairs(f, *operands):
        return tuple(f(*parts) for parts in zip(*operands))

    def below_of(v):
        return pairs(lambda x: pltpu.roll(x, tall - 1, 0), v)

    def above_of(v):
        return pairs(lambda x: pltpu.roll(x, 1, 0), v)

    def right_of(v):
        a, b = (pltpu.roll(x, LANES - 1, 1) for x in v)
        end = lane == LANES - 1
        return (jnp.where(end, b, a), jnp.where(end, a, b))

    def left_of(v):
        a, b = (pltpu.roll(x, 1, 1) for x in v)
        end = lane == 0
        return (jnp.where(end, b, a), jnp.where(end, a, b))

    bond_x, bond_y = field(7), field(8)
    low_x, low_y = above_of(bond_x), left_of(bond_y)
    scale = pairs(lambda a, b, c, d, e: a + b + c + d + e, bond_x, low_x, bond_y, low_y, field(6))

    def neighbours(v):
        return pairs(
            lambda bx, vb, lx, va, by, vr, ly, vl: bx * vb + lx * va + by * vr + ly * vl,
            bond_x, below_of(v), low_x, above_of(v), bond_y, right_of(v), low_y, left_of(v),
        )

    load = load_ref[0]
    sources = []
    for c in range(3):
        jump = field(c)
        external = field(3 + c)
        residual = pairs(
            lambda s, j, n, t, e: s * j - n + t - load * e, scale, jump, neighbours(jump), grid(c), external
        )
        sources.append((pairs(lambda r: -r, residual), external))

    def inverse_of(s, t00, t11, t22, t01, t02, t12, ok):
        d00, d11, d22 = s + t00, s + t11, s + t22
        c00 = d11 * d22 - t12 * t12
        c11 = d00 * d22 - t02 * t02
        c22 = d00 * d11 - t01 * t01
        c01 = t02 * t12 - t01 * d22
        c02 = t01 * t12 - t02 * d11
        c12 = t01 * t02 - d00 * t12
        determinant = d00 * c00 + t01 * c01 + t02 * c02
        over = jnp.where(ok, 1.0 / jnp.where(ok, determinant, 1.0), 0.0)
        return tuple(c * over for c in (c00, c11, c22, c01, c02, c12))

    both = pairs(inverse_of, scale, *(grid(3 + k) for k in range(6)), valid)
    i00, i11, i22, i01, i02, i12 = (tuple(both[t][k] for t in range(2)) for k in range(6))

    def dot3(a, x, b, y, c, z):
        return pairs(lambda a, x, b, y, c, z: a * x + b * y + c * z, a, x, b, y, c, z)

    def solve(w):
        return [
            dot3(i00, w[0], i01, w[1], i02, w[2]),
            dot3(i01, w[0], i11, w[1], i12, w[2]),
            dot3(i02, w[0], i12, w[1], i22, w[2]),
        ]

    done = []
    for half in range(2):
        source = [sources[c][half] for c in range(3)]
        iterate = solve(source)
        for _ in range(SWEEPS):
            iterate = solve([pairs(jnp.add, source[c], neighbours(iterate[c])) for c in range(3)])
        done.append([iterate[c][0][:rows] for c in range(3)])
    cross = square = 0.0
    for c in range(3):
        moved_ref[c] = field_ref[c] + done[0][c]
        moved_ref[3 + c] = done[1][c]
        cross = cross + done[0][c] * done[1][c]
        square = square + done[1][c] * done[1][c]
    half = iota((1, 1, LANES), 2) < LANES // 2
    sums_ref[...] = jnp.broadcast_to(jnp.where(half, jnp.sum(cross), jnp.sum(square)), sums_ref.shape)
    copy = pltpu.make_async_copy(sums_ref, packed_out.at[:, :, packed_out.shape[2] - LANES :], sem)
    copy.start()
    copy.wait()


def last_kernel(
    entries, plan_ref, load_ref, radius_ref, arrived_ref, moved_ref,
    new_jump_ref, new_load_ref, new_state_ref, new_history_ref,
):
    new_cap, cells = new_state_ref.shape
    whole = jnp.sum(arrived_ref[:, 0, 4 * cells :], axis=0, keepdims=True)
    half = iota(whole.shape, 1) < LANES // 2
    other = pltpu.roll(whole, LANES // 2, 1)
    cross, square = jnp.where(half, whole, other), jnp.where(half, other, whole)
    shifted = square + 0.25 * entries
    increment = (radius_ref[0] * (entries**0.5) * jnp.sqrt(shifted) - cross) / shifted
    for c in range(3):
        new_jump_ref[c] = moved_ref[c] + increment * moved_ref[3 + c]
    new_load_ref[0] = load_ref[0] + jnp.max(increment)
    group = 8

    def one(block, carry):
        at = pl.multiple_of(block * group, group)
        for k in range(group):
            index = plan_ref[0, at + k]
            valid = index >= 0
            source = jnp.maximum(index, 0)
            at_lane = pl.multiple_of((source & 1) * (2 * cells), LANES)
            state = arrived_ref[pl.ds(source >> 1, 1), 0, pl.ds(at_lane, cells)]
            history = arrived_ref[pl.ds(source >> 1, 1), 0, pl.ds(at_lane + cells, cells)]
            new_state_ref[pl.ds(at + k, 1), :] = jnp.where(valid, state, 0.0)
            new_history_ref[pl.ds(at + k, 1), :] = jnp.where(valid, jnp.maximum(history, jnp.abs(state)), 0.0)
        return carry

    lax.fori_loop(0, new_cap // group, one, 0)


LONG = pl.CostEstimate(flops=10_000_000_000, transcendentals=0, bytes_accessed=60_000_000)


def shape(*dims, dtype=F32):
    return jax.ShapeDtypeStruct(dims, dtype)


def call(kernel, outs, ins, out_specs, mib, scratch=(), cost=None, aliases=None):
    return pl.pallas_call(
        kernel,
        out_shape=outs,
        in_specs=ins,
        out_specs=out_specs,
        scratch_shapes=scratch,
        cost_estimate=cost,
        input_output_aliases=aliases or {},
        compiler_params=pltpu.CompilerParams(vmem_limit_bytes=mib * 1024 * 1024),
    )


def swap(near, far, axis):
    size = lax.axis_size(axis)
    pairs = [(i, i + 1) for i in range(size - 1)]
    both = [pairs[k::2] + [(b, a) for a, b in pairs[k::2]] for k in range(2)]
    return lax.ppermute(near, axis, both[0]), lax.ppermute(far, axis, both[1])


def on_device(
    jump, external, cohesive, bond_mask, load_factor, arc_radius, stiffness, coupling,
    old_state, old_history, newton_steps, point_ids,
):
    n_row, n_col = lax.axis_size("row"), lax.axis_size("col")
    devices = n_row * n_col
    row_at, col_at = lax.axis_index("row"), lax.axis_index("col")
    here = (row_at * n_col + col_at).astype(jnp.int32)
    slots, cells = old_state.shape
    _, rows, lanes = jump.shape
    edge = HALO * FIELDS
    packed_shape = shape(devices, 1, 4 * cells + LANES)
    place = jnp.stack([row_at, col_at, n_row, n_col]).astype(jnp.int32)
    ids_row = point_ids.reshape(1, slots)
    steps_row = newton_steps.reshape(1, slots)

    mine = call(count_kernel, shape(devices, 1, LANES), [VMEM], VMEM, 2, cost=LONG)(steps_row)
    state, grid = call(
        newton_kernel,
        (shape(slots, cells), shape(FIELDS - INPUT_FIELDS, rows, lanes)),
        [VMEM] * 3 + [HBM, VMEM, HBM, HBM, HBM],
        (VMEM, VMEM),
        NEWTON_MIB,
        scratch=(
            pltpu.VMEM(stiffness.shape, BF16),
            pltpu.VMEM((slots, cells), F32),
            pltpu.VMEM((slots, cells), F32),
            pltpu.VMEM((1, cells), F32),
            pltpu.VMEM((2, slots, cells), BF16),
            pltpu.SemaphoreType.DMA((cells // 256 + 2,)),
        ),
        cost=pl.CostEstimate(
            flops=2 * MAX_STEPS * slots * cells * cells,
            transcendentals=2 * MAX_STEPS * slots * cells,
            bytes_accessed=2 * cells * cells + 12 * slots * cells,
        ),
    )(ids_row, steps_row, jump, stiffness, coupling, old_state, old_history, mine)
    fields, near, far = call(
        fields_kernel,
        (shape(FIELDS, rows, lanes), shape(edge, lanes), shape(edge, lanes)),
        [VMEM] * 7,
        (VMEM,) * 3,
        4,
    )(ids_row, steps_row, jump, external, cohesive, bond_mask, grid)
    row_near, row_far = swap(near, far, "row")
    counts = lax.all_to_all(mine, ROWS_COLS, 0, 0, tiled=True).reshape(devices, LANES)
    packed = call(pack_kernel, packed_shape, [SMEM, SMEM, VMEM, VMEM, VMEM], VMEM, 12)(
        here[None], newton_steps, counts, state, old_history
    )
    near, far = call(
        lane_edges_kernel, (shape(edge, lanes), shape(edge, lanes)), [VMEM] * 3, (VMEM, VMEM), 4
    )(fields, row_near, row_far)
    col_near, col_far = swap(near, far, "col")
    moved, packed = call(
        macro_kernel,
        (shape(6, rows, lanes), packed_shape),
        [SMEM, SMEM] + [VMEM] * 5 + [HBM],
        (VMEM, HBM),
        12,
        scratch=(pltpu.VMEM((devices, 1, LANES), F32), pltpu.SemaphoreType.DMA),
        cost=pl.CostEstimate(flops=200_000_000, transcendentals=0, bytes_accessed=2_000_000),
        aliases={7: 1},
    )(place, load_factor, fields, row_near, row_far, col_near, col_far, packed)
    arrived = lax.all_to_all(packed, ROWS_COLS, 0, 0, tiled=True)
    plan = call(plan_kernel, shape(8, LANES, dtype=jnp.int32), [SMEM, VMEM], VMEM, 2)(here[None], counts)
    new_jump, new_load, new_state, new_history = call(
        functools.partial(last_kernel, 3.0 * rows * lanes * devices),
        (shape(3, rows, lanes), shape(1), shape(slots // 2, cells), shape(slots // 2, cells)),
        [SMEM, SMEM, SMEM, VMEM, VMEM],
        (VMEM, SMEM, VMEM, VMEM),
        12,
    )(plan, load_factor, arc_radius, arrived, moved)
    return (new_jump, new_load, new_state, new_history)


def solution(mesh):
    whole = P(None, "row", "col")
    slot_rows = P(ROWS_COLS, None)
    return jax.shard_map(
        on_device,
        mesh=mesh,
        in_specs=(
            whole, whole, P("row", "col"), whole, P(), P(), P(), P(),
            slot_rows, slot_rows, P(ROWS_COLS), P(ROWS_COLS),
        ),
        out_specs=(whole, P(), slot_rows, slot_rows),
        check_vma=False,
    )
```

```python
import functools

import jax
import jax.numpy as jnp
from jax import lax
from jax.experimental import pallas as pl
from jax.experimental.pallas import tpu as pltpu
from jax.sharding import PartitionSpec as P


MAX_STEPS = 9
SWEEPS = 3
HALO = 4
INPUT_FIELDS = 9
FIELDS = 18
NEWTON_MIB = 52
LANES = 128
ROWS_COLS = ("row", "col")
VMEM = pl.BlockSpec(memory_space=pltpu.VMEM)
SMEM = pl.BlockSpec(memory_space=pltpu.SMEM)
HBM = pl.BlockSpec(memory_space=pltpu.HBM)
F32 = jnp.float32
BF16 = jnp.bfloat16


def iota(shape, dim):
    return lax.broadcasted_iota(jnp.int32, shape, dim)


def three_parts(x):
    high = x.astype(BF16)
    rest = x - high.astype(F32)
    middle = rest.astype(BF16)
    low = (rest - middle.astype(F32)).astype(BF16)
    return high, middle, low


def times_transposed(a, b):
    return lax.dot_general(a, b, (((1,), (1,)), ((), ())), preferred_element_type=F32)


def even_on(axis):
    return lax.rem(lax.axis_index(axis), 2) == 0


def by_parity(even, first, second):
    return jnp.where(even, first, second), jnp.where(even, second, first)


def put_row_edges(field_ref, near_ref, far_ref):
    fields, rows, _ = field_ref.shape
    even = even_on("row")
    for c in range(fields):
        part = slice(HALO * c, HALO * (c + 1))
        near_ref[part, :], far_ref[part, :] = by_parity(even, field_ref[c, rows - HALO :, :], field_ref[c, :HALO, :])


def with_row_halo(field, below, above, c):
    part = slice(HALO * c, HALO * (c + 1))
    return jnp.concatenate([field, below[part], above[part]], axis=0)


def count_kernel(steps_ref, out_ref):
    live = jnp.sum((steps_ref[...] > 0).astype(F32), axis=1, keepdims=True)
    out_ref[...] = jnp.broadcast_to(live[None], out_ref.shape)


def lane_edges_kernel(field_ref, row_near_ref, row_far_ref, near_ref, far_ref):
    below, above = by_parity(even_on("row"), row_near_ref[...], row_far_ref[...])
    fields, rows, lanes = field_ref.shape
    tall = rows + 2 * HALO
    group = iota((tall, lanes), 1) // HALO
    heads = tails = jnp.zeros((tall, lanes), F32)
    for c in range(fields):
        whole = with_row_halo(field_ref[c], below, above, c)
        heads = jnp.where(group == c, pltpu.roll(whole, HALO * c, 1) if c else whole, heads)
        tails = jnp.where(group == c, pltpu.roll(whole, HALO * (c + 1), 1), tails)
    fill = jnp.zeros((lanes - tall, lanes), F32)
    to_left = jnp.concatenate([heads, fill], axis=0).T[: HALO * fields]
    to_right = jnp.concatenate([tails, fill], axis=0).T[: HALO * fields]
    near_ref[...], far_ref[...] = by_parity(even_on("col"), to_right, to_left)


def newton_kernel(
    ids_ref, steps_ref, jump_ref, stiffness_hbm, coupling_ref, old_state_hbm, history_hbm, count_in,
    state_ref, grid_ref, count_out,
    stiffness_ref, damage_ref, load_ref, diagonal_ref, rounded_ref, sems,
):
    del count_in, count_out
    width = 256
    cuts = [slice(t * width, (t + 1) * width) for t in range(stiffness_hbm.shape[1] // width)]
    copies = [
        pltpu.make_async_copy(stiffness_hbm.at[:, part], stiffness_ref.at[:, part], sems.at[t])
        for t, part in enumerate(cuts)
    ]
    get_history = pltpu.make_async_copy(history_hbm, damage_ref, sems.at[len(cuts)])
    get_state = pltpu.make_async_copy(old_state_hbm, state_ref, sems.at[len(cuts) + 1])
    for copy in (get_history, get_state):
        copy.start()
    slots, cells = state_ref.shape
    _, rows, lanes = jump_ref.shape
    wide = 2 * lanes
    fill = jnp.zeros((1, wide - slots), jnp.int32)
    ids_row = jnp.concatenate([ids_ref[...], fill], axis=1)
    steps_row = jnp.concatenate([steps_ref[...], fill], axis=1)
    own = iota((slots, wide), 0) == iota((slots, wide), 1)

    def column(values):
        return jnp.sum(jnp.where(own, values, 0.0), axis=1, keepdims=True)

    steps = column(steps_row.astype(F32))
    at_x = column((ids_row // lanes).astype(F32))
    at_y = column((ids_row % lanes).astype(F32))
    pick_x = (iota((slots, rows), 1).astype(F32) == at_x).astype(F32).astype(BF16)
    pick_y = iota((slots, lanes), 1).astype(F32) == at_y
    at_row = iota((rows, wide), 0) == ids_row // lanes
    at_lane = (iota((lanes, wide), 0) == ids_row % lanes).astype(F32).astype(BF16)
    drive = []
    for c in range(3):
        parts = three_parts(jump_ref[c])
        picked = [jnp.dot(pick_x, part, preferred_element_type=F32) for part in parts]
        whole = (picked[0] + picked[1]) + picked[2]
        drive.append(jnp.sum(jnp.where(pick_y, whole, 0.0), axis=1, keepdims=True))
    load_ref[...] = (
        drive[0] * coupling_ref[0:1, :] + drive[1] * coupling_ref[1:2, :] + drive[2] * coupling_ref[2:3, :]
    )
    for copy in copies:
        copy.start()
    get_history.wait()
    damage_ref[...] = jnp.exp(-damage_ref[...])
    get_state.wait()
    rounded_ref[0] = state_ref[...].astype(BF16)
    eye = iota((LANES, LANES), 0) == iota((LANES, LANES), 1)

    def advance(count, carry, waiting=False):
        now = count % 2 if waiting else lax.rem(count, 2)
        rounded = rounded_ref[now]
        moving = steps > jnp.asarray(count, jnp.int32).astype(F32)
        for t, part in enumerate(cuts):
            if waiting:
                copies[t].wait()
                for low in range(part.start, part.stop, LANES):
                    near = slice(low, low + LANES)
                    block = stiffness_ref[near, near].astype(F32)
                    diagonal_ref[:, near] = jnp.sum(jnp.where(eye, block, 0.0), axis=0, keepdims=True)
            force = jnp.dot(rounded, stiffness_ref[:, part], preferred_element_type=F32)
            current = state_ref[:, part]
            bent = jnp.tanh(current)
            damage = damage_ref[:, part]
            misfit = force + damage * bent - load_ref[:, part]
            slope = diagonal_ref[:, part] + damage * (1.0 - bent * bent)
            current = jnp.where(moving, current - misfit / slope, current)
            state_ref[:, part] = current
            rounded_ref[1 - now, :, part] = current.astype(BF16)
        return carry

    advance(0, 0, waiting=True)
    lax.fori_loop(1, MAX_STEPS, advance, 0)
    bent = jnp.tanh(state_ref[...])
    damage = damage_ref[...]
    pull = damage * bent
    weight = damage * (1.0 - bent * bent)
    c0, c1, c2 = (coupling_ref[k : k + 1, :] for k in range(3))
    sums = [jnp.sum(pull * c, axis=1, keepdims=True) for c in (c0, c1, c2)]
    sums += [
        jnp.sum(weight * c, axis=1, keepdims=True)
        for c in (c0 * c0, c1 * c1, c2 * c2, c0 * c1, c0 * c2, c1 * c2)
    ]
    lane = iota((slots, LANES), 1)
    table = jnp.zeros((slots, LANES), F32)
    for k, value in enumerate(sums):
        table = jnp.where(lane == k, value * (1.0 / cells), table)
    table = jnp.where(steps > 0.0, table, 0.0)
    table = jnp.concatenate([table, jnp.zeros((wide - slots, LANES), F32)], axis=0).T
    pieces = []
    for c in range(len(sums)):
        placed = jnp.where(at_row, table[c : c + 1, :], 0.0)
        pieces.extend(three_parts(placed))
    spread = times_transposed(jnp.concatenate(pieces, axis=0), at_lane)
    for c in range(len(sums)):
        at = 3 * c * rows
        grid_ref[c] = spread[at : at + rows] + spread[at + rows : at + 2 * rows] + spread[at + 2 * rows : at + 3 * rows]


def fields_kernel(
    ids_ref, steps_ref, jump_ref, external_ref, cohesive_ref, mask_ref, grid_ref, field_ref, near_ref, far_ref
):
    rows, lanes = cohesive_ref.shape
    slots = ids_ref.shape[1]
    ids = ids_ref[...]
    at_row = ((iota((rows, slots), 0) == ids // lanes) & (steps_ref[...] > 0)).astype(F32).astype(BF16)
    at_lane = (iota((lanes, slots), 0) == ids % lanes).astype(F32).astype(BF16)
    soft = times_transposed(at_row, at_lane)
    for c in range(3):
        field_ref[c] = jump_ref[c]
        field_ref[3 + c] = external_ref[c]
    field_ref[6] = (1.0 - soft) * cohesive_ref[...]
    field_ref[7] = 0.25 + 0.75 * mask_ref[0].astype(F32)
    field_ref[8] = 0.25 + 0.75 * mask_ref[1].astype(F32)
    for c in range(FIELDS - INPUT_FIELDS):
        field_ref[INPUT_FIELDS + c] = grid_ref[c]
    put_row_edges(field_ref, near_ref, far_ref)


def plan_kernel(here_ref, counts_ref, plan_ref):
    devices = counts_ref.shape[0]
    counts = counts_ref[...]
    before = (iota((devices, devices), 1) < iota((devices, devices), 0)).astype(F32).astype(BF16)
    starts = jnp.dot(before, counts.astype(BF16), preferred_element_type=F32)
    total = jnp.sum(counts, axis=0, keepdims=True)
    slot = iota((1, LANES), 1)
    wanted = (2 * (here_ref[0] + devices * (slot // 2)) + slot % 2).astype(F32)
    source = jnp.sum(jnp.where(starts <= wanted, 1.0, 0.0), axis=0, keepdims=True) - 1.0
    index = jnp.where(wanted < total, 2.0 * source + (slot % 2).astype(F32), -1.0).astype(jnp.int32)
    plan_ref[...] = jnp.broadcast_to(index, plan_ref.shape)


def pack_kernel(here_ref, steps_ref, counts_ref, state_ref, history_ref, out_ref):
    slots, cells = state_ref.shape
    counts = counts_ref[...]
    row = iota(counts.shape, 0)
    start = jnp.sum(jnp.where(row < here_ref[0], counts, 0.0)[:, 0:1]).astype(jnp.int32)
    places = 2 * out_ref.shape[0]
    assert places & (places - 1) == 0
    last = places - 1
    unused = (start - 2) & last & -2
    group = 8

    def one(block, rank):
        at = pl.multiple_of(block * group, group)
        state = state_ref[pl.ds(at, group), :]
        history = history_ref[pl.ds(at, group), :]
        for k in range(group):
            alive = steps_ref[at + k] > 0
            to = jnp.where(alive, rank & last, unused)
            at_lane = pl.multiple_of((to & 1) * (2 * cells), LANES)
            out_ref[pl.ds(to >> 1, 1), 0, pl.ds(at_lane, cells)] = state[k : k + 1]
            out_ref[pl.ds(to >> 1, 1), 0, pl.ds(at_lane + cells, cells)] = history[k : k + 1]
            rank = rank + alive.astype(jnp.int32)
        return rank

    lax.fori_loop(0, slots // group, one, start)


def macro_kernel(
    place_ref, load_ref, field_ref, row_near_ref, row_far_ref, col_near_ref, col_far_ref, packed_hbm,
    moved_ref, packed_out, sums_ref, sem,
):
    del packed_hbm
    rows = field_ref.shape[1]
    tall = rows + 2 * HALO
    lane = iota((tall, LANES), 1)
    line = iota((tall, LANES), 0)
    row_at, col_at = place_ref[0], place_ref[1]
    has_above = (row_at > 0).astype(jnp.int32)
    has_below = (row_at < place_ref[2] - 1).astype(jnp.int32)
    has_left = (col_at > 0).astype(jnp.int32)
    has_right = (col_at < place_ref[3] - 1).astype(jnp.int32)
    row_ok = jnp.where(line < rows, 1, jnp.where(line < rows + HALO, has_below, has_above)) > 0
    side_ok = jnp.where(lane < HALO, has_right, jnp.where(lane >= LANES - HALO, has_left, 0)) > 0
    valid = (row_ok, row_ok & side_ok)
    below, above = by_parity(even_on("row"), row_near_ref[...], row_far_ref[...])
    right, left = by_parity(even_on("col"), col_near_ref[...], col_far_ref[...])
    fill = jnp.zeros((LANES - left.shape[0], LANES), F32)
    left = jnp.concatenate([left, fill], axis=0).T[:tall]
    right = jnp.concatenate([right, fill], axis=0).T[:tall]

    def field(c):
        middle = with_row_halo(field_ref[c], below, above, c)
        from_left = pltpu.roll(left, (LANES - HALO - HALO * c) % LANES, 1)
        from_right = pltpu.roll(right, (LANES - HALO * c) % LANES, 1) if c else right
        side = jnp.where(lane >= LANES - HALO, from_left, jnp.where(lane < HALO, from_right, 0.0))
        return (middle, side)

    def grid(c):
        return field(INPUT_FIELDS + c)

    def pairs(f, *operands):
        return tuple(f(*parts) for parts in zip(*operands))

    def below_of(v):
        return pairs(lambda x: pltpu.roll(x, tall - 1, 0), v)

    def above_of(v):
        return pairs(lambda x: pltpu.roll(x, 1, 0), v)

    def right_of(v):
        a, b = (pltpu.roll(x, LANES - 1, 1) for x in v)
        end = lane == LANES - 1
        return (jnp.where(end, b, a), jnp.where(end, a, b))

    def left_of(v):
        a, b = (pltpu.roll(x, 1, 1) for x in v)
        end = lane == 0
        return (jnp.where(end, b, a), jnp.where(end, a, b))

    bond_x, bond_y = field(7), field(8)
    low_x, low_y = above_of(bond_x), left_of(bond_y)
    scale = pairs(lambda a, b, c, d, e: a + b + c + d + e, bond_x, low_x, bond_y, low_y, field(6))

    def neighbours(v):
        return pairs(
            lambda bx, vb, lx, va, by, vr, ly, vl: bx * vb + lx * va + by * vr + ly * vl,
            bond_x, below_of(v), low_x, above_of(v), bond_y, right_of(v), low_y, left_of(v),
        )

    load = load_ref[0]
    sources = []
    for c in range(3):
        jump = field(c)
        external = field(3 + c)
        residual = pairs(
            lambda s, j, n, t, e: s * j - n + t - load * e, scale, jump, neighbours(jump), grid(c), external
        )
        sources.append((pairs(lambda r: -r, residual), external))

    def inverse_of(s, t00, t11, t22, t01, t02, t12, ok):
        d00, d11, d22 = s + t00, s + t11, s + t22
        c00 = d11 * d22 - t12 * t12
        c11 = d00 * d22 - t02 * t02
        c22 = d00 * d11 - t01 * t01
        c01 = t02 * t12 - t01 * d22
        c02 = t01 * t12 - t02 * d11
        c12 = t01 * t02 - d00 * t12
        determinant = d00 * c00 + t01 * c01 + t02 * c02
        over = jnp.where(ok, 1.0 / jnp.where(ok, determinant, 1.0), 0.0)
        return tuple(c * over for c in (c00, c11, c22, c01, c02, c12))

    both = pairs(inverse_of, scale, *(grid(3 + k) for k in range(6)), valid)
    i00, i11, i22, i01, i02, i12 = (tuple(both[t][k] for t in range(2)) for k in range(6))

    def dot3(a, x, b, y, c, z):
        return pairs(lambda a, x, b, y, c, z: a * x + b * y + c * z, a, x, b, y, c, z)

    def solve(w):
        return [
            dot3(i00, w[0], i01, w[1], i02, w[2]),
            dot3(i01, w[0], i11, w[1], i12, w[2]),
            dot3(i02, w[0], i12, w[1], i22, w[2]),
        ]

    done = []
    for half in range(2):
        source = [sources[c][half] for c in range(3)]
        iterate = solve(source)
        for _ in range(SWEEPS):
            iterate = solve([pairs(jnp.add, source[c], neighbours(iterate[c])) for c in range(3)])
        done.append([iterate[c][0][:rows] for c in range(3)])
    cross = square = 0.0
    for c in range(3):
        moved_ref[c] = field_ref[c] + done[0][c]
        moved_ref[3 + c] = done[1][c]
        cross = cross + done[0][c] * done[1][c]
        square = square + done[1][c] * done[1][c]
    half = iota((1, 1, LANES), 2) < LANES // 2
    sums_ref[...] = jnp.broadcast_to(jnp.where(half, jnp.sum(cross), jnp.sum(square)), sums_ref.shape)
    copy = pltpu.make_async_copy(sums_ref, packed_out.at[:, :, packed_out.shape[2] - LANES :], sem)
    copy.start()
    copy.wait()


def last_kernel(
    entries, plan_ref, load_ref, radius_ref, arrived_ref, moved_ref,
    new_jump_ref, new_load_ref, new_state_ref, new_history_ref,
):
    new_cap, cells = new_state_ref.shape
    whole = jnp.sum(arrived_ref[:, 0, 4 * cells :], axis=0, keepdims=True)
    half = iota(whole.shape, 1) < LANES // 2
    other = pltpu.roll(whole, LANES // 2, 1)
    cross, square = jnp.where(half, whole, other), jnp.where(half, other, whole)
    shifted = square + 0.25 * entries
    increment = (radius_ref[0] * (entries**0.5) * jnp.sqrt(shifted) - cross) / shifted
    for c in range(3):
        new_jump_ref[c] = moved_ref[c] + increment * moved_ref[3 + c]
    new_load_ref[0] = load_ref[0] + jnp.max(increment)
    group = 8

    def one(block, carry):
        at = pl.multiple_of(block * group, group)
        for k in range(group):
            index = plan_ref[0, at + k]
            valid = index >= 0
            source = jnp.maximum(index, 0)
            at_lane = pl.multiple_of((source & 1) * (2 * cells), LANES)
            state = arrived_ref[pl.ds(source >> 1, 1), 0, pl.ds(at_lane, cells)]
            history = arrived_ref[pl.ds(source >> 1, 1), 0, pl.ds(at_lane + cells, cells)]
            new_state_ref[pl.ds(at + k, 1), :] = jnp.where(valid, state, 0.0)
            new_history_ref[pl.ds(at + k, 1), :] = jnp.where(valid, jnp.maximum(history, jnp.abs(state)), 0.0)
        return carry

    lax.fori_loop(0, new_cap // group, one, 0)


LONG = pl.CostEstimate(flops=10_000_000_000, transcendentals=0, bytes_accessed=60_000_000)


def shape(*dims, dtype=F32):
    return jax.ShapeDtypeStruct(dims, dtype)


def call(kernel, outs, ins, out_specs, mib, scratch=(), cost=None, aliases=None):
    return pl.pallas_call(
        kernel,
        out_shape=outs,
        in_specs=ins,
        out_specs=out_specs,
        scratch_shapes=scratch,
        cost_estimate=cost,
        input_output_aliases=aliases or {},
        compiler_params=pltpu.CompilerParams(vmem_limit_bytes=mib * 1024 * 1024),
    )


def swap(near, far, axis):
    size = lax.axis_size(axis)
    pairs = [(i, i + 1) for i in range(size - 1)]
    both = [pairs[k::2] + [(b, a) for a, b in pairs[k::2]] for k in range(2)]
    return lax.ppermute(near, axis, both[0]), lax.ppermute(far, axis, both[1])


def on_device(
    jump, external, cohesive, bond_mask, load_factor, arc_radius, stiffness, coupling,
    old_state, old_history, newton_steps, point_ids,
):
    n_row, n_col = lax.axis_size("row"), lax.axis_size("col")
    devices = n_row * n_col
    row_at, col_at = lax.axis_index("row"), lax.axis_index("col")
    here = (row_at * n_col + col_at).astype(jnp.int32)
    slots, cells = old_state.shape
    _, rows, lanes = jump.shape
    edge = HALO * FIELDS
    packed_shape = shape(devices, 1, 4 * cells + LANES)
    place = jnp.stack([row_at, col_at, n_row, n_col]).astype(jnp.int32)
    ids_row = point_ids.reshape(1, slots)
    steps_row = newton_steps.reshape(1, slots)

    mine = call(count_kernel, shape(devices, 1, LANES), [VMEM], VMEM, 2, cost=LONG)(steps_row)
    state, grid, mine = call(
        newton_kernel,
        (shape(slots, cells), shape(FIELDS - INPUT_FIELDS, rows, lanes), shape(devices, 1, LANES)),
        [VMEM] * 3 + [HBM, VMEM, HBM, HBM, HBM],
        (VMEM, VMEM, HBM),
        NEWTON_MIB,
        scratch=(
            pltpu.VMEM(stiffness.shape, BF16),
            pltpu.VMEM((slots, cells), F32),
            pltpu.VMEM((slots, cells), F32),
            pltpu.VMEM((1, cells), F32),
            pltpu.VMEM((2, slots, cells), BF16),
            pltpu.SemaphoreType.DMA((cells // 256 + 2,)),
        ),
        cost=pl.CostEstimate(
            flops=2 * MAX_STEPS * slots * cells * cells,
            transcendentals=2 * MAX_STEPS * slots * cells,
            bytes_accessed=2 * cells * cells + 12 * slots * cells,
        ),
        aliases={7: 2},
    )(ids_row, steps_row, jump, stiffness, coupling, old_state, old_history, mine)
    fields, near, far = call(
        fields_kernel,
        (shape(FIELDS, rows, lanes), shape(edge, lanes), shape(edge, lanes)),
        [VMEM] * 7,
        (VMEM,) * 3,
        4,
    )(ids_row, steps_row, jump, external, cohesive, bond_mask, grid)
    row_near, row_far = swap(near, far, "row")
    counts = lax.all_to_all(mine, ROWS_COLS, 0, 0, tiled=True).reshape(devices, LANES)
    packed = call(pack_kernel, packed_shape, [SMEM, SMEM, VMEM, VMEM, VMEM], VMEM, 12)(
        here[None], newton_steps, counts, state, old_history
    )
    near, far = call(
        lane_edges_kernel, (shape(edge, lanes), shape(edge, lanes)), [VMEM] * 3, (VMEM, VMEM), 4
    )(fields, row_near, row_far)
    col_near, col_far = swap(near, far, "col")
    moved, packed = call(
        macro_kernel,
        (shape(6, rows, lanes), packed_shape),
        [SMEM, SMEM] + [VMEM] * 5 + [HBM],
        (VMEM, HBM),
        12,
        scratch=(pltpu.VMEM((devices, 1, LANES), F32), pltpu.SemaphoreType.DMA),
        cost=pl.CostEstimate(flops=200_000_000, transcendentals=0, bytes_accessed=2_000_000),
        aliases={7: 1},
    )(place, load_factor, fields, row_near, row_far, col_near, col_far, packed)
    arrived = lax.all_to_all(packed, ROWS_COLS, 0, 0, tiled=True)
    plan = call(plan_kernel, shape(8, LANES, dtype=jnp.int32), [SMEM, VMEM], VMEM, 2)(here[None], counts)
    new_jump, new_load, new_state, new_history = call(
        functools.partial(last_kernel, 3.0 * rows * lanes * devices),
        (shape(3, rows, lanes), shape(1), shape(slots // 2, cells), shape(slots // 2, cells)),
        [SMEM, SMEM, SMEM, VMEM, VMEM],
        (VMEM, SMEM, VMEM, VMEM),
        12,
    )(plan, load_factor, arc_radius, arrived, moved)
    return (new_jump, new_load, new_state, new_history)


def solution(mesh):
    whole = P(None, "row", "col")
    slot_rows = P(ROWS_COLS, None)
    return jax.shard_map(
        on_device,
        mesh=mesh,
        in_specs=(
            whole, whole, P("row", "col"), whole, P(), P(), P(), P(),
            slot_rows, slot_rows, P(ROWS_COLS), P(ROWS_COLS),
        ),
        out_specs=(whole, P(), slot_rows, slot_rows),
        check_vma=False,
    )
```
